256 devices in a mesh: gx: 16 (over y, x), gy: 8 (over z), gz: 2 (over core).
Axes of the slice: x: 4, y: 4, z: 8, core: 2. Of those that a mesh axis runs over, the one named last changes fastest.
Arguments:
- estimate: float32 [16, 1024, 1024], P('gz', 'gx', 'gy'), may hold values from 0.25 to 4
- view_data: float32 [16, 1024, 1024], P('gz', 'gx', 'gy'), may hold values from 0.25 to 4
- psf_stack: float32 [6, 31, 31, 31], replicated, may hold values from 0.01 to 1.53, as said below
- view_index: int32 [1], replicated, may hold values from 0 to 5
Outputs:
- updated_estimate: float32 [16, 1024, 1024], P('gz', 'gx', 'gy')
- level_one: float32 [8, 512, 512], P('gz', 'gx', 'gy')
- level_two: float32 [4, 256, 256], P('gz', 'gx', 'gy')
- level_three: float32 [2, 128, 128], P('gz', 'gx', 'gy')
- level_four: float32 [1, 64, 64], P(None, 'gx', 'gy')
- level_five: float32 [1, 32, 32], replicated
The draws below stay inside these ranges and needn't reach their ends.
Inputs may be any that keep to these rules, and one draw needn't show every extreme that they name: `psf_stack`: every entry of every view's point spread function is positive.
All inputs are finite; a program needn't handle non-finite values.
Results may differ from the reference program's by a relative error of at most 0.000075.
Values sent between devices are 32-bit elements; how exact they have to be, the bound alone decides.
A program may use at most 128 MiB of HBM per device.

```python
import math
import jax
import jax.numpy as jnp
from jax import lax

HALO = 15
VIEWS = 6
NX = 1024
NY = 1024
NZ = 16


def draw_psf_stack(key, part):
    extent = 2 * HALO + 1
    first, second, third = jax.random.split(jax.random.fold_in(key, 7), 3)
    widths = jax.random.uniform(first, (VIEWS, 3), jnp.float32, 1.0, 4.5)
    offsets = jnp.arange(extent, dtype=jnp.float32) - HALO
    depth_term = offsets[None, :, None, None] / widths[:, 0, None, None, None]
    row_term = offsets[None, None, :, None] / widths[:, 1, None, None, None]
    column_term = offsets[None, None, None, :] / widths[:, 2, None, None, None]
    exponent = depth_term * depth_term + row_term * row_term + column_term * column_term
    roughness = jax.random.uniform(second, (VIEWS, extent, extent, extent), jnp.float32, 0.5, 1.5)
    floor_part = 0.02 * jax.random.uniform(third, (VIEWS, extent, extent, extent), jnp.float32, 0.5, 1.5)
    return jnp.exp(-0.5 * exponent) * roughness + floor_part


def levels(own_key, shape, cuts, least, high):
    def one(position, parts):
        steps = jax.random.uniform(jax.random.fold_in(jax.random.fold_in(own_key, 6), position), (parts,), jnp.float32, least / len(cuts), high / len(cuts))
        return jnp.repeat(jnp.exp(steps), shape[position] // parts).reshape((-1,) + (1,) * (len(shape) - position - 1))

    loudness = one(*cuts[0])
    for cut in cuts[1:]:
        loudness = loudness * one(*cut)
    return loudness


def setup_inputs(seed: int = 0) -> dict:
    streams_of = jax.random.split(jax.random.key(seed), 5)
    return {
        "estimate": jnp.clip(jnp.exp(math.log(4.0) - 2.7725887 * jax.random.uniform(streams_of[0], (NZ, NX, NY), jnp.float32) ** levels(streams_of[0], (NZ, NX, NY), ((0, 2), (1, 16), (2, 8)), -0.2, 0.2)), 0.25, 4.0),
        "view_data": jnp.clip(jnp.exp(math.log(4.0) - 2.7725887 * jax.random.uniform(streams_of[1], (NZ, NX, NY), jnp.float32) ** levels(streams_of[1], (NZ, NX, NY), ((0, 2), (1, 16), (2, 8)), -0.2, 0.2)), 0.25, 4.0),
        "psf_stack": draw_psf_stack(jax.random.fold_in(streams_of[4], 71), 0),
        "view_index": jax.random.randint(streams_of[3], (1,), 0, VIEWS).astype(jnp.int32),
    }


def convolve(volume, kernel):
    radius = (kernel.shape[0] - 1) // 2
    fft_sizes = tuple(((extent + 2 * radius + 15) // 16) * 16 for extent in volume.shape)
    product = jnp.fft.rfftn(volume, fft_sizes) * jnp.fft.rfftn(kernel, fft_sizes)
    full_conv = jnp.fft.irfftn(product, fft_sizes)
    plane_count, row_count, column_count = volume.shape
    return full_conv[radius:radius + plane_count, radius:radius + row_count, radius:radius + column_count].astype(jnp.float32)


def average_blocks(volume, depth):
    plane_count, row_count, column_count = volume.shape
    if depth:
        blocks = volume.reshape(plane_count // 2, 2, row_count // 2, 2, column_count // 2, 2)
        return jnp.mean(blocks, axis=(1, 3, 5))
    blocks = volume.reshape(plane_count, row_count // 2, 2, column_count // 2, 2)
    return jnp.mean(blocks, axis=(2, 4))


def reference(estimate, view_data, psf_stack, view_index):
    kernel = lax.dynamic_index_in_dim(psf_stack, view_index[0], 0, keepdims=False)
    kernel = kernel / jnp.sum(kernel)
    blurred = convolve(estimate, kernel)
    ratio_field = view_data / blurred
    correction = convolve(ratio_field, jnp.flip(kernel))
    updated = estimate * correction
    level_one = average_blocks(updated, True)
    level_two = average_blocks(level_one, True)
    level_three = average_blocks(level_two, True)
    level_four = average_blocks(level_three, True)
    level_five = average_blocks(level_four, False)
    return updated, level_one, level_two, level_three, level_four, level_five
```

```python
import functools

import jax
import jax.numpy as jnp
import numpy as np
from jax import lax
from jax.experimental import pallas as pl
from jax.experimental.pallas import tpu as pltpu
from jax.sharding import PartitionSpec as P

MESH = pl.DeviceIdType.MESH
HALO = 15
EDGE = 16
ROWS, COLUMNS = 64, 128
LX, LY = ROWS + 2 * EDGE, COLUMNS + 2 * EDGE
HALF = LY // 2 + 1
TAPS = 2 * HALO + 1
BF16, F32 = jnp.bfloat16, jnp.float32


def parts_of(table):
    table = np.asarray(table, np.float64)
    high = table.astype(np.float32).astype(BF16)
    low = (table - high.astype(np.float64)).astype(np.float32).astype(BF16)
    return high, low


def stacked(table):
    high, low = parts_of(table)
    return np.concatenate([high, low, high], axis=0)


def beside(table):
    high, low = parts_of(table)
    return np.concatenate([high, high, low], axis=1)


def column_table(positions):
    angle = 2.0 * np.pi / LY * np.outer(positions, np.arange(HALF))
    table = np.zeros((len(positions), 256))
    table[:, :HALF] = np.cos(angle)
    table[:, 128 : 128 + HALF] = -np.sin(angle)
    return table


def row_table(positions):
    angle = 2.0 * np.pi / LX * np.outer(np.arange(LX), positions)
    c, s = np.cos(angle), np.sin(angle)
    return np.block([[c, s], [-s, c]])


def tables():
    inner = column_table(EDGE + np.arange(COLUMNS))
    left = column_table(np.arange(EDGE))
    right = column_table(LY - EDGE + np.arange(EDGE))
    first = stacked(np.concatenate([inner] + [left, right] * 4))
    second = stacked(np.concatenate([inner] + [right, left] * 4))
    rows = beside(row_table(np.arange(LX)))
    angle = 2.0 * np.pi / LX * np.outer(EDGE + np.arange(ROWS), np.arange(LX))
    c, s = np.cos(angle), np.sin(angle)
    rows_back = beside(np.block([[c, -s], [s, c]]))
    angle = 2.0 * np.pi / LY * np.outer(np.arange(HALF), EDGE + np.arange(COLUMNS))
    weight = np.where(np.isin(np.arange(HALF), (0, LY // 2)), 1.0, 2.0)[:, None] / (LX * LY)
    back = np.zeros((256, COLUMNS))
    back[:HALF] = weight * np.cos(angle)
    back[128 : 128 + HALF] = -weight * np.sin(angle)
    columns_back = stacked(back)
    taps = column_table(np.concatenate([np.arange(TAPS) - HALO, [0]]))
    taps[TAPS] = 0.0
    tap_columns = np.concatenate([stacked(taps), np.zeros((32, 256), BF16)], axis=0)
    tap_rows_table = row_table(np.concatenate([np.arange(TAPS) - HALO, [0]]))
    tap_rows_table[:, TAPS] = 0.0
    tap_rows_table[:, 32 + TAPS] = 0.0
    tap_rows = beside(tap_rows_table)
    pools = np.zeros((128, 512), np.float32)
    for level in range(4):
        step = 2 ** (level + 1)
        for column in range(COLUMNS):
            pools[column, 128 * level + column // step] = 1.0 / step
    pools = np.concatenate([pools] * 3, axis=0).astype(BF16)
    return first, second, rows, rows_back, columns_back, tap_columns, tap_rows, pools


def two(x):
    high = x.astype(BF16)
    return high, (x - high.astype(F32)).astype(BF16)


def dot(a, b):
    return jnp.dot(a, b, preferred_element_type=F32)


def left_triple(x):
    high, low = two(x)
    return jnp.concatenate([high, high, low], axis=1)


def right_triple(x):
    high, low = two(x)
    return jnp.concatenate([high, low, high], axis=0)


def exact_triple(x):
    high = x.astype(BF16)
    rest = x - high.astype(F32)
    middle = rest.astype(BF16)
    low = (rest - middle.astype(F32)).astype(BF16)
    return jnp.concatenate([high, middle, low], axis=1)


def body(
    nx,
    ny,
    index_ref,
    est_ref,
    view_ref,
    psf_hbm,
    first_ref,
    second_ref,
    rows_ref,
    rows_back_ref,
    columns_back_ref,
    tap_columns_ref,
    tap_rows_ref,
    pools_ref,
    updated_ref,
    one_ref,
    two_ref,
    three_ref,
    four_ref,
    five_ref,
    psf_ref,
    taps_ref,
    tap_half_ref,
    kernel_ref,
    ratio_ref,
    edge_rows,
    edge_columns,
    packed,
    own_ref,
    other_ref,
    product_ref,
    pool_a,
    pool_b,
    pool_c,
    pool_d,
    plane_ref,
    tile_ref,
    strips_ref,
    local_sem,
    send_sem,
    recv_sem,
    part_send,
    part_recv,
    ring_send,
    ring_recv,
):
    gx, gy, gz = lax.axis_index("gx"), lax.axis_index("gy"), lax.axis_index("gz")

    def device(dx, dy, dz=0):
        return {
            "gx": lax.rem(gx + dx + nx, nx),
            "gy": lax.rem(gy + dy + ny, ny),
            "gz": lax.rem(gz + dz, 2),
        }

    fetch = pltpu.make_async_copy(psf_hbm, psf_ref, local_sem)
    fetch.start()

    peers = [(dx, dy, 0) for dx in (-1, 0, 1) for dy in (-1, 0, 1) if (dx, dy) != (0, 0)]
    peers.append((0, 0, 1))
    peers += [(0, k, 0) for k in range(2, ny - 1)]
    peers += [(k, 0, 0) for k in range(2, nx - 1)]
    barrier = pltpu.get_barrier_semaphore()
    for peer in peers:
        pl.semaphore_signal(barrier, inc=1, device_id=device(*peer), device_id_type=MESH)

    def pack(source, turn):
        lane = lax.broadcasted_iota(jnp.int32, (ROWS, 128), 1)
        to_right = jnp.zeros((ROWS, 128), F32)
        to_left = jnp.zeros((ROWS, 128), F32)
        for z in range(8):
            base = (z % 4) * 32
            low, high = (base, base + EDGE) if z < 4 else (base + EDGE, base)
            plane = source[z]
            shift = (low - (COLUMNS - EDGE)) % 128
            rolled = pltpu.roll(plane, shift, 1) if shift else plane
            to_right = jnp.where((lane >= low) & (lane < low + EDGE), rolled, to_right)
            rolled = pltpu.roll(plane, high, 1) if high else plane
            to_left = jnp.where((lane >= high) & (lane < high + EDGE), rolled, to_left)
        packed[turn, 0] = to_right
        packed[turn, 1] = to_left

    middle, top, bottom = pl.ds(EDGE, ROWS), pl.ds(0, EDGE), pl.ds(EDGE + ROWS, EDGE)
    head, tail = pl.ds(0, EDGE), pl.ds(ROWS - EDGE, EDGE)

    def halo_copies(source, turn):
        def copy(src, dst, at, dx, dy):
            return pltpu.make_async_remote_copy(
                src_ref=src,
                dst_ref=dst,
                send_sem=send_sem.at[turn, at],
                recv_sem=recv_sem.at[turn, at],
                device_id=device(dx, dy),
                device_id_type=MESH,
            )

        right, left = packed.at[turn, 0], packed.at[turn, 1]
        from_left, from_right = edge_columns.at[turn, 0], edge_columns.at[turn, 1]
        return [
            copy(source.at[:, tail, :], edge_rows.at[turn, 0], 0, 1, 0),
            copy(source.at[:, head, :], edge_rows.at[turn, 1], 1, -1, 0),
            copy(right.at[tail, :], from_left.at[top, :], 2, 1, 1),
            copy(right.at[head, :], from_left.at[bottom, :], 3, -1, 1),
            copy(left.at[tail, :], from_right.at[top, :], 4, 1, -1),
            copy(left.at[head, :], from_right.at[bottom, :], 5, -1, -1),
            copy(right, from_left.at[middle, :], 6, 0, 1),
            copy(left, from_right.at[middle, :], 7, 0, -1),
        ]

    def clear_borders(turn):
        @pl.when(gx == 0)
        def _():
            edge_rows[turn, 0] = jnp.zeros((8, EDGE, 128), F32)
            for side in (0, 1):
                edge_columns[turn, side, top, :] = jnp.zeros((EDGE, 128), F32)

        @pl.when(gx == nx - 1)
        def _():
            edge_rows[turn, 1] = jnp.zeros((8, EDGE, 128), F32)
            for side in (0, 1):
                edge_columns[turn, side, bottom, :] = jnp.zeros((EDGE, 128), F32)

        @pl.when(gy == 0)
        def _():
            edge_columns[turn, 0] = jnp.zeros((LX, 128), F32)

        @pl.when(gy == ny - 1)
        def _():
            edge_columns[turn, 1] = jnp.zeros((LX, 128), F32)

    def partner_copy(turn, z):
        return pltpu.make_async_remote_copy(
            src_ref=own_ref.at[turn, z],
            dst_ref=other_ref.at[turn, z],
            send_sem=part_send.at[turn, z],
            recv_sem=part_recv.at[turn, z],
            device_id=device(0, 0, 1),
            device_id_type=MESH,
        )

    def forward(source, turn):
        lane = lax.broadcasted_iota(jnp.int32, (LX, 128), 1)
        even = (lane & EDGE) == 0
        left, right = edge_columns[turn, 0], edge_columns[turn, 1]
        for group, table in ((0, first_ref), (1, second_ref)):
            mixed = jnp.where(even, left, right) if group == 0 else jnp.where(even, right, left)
            rows = []
            for j in range(4):
                z = 4 * group + j
                plane = jnp.concatenate(
                    [edge_rows[turn, 0, z], source[z], edge_rows[turn, 1, z]], axis=0
                )
                side = jnp.where((lane >= 32 * j) & (lane < 32 * j + 32), mixed, 0.0)
                rows.append(jnp.concatenate([plane, side], axis=1))
            half = dot(left_triple(jnp.concatenate(rows, axis=0)), table[...])
            for pair in (0, 1):
                a = half[192 * pair : 192 * pair + 96]
                b = half[192 * pair + 96 : 192 * pair + 192]
                joint = jnp.concatenate(
                    [
                        jnp.concatenate([a[:, :128], b[:, :128]], axis=1),
                        jnp.concatenate([a[:, 128:], b[:, 128:]], axis=1),
                    ],
                    axis=0,
                )
                full = dot(rows_ref[...], right_triple(joint))
                z = 4 * group + 2 * pair
                own_ref[turn, z] = full[:, :128]
                own_ref[turn, z + 1] = full[:, 128:]
                partner_copy(turn, z).start()
                partner_copy(turn, z + 1).start()

    def depth(x_ref, turn, base, mirrored, adding):
        def block(step, carry):
            at = pl.multiple_of(step * 8, 8)
            re, im = pl.ds(at, 8), pl.ds(pl.multiple_of(at + LX, 8), 8)
            xr = [x_ref[turn, z, re, :] for z in range(8)]
            xi = [x_ref[turn, z, im, :] for z in range(8)]
            if adding:
                yr = [product_ref[z, re, :] for z in range(8)]
                yi = [product_ref[z, im, :] for z in range(8)]
            else:
                yr, yi = [None] * 8, [None] * 8
            for d in range(-7, 8):
                kr, ki = kernel_ref[base + d, re, :], kernel_ref[base + d, im, :]
                for out in range(8):
                    z = out + d if mirrored else out - d
                    if not 0 <= z < 8:
                        continue
                    if mirrored:
                        r = kr * xr[z] + ki * xi[z]
                        i = kr * xi[z] - ki * xr[z]
                    else:
                        r = kr * xr[z] - ki * xi[z]
                        i = kr * xi[z] + ki * xr[z]
                    yr[out] = r if yr[out] is None else yr[out] + r
                    yi[out] = i if yi[out] is None else yi[out] + i
            for z in range(8):
                product_ref[z, re, :] = yr[z]
                product_ref[z, im, :] = yi[z]
            return carry

        lax.fori_loop(0, LX // 8, block, 0)

    def inverse(group):
        rows = []
        for pair in (0, 1):
            z = 4 * group + 2 * pair
            joint = jnp.concatenate([product_ref[z], product_ref[z + 1]], axis=1)
            half = dot(rows_back_ref[...], right_triple(joint))
            for b in (0, 1):
                lanes = slice(128 * b, 128 * b + 128)
                rows.append(jnp.concatenate([half[:ROWS, lanes], half[ROWS:, lanes]], axis=1))
        full = dot(left_triple(jnp.concatenate(rows, axis=0)), columns_back_ref[...])
        return full.reshape(4, ROWS, COLUMNS)

    def convolve(source, turn, mirrored):
        forward(source, turn)
        depth(own_ref, turn, HALO, mirrored, False)
        for z in range(8):
            partner_copy(turn, z).wait_recv()
        base = HALO + 8 - 16 * gz if mirrored else HALO - 8 + 16 * gz
        depth(other_ref, turn, base, mirrored, True)

    def spectrum():
        fetch.wait()
        view = index_ref[0]
        taps_ref[...] = jnp.zeros((32, 32, 128), F32)

        def load(z, total):
            values = psf_ref[view, z]
            taps_ref[z, 0:TAPS, 0:TAPS] = values
            return total

        lax.fori_loop(0, TAPS, load, 0)
        total = jnp.sum(jnp.sum(taps_ref[...], axis=0), axis=(0, 1), keepdims=True)
        scale = 1.0 / total

        def columns(step, carry):
            x = taps_ref[pl.ds(step * 8, 8)].reshape(256, 128) * scale
            high = x.astype(BF16).astype(F32)
            low = x - high
            joint = high + pltpu.roll(high, 32, 1) + pltpu.roll(low, 64, 1)
            tap_half_ref[pl.ds(step * 8, 8)] = dot(joint.astype(BF16), tap_columns_ref[...]).reshape(
                8, 32, 256
            )
            return carry

        lax.fori_loop(0, 4, columns, 0)

        def rows(step, carry):
            a, b = tap_half_ref[2 * step], tap_half_ref[2 * step + 1]
            joint = jnp.concatenate(
                [
                    jnp.concatenate([a[:, :128], b[:, :128]], axis=1),
                    jnp.concatenate([a[:, 128:], b[:, 128:]], axis=1),
                ],
                axis=0,
            )
            full = dot(tap_rows_ref[...], right_triple(joint))
            kernel_ref[2 * step] = full[:, :128]
            kernel_ref[2 * step + 1] = full[:, 128:]
            return carry

        lax.fori_loop(0, 16, rows, 0)

    pack(est_ref, 0)
    pl.semaphore_wait(barrier, len(peers))
    copies = halo_copies(est_ref, 0)
    for copy in copies:
        copy.start()
    spectrum()
    for copy in copies:
        copy.wait_recv()
    clear_borders(0)
    convolve(est_ref, 0, False)
    for group in (0, 1):
        at = pl.ds(4 * group, 4)
        ratio_ref[at] = view_ref[at] / inverse(group)

    pack(ratio_ref, 1)
    later = halo_copies(ratio_ref, 1)
    for copy in later:
        copy.start()
    for copy in later:
        copy.wait_recv()
    clear_borders(1)
    convolve(ratio_ref, 1, True)
    for group in (0, 1):
        at = pl.ds(4 * group, 4)
        updated = est_ref[at] * inverse(group)
        updated_ref[at] = updated
        for pair in (0, 1):
            pool_a[2 * group + pair] = updated[2 * pair] + updated[2 * pair + 1]

    even, odd = pl.ds(0, ROWS // 2, stride=2), pl.ds(1, ROWS // 2, stride=2)
    level_one = [(pool_a[k, even, :] + pool_a[k, odd, :]) * 0.25 for k in range(4)]
    for k in (0, 1):
        pool_b[k] = level_one[2 * k] + level_one[2 * k + 1]
    even, odd = pl.ds(0, ROWS // 4, stride=2), pl.ds(1, ROWS // 4, stride=2)
    level_two = [(pool_b[k, even, :] + pool_b[k, odd, :]) * 0.25 for k in (0, 1)]
    pool_c[...] = level_two[0] + level_two[1]
    even, odd = pl.ds(0, ROWS // 8, stride=2), pl.ds(1, ROWS // 8, stride=2)
    level_three = (pool_c[even, :] + pool_c[odd, :]) * 0.25
    pool_d[0:8] = level_three
    pool_d[8:16] = jnp.zeros((8, 128), F32)
    even, odd = pl.ds(0, 8, stride=2), pl.ds(1, 8, stride=2)
    level_four = (pool_d[even, :] + pool_d[odd, :]) * 0.5
    plane_ref[0] = dot(exact_triple(level_four), pools_ref[:, 384:])
    swap = pltpu.make_async_remote_copy(
        src_ref=plane_ref.at[0],
        dst_ref=plane_ref.at[1],
        send_sem=ring_send.at[0],
        recv_sem=ring_recv.at[0],
        device_id=device(0, 0, 1),
        device_id_type=MESH,
    )
    swap.start()
    third = dot(exact_triple(level_three), pools_ref[:, 256:384])
    three_ref[0] = third[:, :16]
    second = dot(exact_triple(jnp.concatenate(level_two, axis=0)), pools_ref[:, 128:256])
    for k in (0, 1):
        two_ref[k] = second[16 * k : 16 * k + 16, :32]
    full = dot(exact_triple(jnp.concatenate(level_one, axis=0)), pools_ref[:, :128])
    for k in range(4):
        one_ref[k] = full[32 * k : 32 * k + 32, :64]
    swap.wait_recv()
    fourth = (plane_ref[0] + plane_ref[1]) * 0.5
    four_ref[0] = fourth[:4, :8]
    pool_d[0:8] = fourth
    fifth = pool_d[even, :] + pool_d[odd, :]
    source = lax.broadcasted_iota(jnp.int32, (384, 128), 0) % 128
    target = lax.broadcasted_iota(jnp.int32, (384, 128), 1)
    place = (source < 8) & (target == 4 * gy + source // 2)
    tile_ref[0] = dot(exact_triple(fifth), jnp.where(place, 0.25, 0.0).astype(BF16))

    def tile_copy(k):
        return pltpu.make_async_remote_copy(
            src_ref=tile_ref.at[0],
            dst_ref=tile_ref.at[k],
            send_sem=ring_send.at[k],
            recv_sem=ring_recv.at[k],
            device_id=device(0, k),
            device_id_type=MESH,
        )

    def strip_copy(k):
        return pltpu.make_async_remote_copy(
            src_ref=strips_ref.at[gx],
            dst_ref=strips_ref.at[gx],
            send_sem=ring_send.at[ny + k],
            recv_sem=ring_recv.at[ny + k],
            device_id=device(k, 0),
            device_id_type=MESH,
        )

    def strip_wait(k):
        slot = strips_ref.at[lax.rem(gx - k + nx, nx)]
        pltpu.make_async_remote_copy(
            src_ref=slot,
            dst_ref=slot,
            send_sem=ring_send.at[ny + k],
            recv_sem=ring_recv.at[ny + k],
            device_id=device(k, 0),
            device_id_type=MESH,
        ).wait_recv()

    for k in range(1, ny):
        tile_copy(k).start()
    strip = tile_ref[0]
    for k in range(1, ny):
        tile_copy(k).wait_recv()
        strip = strip + tile_ref[k]
    strips_ref[gx] = strip
    for k in range(1, nx):
        strip_copy(k).start()
    for k in range(1, nx):
        strip_wait(k)
    for g in range(nx):
        five_ref[0, 2 * g : 2 * g + 2, :] = strips_ref[g, 0:2, : 4 * ny]

    for copy in copies + later:
        copy.wait_send()
    for turn in (0, 1):
        for z in range(8):
            partner_copy(turn, z).wait_send()
    swap.wait_send()
    for k in range(1, ny):
        tile_copy(k).wait_send()
    for k in range(1, nx):
        strip_copy(k).wait_send()


def local(nx, ny, estimate, view_data, psf_stack, view_index):
    vmem = pl.BlockSpec(memory_space=pltpu.VMEM)
    shape = jax.ShapeDtypeStruct
    constants = [jnp.asarray(t) for t in tables()]
    return pl.pallas_call(
        functools.partial(body, nx, ny),
        out_shape=(
            shape((8, 64, 128), F32),
            shape((4, 32, 64), F32),
            shape((2, 16, 32), F32),
            shape((1, 8, 16), F32),
            shape((1, 4, 8), F32),
            shape((1, 2 * nx, 4 * ny), F32),
        ),
        in_specs=[
            pl.BlockSpec(memory_space=pltpu.SMEM),
            vmem,
            vmem,
            pl.BlockSpec(memory_space=pl.ANY),
        ]
        + [vmem] * len(constants),
        out_specs=(vmem,) * 6,
        scratch_shapes=[
            pltpu.VMEM(psf_stack.shape, F32),
            pltpu.VMEM((32, 32, 128), F32),
            pltpu.VMEM((32, 32, 256), F32),
            pltpu.VMEM((32, 2 * LX, 128), F32),
            pltpu.VMEM((8, ROWS, COLUMNS), F32),
            pltpu.VMEM((2, 2, 8, EDGE, 128), F32),
            pltpu.VMEM((2, 2, LX, 128), F32),
            pltpu.VMEM((2, 2, ROWS, 128), F32),
            pltpu.VMEM((2, 8, 2 * LX, 128), F32),
            pltpu.VMEM((2, 8, 2 * LX, 128), F32),
            pltpu.VMEM((8, 2 * LX, 128), F32),
            pltpu.VMEM((4, 64, 128), F32),
            pltpu.VMEM((2, 32, 128), F32),
            pltpu.VMEM((16, 128), F32),
            pltpu.VMEM((16, 128), F32),
            pltpu.VMEM((2, 8, 128), F32),
            pltpu.VMEM((ny, 8, 128), F32),
            pltpu.VMEM((nx, 8, 128), F32),
            pltpu.SemaphoreType.DMA,
            pltpu.SemaphoreType.DMA((2, 8)),
            pltpu.SemaphoreType.DMA((2, 8)),
            pltpu.SemaphoreType.DMA((2, 8)),
            pltpu.SemaphoreType.DMA((2, 8)),
            pltpu.SemaphoreType.DMA((nx + ny,)),
            pltpu.SemaphoreType.DMA((nx + ny,)),
        ],
        compiler_params=pltpu.CompilerParams(collective_id=0, has_side_effects=True),
    )(view_index, estimate, view_data, psf_stack, *constants)


def solution(mesh):
    spread = P("gz", "gx", "gy")
    return jax.shard_map(
        functools.partial(local, mesh.shape["gx"], mesh.shape["gy"]),
        mesh=mesh,
        in_specs=(spread, spread, P(), P()),
        out_specs=(spread, spread, spread, spread, P(None, "gx", "gy"), P()),
        check_vma=False,
    )
```

```python
import functools

import jax
import jax.numpy as jnp
import numpy as np
from jax import lax
from jax.experimental import pallas as pl
from jax.experimental.pallas import tpu as pltpu
from jax.sharding import PartitionSpec as P

MESH = pl.DeviceIdType.MESH
HALO = 15
EDGE = 16
ROWS, COLUMNS = 64, 128
LX, LY = ROWS + 2 * EDGE, COLUMNS + 2 * EDGE
HALF = LY // 2 + 1
TAPS = 2 * HALO + 1
BF16, F32 = jnp.bfloat16, jnp.float32


def parts_of(table):
    table = np.asarray(table, np.float64)
    high = table.astype(np.float32).astype(BF16)
    low = (table - high.astype(np.float64)).astype(np.float32).astype(BF16)
    return high, low


def stacked(table):
    high, low = parts_of(table)
    return np.concatenate([high, low, high], axis=0)


def beside(table):
    high, low = parts_of(table)
    return np.concatenate([high, high, low], axis=1)


def column_table(positions):
    angle = 2.0 * np.pi / LY * np.outer(positions, np.arange(HALF))
    table = np.zeros((len(positions), 256))
    table[:, :HALF] = np.cos(angle)
    table[:, 128 : 128 + HALF] = -np.sin(angle)
    return table


def row_table(positions):
    angle = 2.0 * np.pi / LX * np.outer(np.arange(LX), positions)
    c, s = np.cos(angle), np.sin(angle)
    return np.block([[c, s], [-s, c]])


def tables():
    inner = column_table(EDGE + np.arange(COLUMNS))
    left = column_table(np.arange(EDGE))
    right = column_table(LY - EDGE + np.arange(EDGE))
    first = stacked(np.concatenate([inner] + [left, right] * 4))
    second = stacked(np.concatenate([inner] + [right, left] * 4))
    rows = beside(row_table(np.arange(LX)))
    angle = 2.0 * np.pi / LX * np.outer(EDGE + np.arange(ROWS), np.arange(LX))
    c, s = np.cos(angle), np.sin(angle)
    rows_back = beside(np.block([[c, -s], [s, c]]))
    angle = 2.0 * np.pi / LY * np.outer(np.arange(HALF), EDGE + np.arange(COLUMNS))
    weight = np.where(np.isin(np.arange(HALF), (0, LY // 2)), 1.0, 2.0)[:, None] / (LX * LY)
    back = np.zeros((256, COLUMNS))
    back[:HALF] = weight * np.cos(angle)
    back[128 : 128 + HALF] = -weight * np.sin(angle)
    columns_back = stacked(back)
    taps = column_table(np.concatenate([np.arange(TAPS) - HALO, [0]]))
    taps[TAPS] = 0.0
    tap_columns = np.concatenate([stacked(taps), np.zeros((32, 256), BF16)], axis=0)
    tap_rows_table = row_table(np.concatenate([np.arange(TAPS) - HALO, [0]]))
    tap_rows_table[:, TAPS] = 0.0
    tap_rows_table[:, 32 + TAPS] = 0.0
    tap_rows = beside(tap_rows_table)
    pools = np.zeros((128, 512), np.float32)
    for level in range(4):
        step = 2 ** (level + 1)
        for column in range(COLUMNS):
            pools[column, 128 * level + column // step] = 1.0 / step
    pools = np.concatenate([pools] * 3, axis=0).astype(BF16)
    return first, second, rows, rows_back, columns_back, tap_columns, tap_rows, pools


def two(x):
    high = x.astype(BF16)
    return high, (x - high.astype(F32)).astype(BF16)


def dot(a, b):
    return jnp.dot(a, b, preferred_element_type=F32)


def left_triple(x):
    high, low = two(x)
    return jnp.concatenate([high, high, low], axis=1)


def right_triple(x):
    high, low = two(x)
    return jnp.concatenate([high, low, high], axis=0)


def exact_triple(x):
    high = x.astype(BF16)
    rest = x - high.astype(F32)
    middle = rest.astype(BF16)
    low = (rest - middle.astype(F32)).astype(BF16)
    return jnp.concatenate([high, middle, low], axis=1)


def body(nx, ny, index_ref, *refs):
    inputs, refs = refs[:11], refs[11:]
    updated_ref, one_ref, two_ref, three_ref, four_ref, five_ref = refs[:6]
    held, refs = refs[6:17], refs[17:]
    (
        est_ref,
        view_ref,
        psf_ref,
        first_ref,
        second_ref,
        rows_ref,
        rows_back_ref,
        columns_back_ref,
        tap_columns_ref,
        tap_rows_ref,
        pools_ref,
    ) = held
    (
        taps_ref,
        tap_half_ref,
        kernel_ref,
        ratio_ref,
        edge_rows,
        edge_columns,
        packed,
        own_ref,
        other_ref,
        product_ref,
        pool_a,
        pool_b,
        pool_c,
        pool_d,
        plane_ref,
        tile_ref,
        gathered,
        local_sem,
        send_sem,
        recv_sem,
        part_send,
        part_recv,
        swap_send,
        swap_recv,
        all_send,
        all_recv,
        wider_sem,
        widest_sem,
    ) = refs
    gx, gy, gz = lax.axis_index("gx"), lax.axis_index("gy"), lax.axis_index("gz")

    def device(dx, dy, dz=0):
        return {
            "gx": lax.rem(gx + dx + nx, nx),
            "gy": lax.rem(gy + dy + ny, ny),
            "gz": lax.rem(gz + dz, 2),
        }

    fetches = [
        pltpu.make_async_copy(source, target, local_sem.at[k])
        for k, (source, target) in enumerate(zip(inputs, held))
    ]
    fetches[0].start()

    peers = [(dx, dy, 0) for dx in (-1, 0, 1) for dy in (-1, 0, 1) if (dx, dy) != (0, 0)]
    peers.append((0, 0, 1))
    count = nx * ny
    centre = (nx // 2) * ny + ny // 2
    barrier = pltpu.get_barrier_semaphore()
    for peer in peers:
        pl.semaphore_signal(barrier, inc=1, device_id=device(*peer), device_id_type=MESH)
    for k in (2, 8, 9, 3, 4, 5, 6, 7, 1, 10):
        fetches[k].start()

    def far(k):
        dx, dy = k // ny + nx // 2, lax.rem(k, ny) + ny // 2
        return lax.rem(dx, nx), lax.rem(dy, ny)

    def over_far(step):
        lax.fori_loop(0, centre, step, 0)
        lax.fori_loop(centre + 1, count, step, 0)

    def spread_word(sem, offsets):
        for dx, dy in offsets:
            pl.semaphore_signal(sem, inc=1, device_id=device(dx, dy), device_id_type=MESH)

    wider = [(dx, dy) for dx in (-2, 0, 2) for dy in (-2, 0, 2) if (dx, dy) != (0, 0)]
    widest = [(-4, 0), (4, 0)]

    def pack(source, turn):
        lane = lax.broadcasted_iota(jnp.int32, (ROWS, 128), 1)
        to_right = jnp.zeros((ROWS, 128), F32)
        to_left = jnp.zeros((ROWS, 128), F32)
        for z in range(8):
            base = (z % 4) * 32
            low, high = (base, base + EDGE) if z < 4 else (base + EDGE, base)
            plane = source[z]
            shift = (low - (COLUMNS - EDGE)) % 128
            rolled = pltpu.roll(plane, shift, 1) if shift else plane
            to_right = jnp.where((lane >= low) & (lane < low + EDGE), rolled, to_right)
            rolled = pltpu.roll(plane, high, 1) if high else plane
            to_left = jnp.where((lane >= high) & (lane < high + EDGE), rolled, to_left)
        packed[turn, 0] = to_right
        packed[turn, 1] = to_left

    middle, top, bottom = pl.ds(EDGE, ROWS), pl.ds(0, EDGE), pl.ds(EDGE + ROWS, EDGE)
    head, tail = pl.ds(0, EDGE), pl.ds(ROWS - EDGE, EDGE)

    def halo_copies(source, turn):
        def copy(src, dst, at, dx, dy):
            return pltpu.make_async_remote_copy(
                src_ref=src,
                dst_ref=dst,
                send_sem=send_sem.at[turn, at],
                recv_sem=recv_sem.at[turn, at],
                device_id=device(dx, dy),
                device_id_type=MESH,
            )

        right, left = packed.at[turn, 0], packed.at[turn, 1]
        from_left, from_right = edge_columns.at[turn, 0], edge_columns.at[turn, 1]
        return [
            copy(source.at[:, tail, :], edge_rows.at[turn, 0], 0, 1, 0),
            copy(source.at[:, head, :], edge_rows.at[turn, 1], 1, -1, 0),
            copy(right.at[tail, :], from_left.at[top, :], 2, 1, 1),
            copy(right.at[head, :], from_left.at[bottom, :], 3, -1, 1),
            copy(left.at[tail, :], from_right.at[top, :], 4, 1, -1),
            copy(left.at[head, :], from_right.at[bottom, :], 5, -1, -1),
            copy(right, from_left.at[middle, :], 6, 0, 1),
            copy(left, from_right.at[middle, :], 7, 0, -1),
        ]

    def clear_borders(turn):
        @pl.when(gx == 0)
        def _():
            edge_rows[turn, 0] = jnp.zeros((8, EDGE, 128), F32)
            for side in (0, 1):
                edge_columns[turn, side, top, :] = jnp.zeros((EDGE, 128), F32)

        @pl.when(gx == nx - 1)
        def _():
            edge_rows[turn, 1] = jnp.zeros((8, EDGE, 128), F32)
            for side in (0, 1):
                edge_columns[turn, side, bottom, :] = jnp.zeros((EDGE, 128), F32)

        @pl.when(gy == 0)
        def _():
            edge_columns[turn, 0] = jnp.zeros((LX, 128), F32)

        @pl.when(gy == ny - 1)
        def _():
            edge_columns[turn, 1] = jnp.zeros((LX, 128), F32)

    def partner_copy(turn, z):
        return pltpu.make_async_remote_copy(
            src_ref=own_ref.at[turn, z],
            dst_ref=other_ref.at[turn, z],
            send_sem=part_send.at[turn, z],
            recv_sem=part_recv.at[turn, z],
            device_id=device(0, 0, 1),
            device_id_type=MESH,
        )

    def forward(source, turn):
        lane = lax.broadcasted_iota(jnp.int32, (LX, 128), 1)
        even = (lane & EDGE) == 0
        left, right = edge_columns[turn, 0], edge_columns[turn, 1]
        for group, table in ((0, first_ref), (1, second_ref)):
            mixed = jnp.where(even, left, right) if group == 0 else jnp.where(even, right, left)
            rows = []
            for j in range(4):
                z = 4 * group + j
                plane = jnp.concatenate(
                    [edge_rows[turn, 0, z], source[z], edge_rows[turn, 1, z]], axis=0
                )
                side = jnp.where((lane >= 32 * j) & (lane < 32 * j + 32), mixed, 0.0)
                rows.append(jnp.concatenate([plane, side], axis=1))
            half = dot(left_triple(jnp.concatenate(rows, axis=0)), table[...])
            for pair in (0, 1):
                a = half[192 * pair : 192 * pair + 96]
                b = half[192 * pair + 96 : 192 * pair + 192]
                joint = jnp.concatenate(
                    [
                        jnp.concatenate([a[:, :128], b[:, :128]], axis=1),
                        jnp.concatenate([a[:, 128:], b[:, 128:]], axis=1),
                    ],
                    axis=0,
                )
                full = dot(rows_ref[...], right_triple(joint))
                z = 4 * group + 2 * pair
                own_ref[turn, z] = full[:, :128]
                own_ref[turn, z + 1] = full[:, 128:]
                partner_copy(turn, z).start()
                partner_copy(turn, z + 1).start()

    def depth(x_ref, turn, base, mirrored, adding):
        def block(step, carry):
            at = pl.multiple_of(step * 8, 8)
            re, im = pl.ds(at, 8), pl.ds(pl.multiple_of(at + LX, 8), 8)
            xr = [x_ref[turn, z, re, :] for z in range(8)]
            xi = [x_ref[turn, z, im, :] for z in range(8)]
            if adding:
                yr = [product_ref[z, re, :] for z in range(8)]
                yi = [product_ref[z, im, :] for z in range(8)]
            else:
                yr, yi = [None] * 8, [None] * 8
            for d in range(-7, 8):
                kr, ki = kernel_ref[base + d, re, :], kernel_ref[base + d, im, :]
                for out in range(8):
                    z = out + d if mirrored else out - d
                    if not 0 <= z < 8:
                        continue
                    if mirrored:
                        r = kr * xr[z] + ki * xi[z]
                        i = kr * xi[z] - ki * xr[z]
                    else:
                        r = kr * xr[z] - ki * xi[z]
                        i = kr * xi[z] + ki * xr[z]
                    yr[out] = r if yr[out] is None else yr[out] + r
                    yi[out] = i if yi[out] is None else yi[out] + i
            for z in range(8):
                product_ref[z, re, :] = yr[z]
                product_ref[z, im, :] = yi[z]
            return carry

        lax.fori_loop(0, LX // 8, block, 0)

    def inverse(group):
        rows = []
        for pair in (0, 1):
            z = 4 * group + 2 * pair
            joint = jnp.concatenate([product_ref[z], product_ref[z + 1]], axis=1)
            half = dot(rows_back_ref[...], right_triple(joint))
            for b in (0, 1):
                lanes = slice(128 * b, 128 * b + 128)
                rows.append(jnp.concatenate([half[:ROWS, lanes], half[ROWS:, lanes]], axis=1))
        full = dot(left_triple(jnp.concatenate(rows, axis=0)), columns_back_ref[...])
        return full.reshape(4, ROWS, COLUMNS)

    def convolve(source, turn, mirrored):
        forward(source, turn)
        depth(own_ref, turn, HALO, mirrored, False)
        for z in range(8):
            partner_copy(turn, z).wait_recv()
        base = HALO + 8 - 16 * gz if mirrored else HALO - 8 + 16 * gz
        depth(other_ref, turn, base, mirrored, True)

    def spectrum():
        for k in (2, 8, 9):
            fetches[k].wait()
        view = index_ref[0]
        taps_ref[...] = jnp.zeros((32, 32, 128), F32)

        def load(z, total):
            values = psf_ref[view, z]
            taps_ref[z, 0:TAPS, 0:TAPS] = values
            return total

        lax.fori_loop(0, TAPS, load, 0)
        total = jnp.sum(jnp.sum(taps_ref[...], axis=0), axis=(0, 1), keepdims=True)
        scale = 1.0 / total

        def columns(step, carry):
            x = taps_ref[pl.ds(step * 8, 8)].reshape(256, 128) * scale
            high = x.astype(BF16).astype(F32)
            low = x - high
            joint = high + pltpu.roll(high, 32, 1) + pltpu.roll(low, 64, 1)
            tap_half_ref[pl.ds(step * 8, 8)] = dot(joint.astype(BF16), tap_columns_ref[...]).reshape(
                8, 32, 256
            )
            return carry

        lax.fori_loop(0, 4, columns, 0)

        def rows(step, carry):
            a, b = tap_half_ref[2 * step], tap_half_ref[2 * step + 1]
            joint = jnp.concatenate(
                [
                    jnp.concatenate([a[:, :128], b[:, :128]], axis=1),
                    jnp.concatenate([a[:, 128:], b[:, 128:]], axis=1),
                ],
                axis=0,
            )
            full = dot(tap_rows_ref[...], right_triple(joint))
            kernel_ref[2 * step] = full[:, :128]
            kernel_ref[2 * step + 1] = full[:, 128:]
            return carry

        lax.fori_loop(0, 16, rows, 0)

    fetches[0].wait()
    pack(est_ref, 0)
    pl.semaphore_wait(barrier, len(peers))
    copies = halo_copies(est_ref, 0)
    for copy in copies:
        copy.start()
    spectrum()
    for copy in copies:
        copy.wait_recv()
    spread_word(wider_sem, wider)
    clear_borders(0)
    for k in (3, 4, 5, 6, 7, 1, 10):
        fetches[k].wait()
    convolve(est_ref, 0, False)
    for group in (0, 1):
        at = pl.ds(4 * group, 4)
        ratio_ref[at] = view_ref[at] / inverse(group)

    pl.semaphore_wait(wider_sem, len(wider))
    spread_word(widest_sem, widest)
    pack(ratio_ref, 1)
    later = halo_copies(ratio_ref, 1)
    for copy in later:
        copy.start()
    for copy in later:
        copy.wait_recv()
    clear_borders(1)
    convolve(ratio_ref, 1, True)
    for group in (0, 1):
        at = pl.ds(4 * group, 4)
        updated = est_ref[at] * inverse(group)
        updated_ref[at] = updated
        for pair in (0, 1):
            pool_a[2 * group + pair] = updated[2 * pair] + updated[2 * pair + 1]

    even, odd = pl.ds(0, ROWS // 2, stride=2), pl.ds(1, ROWS // 2, stride=2)
    level_one = [(pool_a[k, even, :] + pool_a[k, odd, :]) * 0.25 for k in range(4)]
    for k in (0, 1):
        pool_b[k] = level_one[2 * k] + level_one[2 * k + 1]
    even, odd = pl.ds(0, ROWS // 4, stride=2), pl.ds(1, ROWS // 4, stride=2)
    level_two = [(pool_b[k, even, :] + pool_b[k, odd, :]) * 0.25 for k in (0, 1)]
    pool_c[...] = level_two[0] + level_two[1]
    even, odd = pl.ds(0, ROWS // 8, stride=2), pl.ds(1, ROWS // 8, stride=2)
    level_three = (pool_c[even, :] + pool_c[odd, :]) * 0.25
    pool_d[0:8] = level_three
    pool_d[8:16] = jnp.zeros((8, 128), F32)
    even, odd = pl.ds(0, 8, stride=2), pl.ds(1, 8, stride=2)
    level_four = (pool_d[even, :] + pool_d[odd, :]) * 0.5
    plane_ref[0] = dot(exact_triple(level_four), pools_ref[:, 384:])
    swap = pltpu.make_async_remote_copy(
        src_ref=plane_ref.at[0],
        dst_ref=plane_ref.at[1],
        send_sem=swap_send,
        recv_sem=swap_recv,
        device_id=device(0, 0, 1),
        device_id_type=MESH,
    )
    swap.start()
    third = dot(exact_triple(level_three), pools_ref[:, 256:384])
    three_ref[0] = third[:, :16]
    second = dot(exact_triple(jnp.concatenate(level_two, axis=0)), pools_ref[:, 128:256])
    for k in (0, 1):
        two_ref[k] = second[16 * k : 16 * k + 16, :32]
    full = dot(exact_triple(jnp.concatenate(level_one, axis=0)), pools_ref[:, :128])
    for k in range(4):
        one_ref[k] = full[32 * k : 32 * k + 32, :64]
    swap.wait_recv()
    fourth = (plane_ref[0] + plane_ref[1]) * 0.5
    four_ref[0] = fourth[:4, :8]
    pool_d[0:8] = fourth
    fifth = pool_d[even, :] + pool_d[odd, :]
    source = lax.broadcasted_iota(jnp.int32, (384, 128), 0) % 128
    target = lax.broadcasted_iota(jnp.int32, (384, 128), 1)
    place = (source < 8) & (target == 4 * gy + source // 2)
    placed = dot(exact_triple(fifth), jnp.where(place, 0.25, 0.0).astype(BF16))
    tile_ref[...] = placed[0:1] + pltpu.roll(placed[1:2], 4 * ny, 1)
    me = gx * ny + gy

    def send(k, carry):
        pltpu.make_async_remote_copy(
            src_ref=tile_ref,
            dst_ref=gathered.at[me],
            send_sem=all_send,
            recv_sem=all_recv,
            device_id=device(*far(k)),
            device_id_type=MESH,
        ).start()
        return carry

    pl.semaphore_wait(widest_sem, len(widest))
    over_far(send)
    gathered[me] = tile_ref[...]
    others = gathered.at[pl.ds(0, count - 1)]
    everyone = pltpu.make_async_remote_copy(
        src_ref=others,
        dst_ref=others,
        send_sem=all_send,
        recv_sem=all_recv,
        device_id=device(0, 1),
        device_id_type=MESH,
    )
    everyone.wait_recv()
    strips = jnp.sum(gathered[...].reshape(nx, ny, 128), axis=1)
    five_ref[0, pl.ds(0, nx, stride=2), :] = strips[:, : 4 * ny]
    five_ref[0, pl.ds(1, nx, stride=2), :] = pltpu.roll(strips, 128 - 4 * ny, 1)[:, : 4 * ny]

    for copy in copies + later:
        copy.wait_send()
    for turn in (0, 1):
        for z in range(8):
            partner_copy(turn, z).wait_send()
    swap.wait_send()
    everyone.wait_send()


def hand_over(*refs):
    sources, targets, sems = refs[:6], refs[6:12], refs[12]
    copies = [pltpu.make_async_copy(a, b, sems.at[k]) for k, (a, b) in enumerate(zip(sources, targets))]
    for copy in copies:
        copy.start()
    for copy in copies:
        copy.wait()


def local(nx, ny, estimate, view_data, psf_stack, view_index):
    vmem = pl.BlockSpec(memory_space=pltpu.VMEM)
    anywhere = pl.BlockSpec(memory_space=pl.ANY)
    shape = jax.ShapeDtypeStruct
    out_shape = (
        shape((8, 64, 128), F32),
        shape((4, 32, 64), F32),
        shape((2, 16, 32), F32),
        shape((1, 8, 16), F32),
        shape((1, 4, 8), F32),
        shape((1, 2 * nx, 4 * ny), F32),
    )
    constants = [jnp.asarray(t) for t in tables()]
    kept = [
        pltpu.with_memory_space_constraint(x, pltpu.HBM)
        for x in (estimate, view_data, psf_stack, *constants)
    ]
    results = pl.pallas_call(
        functools.partial(body, nx, ny),
        out_shape=out_shape,
        in_specs=[pl.BlockSpec(memory_space=pltpu.SMEM)]
        + [pl.BlockSpec(memory_space=pltpu.HBM)] * len(kept),
        out_specs=(vmem,) * 6,
        scratch_shapes=[
            pltpu.VMEM(estimate.shape, F32),
            pltpu.VMEM(view_data.shape, F32),
            pltpu.VMEM(psf_stack.shape, F32),
        ]
        + [pltpu.VMEM(c.shape, c.dtype) for c in constants]
        + [
            pltpu.VMEM((32, 32, 128), F32),
            pltpu.VMEM((32, 32, 256), F32),
            pltpu.VMEM((32, 2 * LX, 128), F32),
            pltpu.VMEM((8, ROWS, COLUMNS), F32),
            pltpu.VMEM((2, 2, 8, EDGE, 128), F32),
            pltpu.VMEM((2, 2, LX, 128), F32),
            pltpu.VMEM((2, 2, ROWS, 128), F32),
            pltpu.VMEM((2, 8, 2 * LX, 128), F32),
            pltpu.VMEM((2, 8, 2 * LX, 128), F32),
            pltpu.VMEM((8, 2 * LX, 128), F32),
            pltpu.VMEM((4, 64, 128), F32),
            pltpu.VMEM((2, 32, 128), F32),
            pltpu.VMEM((16, 128), F32),
            pltpu.VMEM((16, 128), F32),
            pltpu.VMEM((2, 8, 128), F32),
            pltpu.VMEM((1, 128), F32),
            pltpu.VMEM((nx * ny, 1, 128), F32),
            pltpu.SemaphoreType.DMA((len(kept),)),
            pltpu.SemaphoreType.DMA((2, 8)),
            pltpu.SemaphoreType.DMA((2, 8)),
            pltpu.SemaphoreType.DMA((2, 8)),
            pltpu.SemaphoreType.DMA((2, 8)),
            pltpu.SemaphoreType.DMA,
            pltpu.SemaphoreType.DMA,
            pltpu.SemaphoreType.DMA,
            pltpu.SemaphoreType.DMA,
            pltpu.SemaphoreType.REGULAR,
            pltpu.SemaphoreType.REGULAR,
        ],
        compiler_params=pltpu.CompilerParams(
            collective_id=0, has_side_effects=True, vmem_limit_bytes=32 << 20
        ),
    )(view_index, *kept)
    return pl.pallas_call(
        hand_over,
        out_shape=out_shape,
        in_specs=[vmem] * 6,
        out_specs=(anywhere,) * 6,
        scratch_shapes=[pltpu.SemaphoreType.DMA((6,))],
        compiler_params=pltpu.CompilerParams(vmem_limit_bytes=4 << 20),
    )(*results)


def solution(mesh):
    spread = P("gz", "gx", "gy")
    return jax.shard_map(
        functools.partial(local, mesh.shape["gx"], mesh.shape["gy"]),
        mesh=mesh,
        in_specs=(spread, spread, P(), P()),
        out_specs=(spread, spread, spread, spread, P(None, "gx", "gy"), P()),
        check_vma=False,
    )
```

```python
import functools

import jax
import jax.numpy as jnp
import numpy as np
from jax import lax
from jax.experimental import pallas as pl
from jax.experimental.pallas import tpu as pltpu
from jax.sharding import PartitionSpec as P

MESH = pl.DeviceIdType.MESH
HALO = 15
EDGE = 16
ROWS, COLUMNS = 64, 128
LX, LY = ROWS + 2 * EDGE, COLUMNS + 2 * EDGE
HALF = LY // 2 + 1
TAPS = 2 * HALO + 1
BF16, F32 = jnp.bfloat16, jnp.float32


def parts_of(table):
    table = np.asarray(table, np.float64)
    high = table.astype(np.float32).astype(BF16)
    low = (table - high.astype(np.float64)).astype(np.float32).astype(BF16)
    return high, low


def stacked(table):
    high, low = parts_of(table)
    return np.concatenate([high, low, high], axis=0)


def beside(table):
    high, low = parts_of(table)
    return np.concatenate([high, high, low], axis=1)


def column_table(positions):
    angle = 2.0 * np.pi / LY * np.outer(positions, np.arange(HALF))
    table = np.zeros((len(positions), 256))
    table[:, :HALF] = np.cos(angle)
    table[:, 128 : 128 + HALF] = -np.sin(angle)
    return table


def row_table(positions):
    angle = 2.0 * np.pi / LX * np.outer(np.arange(LX), positions)
    c, s = np.cos(angle), np.sin(angle)
    return np.block([[c, s], [-s, c]])


def tables():
    inner = column_table(EDGE + np.arange(COLUMNS))
    left = column_table(np.arange(EDGE))
    right = column_table(LY - EDGE + np.arange(EDGE))
    first = stacked(np.concatenate([inner] + [left, right] * 4))
    second = stacked(np.concatenate([inner] + [right, left] * 4))
    inner_rows = beside(row_table(EDGE + np.arange(ROWS)))
    edge_rows = beside(row_table(np.concatenate([np.arange(EDGE), LX - EDGE + np.arange(EDGE)])))
    angle = 2.0 * np.pi / LX * np.outer(EDGE + np.arange(ROWS), np.arange(LX))
    c, s = np.cos(angle), np.sin(angle)
    rows_back = beside(np.block([[c, -s], [s, c]]))
    angle = 2.0 * np.pi / LY * np.outer(np.arange(HALF), EDGE + np.arange(COLUMNS))
    weight = np.where(np.isin(np.arange(HALF), (0, LY // 2)), 1.0, 2.0)[:, None] / (LX * LY)
    back = np.zeros((256, COLUMNS))
    back[:HALF] = weight * np.cos(angle)
    back[128 : 128 + HALF] = -weight * np.sin(angle)
    high, low = parts_of(back)
    columns_back = np.block([[high, low], [high, np.zeros_like(low)]])
    taps = column_table(np.concatenate([np.arange(TAPS) - HALO, [0]]))
    taps[TAPS] = 0.0
    tap_columns = np.concatenate([stacked(taps), np.zeros((32, 256), BF16)], axis=0)
    tap_rows_table = row_table(np.concatenate([np.arange(TAPS) - HALO, [0]]))
    tap_rows_table[:, TAPS] = 0.0
    tap_rows_table[:, 32 + TAPS] = 0.0
    tap_rows = beside(tap_rows_table)
    pools = np.zeros((128, 512), np.float32)
    for level in range(4):
        step = 2 ** (level + 1)
        for column in range(COLUMNS):
            pools[column, 128 * level + column // step] = 1.0 / step
    pools = np.concatenate([pools] * 3, axis=0).astype(BF16)
    return (
        first,
        second,
        inner_rows,
        edge_rows,
        rows_back,
        columns_back,
        tap_columns,
        tap_rows,
        pools,
    )


def two(x):
    high = x.astype(BF16)
    return high, (x - high.astype(F32)).astype(BF16)


def dot(a, b):
    return jnp.dot(a, b, preferred_element_type=F32)


def left_triple(x):
    high, low = two(x)
    return jnp.concatenate([high, high, low], axis=1)


def right_triple(x):
    high, low = two(x)
    return jnp.concatenate([high, low, high], axis=0)


def exact_triple(x):
    high = x.astype(BF16)
    rest = x - high.astype(F32)
    middle = rest.astype(BF16)
    low = (rest - middle.astype(F32)).astype(BF16)
    return jnp.concatenate([high, middle, low], axis=1)


def body(nx, ny, index_ref, *refs):
    inputs, refs = refs[:12], refs[12:]
    updated_ref, one_ref, two_ref, three_ref, four_ref, five_ref = refs[:6]
    held, refs = refs[6:18], refs[18:]
    (
        est_ref,
        view_ref,
        psf_ref,
        first_ref,
        second_ref,
        inner_rows_ref,
        edge_rows_ref,
        rows_back_ref,
        columns_back_ref,
        tap_columns_ref,
        tap_rows_ref,
        pools_ref,
    ) = held
    (
        taps_ref,
        tap_half_ref,
        kernel_ref,
        ratio_ref,
        edge_rows,
        edge_columns,
        packed,
        own_ref,
        other_ref,
        product_ref,
        pool_a,
        pool_b,
        pool_c,
        pool_d,
        plane_ref,
        tile_ref,
        gathered,
        local_sem,
        send_sem,
        recv_sem,
        part_send,
        part_recv,
        swap_send,
        swap_recv,
        all_send,
        all_recv,
        wider_sem,
        widest_sem,
    ) = refs
    gx, gy, gz = lax.axis_index("gx"), lax.axis_index("gy"), lax.axis_index("gz")

    def turned(at, offset, length):
        offset = offset % length
        if offset == 0:
            return at
        return jnp.where(at >= length - offset, at + offset - length, at + offset)

    def device(dx, dy, dz=0):
        return {"gx": turned(gx, dx, nx), "gy": turned(gy, dy, ny), "gz": turned(gz, dz, 2)}

    fetches = [
        pltpu.make_async_copy(source, target, local_sem.at[k])
        for k, (source, target) in enumerate(zip(inputs, held))
    ]
    fetches[0].start()

    peers = [(dx, dy, 0) for dx in (-1, 0, 1) for dy in (-1, 0, 1) if (dx, dy) != (0, 0)]
    peers.append((0, 0, 1))
    count = nx * ny

    def hops(offset):
        dx, dy = offset
        ring = lambda k, n: min(k, n - k)
        return ring(dx % 4, 4) + ring(dx // 4, nx // 4) + ring(dy, ny)

    far = sorted(((dx, dy) for dx in range(nx) for dy in range(ny)), key=hops, reverse=True)[:-1]
    barrier = pltpu.get_barrier_semaphore()
    for peer in peers:
        pl.semaphore_signal(barrier, inc=1, device_id=device(*peer), device_id_type=MESH)
    for k in (2, 9, 10, 3, 4, 5, 6, 7, 8, 1, 11):
        fetches[k].start()

    def spread_word(sem, offsets):
        for dx, dy in offsets:
            pl.semaphore_signal(sem, inc=1, device_id=device(dx, dy), device_id_type=MESH)

    wider = [(dx, dy) for dx in (-2, 0, 2) for dy in (-2, 0, 2) if (dx, dy) != (0, 0)]
    widest = [(-4, 0), (4, 0)]

    def pack(source, turn, group):
        lane = lax.broadcasted_iota(jnp.int32, (ROWS, 128), 1)
        if group == 0:
            to_right = jnp.zeros((ROWS, 128), F32)
            to_left = jnp.zeros((ROWS, 128), F32)
        else:
            to_right, to_left = packed[turn, 0], packed[turn, 1]
        for j in range(4):
            base = 32 * j
            low, high = (base, base + EDGE) if group == 0 else (base + EDGE, base)
            plane = source[4 * group + j]
            shift = (low - (COLUMNS - EDGE)) % 128
            rolled = pltpu.roll(plane, shift, 1) if shift else plane
            to_right = jnp.where((lane >= low) & (lane < low + EDGE), rolled, to_right)
            rolled = pltpu.roll(plane, high, 1) if high else plane
            to_left = jnp.where((lane >= high) & (lane < high + EDGE), rolled, to_left)
        packed[turn, 0] = to_right
        packed[turn, 1] = to_left

    middle, top, bottom = pl.ds(EDGE, ROWS), pl.ds(0, EDGE), pl.ds(EDGE + ROWS, EDGE)
    head, tail = pl.ds(0, EDGE), pl.ds(ROWS - EDGE, EDGE)

    def halo_copies(source, turn):
        def copy(src, dst, at, dx, dy):
            return pltpu.make_async_remote_copy(
                src_ref=src,
                dst_ref=dst,
                send_sem=send_sem.at[turn, at],
                recv_sem=recv_sem.at[turn, at],
                device_id=device(dx, dy),
                device_id_type=MESH,
            )

        right, left = packed.at[turn, 0], packed.at[turn, 1]
        from_left, from_right = edge_columns.at[turn, 0], edge_columns.at[turn, 1]
        along = []
        for group in (0, 1):
            planes = pl.ds(4 * group, 4)
            into = edge_rows.at[turn, 0, planes], edge_rows.at[turn, 1, planes]
            along.append(copy(source.at[planes, tail, :], into[0], 2 * group, 1, 0))
            along.append(copy(source.at[planes, head, :], into[1], 2 * group + 1, -1, 0))
        corners = [
            copy(right.at[tail, :], from_left.at[top, :], 4, 1, 1),
            copy(right.at[head, :], from_left.at[bottom, :], 5, -1, 1),
            copy(left.at[tail, :], from_right.at[top, :], 6, 1, -1),
            copy(left.at[head, :], from_right.at[bottom, :], 7, -1, -1),
        ]
        across = [
            copy(right, from_left.at[middle, :], 8, 0, 1),
            copy(left, from_right.at[middle, :], 9, 0, -1),
        ]
        return along, corners, across

    def clear_columns(turn, rows, height):
        @pl.when(gy == 0)
        def _():
            for at in rows:
                edge_columns[turn, 0, at, :] = jnp.zeros((height, 128), F32)

        @pl.when(gy == ny - 1)
        def _():
            for at in rows:
                edge_columns[turn, 1, at, :] = jnp.zeros((height, 128), F32)

    def clear_rows(turn):
        @pl.when(gx == 0)
        def _():
            edge_rows[turn, 0] = jnp.zeros((8, EDGE, 128), F32)
            for side in (0, 1):
                edge_columns[turn, side, top, :] = jnp.zeros((EDGE, 128), F32)

        @pl.when(gx == nx - 1)
        def _():
            edge_rows[turn, 1] = jnp.zeros((8, EDGE, 128), F32)
            for side in (0, 1):
                edge_columns[turn, side, bottom, :] = jnp.zeros((EDGE, 128), F32)

        clear_columns(turn, (top, bottom), EDGE)

    def partner_copy(turn, z):
        return pltpu.make_async_remote_copy(
            src_ref=own_ref.at[turn, z],
            dst_ref=other_ref.at[turn, z],
            send_sem=part_send.at[turn, z],
            recv_sem=part_recv.at[turn, z],
            device_id=device(0, 0, 1),
            device_id_type=MESH,
        )

    def transform(turn, height, plane_of, left, right, rows_table, adding):
        lane = lax.broadcasted_iota(jnp.int32, (height, 128), 1)
        even = (lane & EDGE) == 0
        for group, table in ((0, first_ref), (1, second_ref)):
            mixed = jnp.where(even, left, right) if group == 0 else jnp.where(even, right, left)
            rows = []
            for j in range(4):
                side = jnp.where((lane >= 32 * j) & (lane < 32 * j + 32), mixed, 0.0)
                rows.append(jnp.concatenate([plane_of(4 * group + j), side], axis=1))
            half = dot(left_triple(jnp.concatenate(rows, axis=0)), table[...])
            for pair in (0, 1):
                a = half[2 * pair * height : (2 * pair + 1) * height]
                b = half[(2 * pair + 1) * height : (2 * pair + 2) * height]
                joint = jnp.concatenate(
                    [
                        jnp.concatenate([a[:, :128], b[:, :128]], axis=1),
                        jnp.concatenate([a[:, 128:], b[:, 128:]], axis=1),
                    ],
                    axis=0,
                )
                full = dot(rows_table[...], right_triple(joint))
                z = 4 * group + 2 * pair
                for b in (0, 1):
                    part = full[:, 128 * b : 128 * b + 128]
                    if adding:
                        own_ref[turn, z + b] = own_ref[turn, z + b] + part
                        partner_copy(turn, z + b).start()
                    else:
                        own_ref[turn, z + b] = part

    def forward_inner(source, turn):
        left, right = edge_columns[turn, 0, middle, :], edge_columns[turn, 1, middle, :]
        transform(turn, ROWS, lambda z: source[z], left, right, inner_rows_ref, False)

    def forward_edge(turn):
        def both(a, b):
            return jnp.concatenate([a, b], axis=0)

        left, right = [
            both(edge_columns[turn, side, top, :], edge_columns[turn, side, bottom, :])
            for side in (0, 1)
        ]

        def plane_of(z):
            return both(edge_rows[turn, 0, z], edge_rows[turn, 1, z])

        transform(turn, 2 * EDGE, plane_of, left, right, edge_rows_ref, True)

    def depth(x_ref, turn, base, mirrored, adding):
        def block(step, carry):
            at = pl.multiple_of(step * 8, 8)
            re, im = pl.ds(at, 8), pl.ds(pl.multiple_of(at + LX, 8), 8)
            xr = [x_ref[turn, z, re, :] for z in range(8)]
            xi = [x_ref[turn, z, im, :] for z in range(8)]
            if adding:
                yr = [product_ref[z, re, :] for z in range(8)]
                yi = [product_ref[z, im, :] for z in range(8)]
            else:
                yr, yi = [None] * 8, [None] * 8
            xs = [r + i for r, i in zip(xr, xi)]
            sums = [[None] * 8 for _ in range(3)]
            for d in range(-7, 8):
                taps = [kernel_ref[base + d, pl.ds(at + LX * k, 8), :] for k in range(3)]
                values = (xs, xi, xr) if mirrored else (xs, xr, xi)
                for out in range(8):
                    z = out + d if mirrored else out - d
                    if not 0 <= z < 8:
                        continue
                    for k in range(3):
                        term = taps[k] * values[k][z]
                        sums[k][out] = term if sums[k][out] is None else sums[k][out] + term
            for z in range(8):
                one, two_, three = (sums[k][z] for k in range(3))
                r = one + two_ if mirrored else one - three
                i = one - three if mirrored else one + two_
                yr[z] = r if yr[z] is None else yr[z] + r
                yi[z] = i if yi[z] is None else yi[z] + i
            for z in range(8):
                product_ref[z, re, :] = yr[z]
                product_ref[z, im, :] = yi[z]
            return carry

        lax.fori_loop(0, LX // 8, block, 0)

    def inverse(group):
        rows = []
        for pair in (0, 1):
            z = 4 * group + 2 * pair
            joint = jnp.concatenate([product_ref[z], product_ref[z + 1]], axis=1)
            half = dot(rows_back_ref[...], right_triple(joint))
            for b in (0, 1):
                lanes = slice(128 * b, 128 * b + 128)
                rows.append(jnp.concatenate([half[:ROWS, lanes], half[ROWS:, lanes]], axis=1))
        full = dot(jnp.concatenate(two(jnp.concatenate(rows, axis=0)), axis=1), columns_back_ref[...])
        return (full[:, :COLUMNS] + full[:, COLUMNS:]).reshape(4, ROWS, COLUMNS)

    def convolve(turn, mirrored):
        depth(own_ref, turn, HALO, mirrored, False)
        for z in range(8):
            partner_copy(turn, z).wait_recv()
        base = HALO + 8 - 16 * gz if mirrored else HALO - 8 + 16 * gz
        depth(other_ref, turn, base, mirrored, True)

    def spectrum():
        for k in (2, 9, 10):
            fetches[k].wait()
        view = index_ref[0]
        taps_ref[...] = jnp.zeros((32, 32, 128), F32)

        taps_ref[0:TAPS, 0:TAPS, 0:TAPS] = psf_ref[view]
        total = jnp.sum(jnp.sum(taps_ref[...], axis=0), axis=(0, 1), keepdims=True)
        scale = 1.0 / total

        for step in range(4):
            x = taps_ref[8 * step : 8 * step + 8].reshape(256, 128) * scale
            high = x.astype(BF16).astype(F32)
            low = x - high
            joint = high + pltpu.roll(high, 32, 1) + pltpu.roll(low, 64, 1)
            half = dot(joint.astype(BF16), tap_columns_ref[...])
            tap_half_ref[8 * step : 8 * step + 8] = half.reshape(8, 32, 256)

        def rows(step, carry):
            for pair in range(4):
                z = 8 * step + 2 * pair
                a, b = tap_half_ref[z], tap_half_ref[z + 1]
                joint = jnp.concatenate(
                    [
                        jnp.concatenate([a[:, :128], b[:, :128]], axis=1),
                        jnp.concatenate([a[:, 128:], b[:, 128:]], axis=1),
                    ],
                    axis=0,
                )
                full = dot(tap_rows_ref[...], right_triple(joint))
                for b in (0, 1):
                    re = full[:LX, 128 * b : 128 * b + 128]
                    im = full[LX:, 128 * b : 128 * b + 128]
                    kernel_ref[z + b, 0:LX] = re
                    kernel_ref[z + b, LX : 2 * LX] = im - re
                    kernel_ref[z + b, 2 * LX :] = im + re
            return carry

        lax.fori_loop(0, 4, rows, 0)

    fetches[0].wait()
    pack(est_ref, 0, 0)
    pack(est_ref, 0, 1)
    pl.semaphore_wait(barrier, len(peers))
    along, corners, across = halo_copies(est_ref, 0)
    for copy in along + corners + across:
        copy.start()
    spectrum()
    for k in (3, 4, 5, 6, 7, 8, 1, 11):
        fetches[k].wait()

    def receive(copies):
        for copy in copies:
            copy.wait_recv()

    receive(across)
    clear_columns(0, (middle,), ROWS)
    forward_inner(est_ref, 0)
    receive(along)
    receive(corners)
    spread_word(wider_sem, wider)
    clear_rows(0)
    forward_edge(0)
    convolve(0, False)
    late_along, late_corners, late_across = halo_copies(ratio_ref, 1)
    for group in (0, 1):
        at = pl.ds(4 * group, 4)
        ratio_ref[at] = view_ref[at] / inverse(group)
        for copy in late_along[2 * group : 2 * group + 2]:
            copy.start()
        pack(ratio_ref, 1, group)
    for copy in late_corners + late_across:
        copy.start()
    pl.semaphore_wait(wider_sem, len(wider))
    spread_word(widest_sem, widest)
    receive(late_across)
    clear_columns(1, (middle,), ROWS)
    forward_inner(ratio_ref, 1)
    receive(late_along)
    receive(late_corners)
    clear_rows(1)
    forward_edge(1)
    convolve(1, True)
    for group in (0, 1):
        at = pl.ds(4 * group, 4)
        updated = est_ref[at] * inverse(group)
        updated_ref[at] = updated
        for pair in (0, 1):
            pool_a[2 * group + pair] = updated[2 * pair] + updated[2 * pair + 1]

    even, odd = pl.ds(0, ROWS // 2, stride=2), pl.ds(1, ROWS // 2, stride=2)
    level_one = [(pool_a[k, even, :] + pool_a[k, odd, :]) * 0.25 for k in range(4)]
    for k in (0, 1):
        pool_b[k] = level_one[2 * k] + level_one[2 * k + 1]
    even, odd = pl.ds(0, ROWS // 4, stride=2), pl.ds(1, ROWS // 4, stride=2)
    level_two = [(pool_b[k, even, :] + pool_b[k, odd, :]) * 0.25 for k in (0, 1)]
    pool_c[...] = level_two[0] + level_two[1]
    even, odd = pl.ds(0, ROWS // 8, stride=2), pl.ds(1, ROWS // 8, stride=2)
    level_three = (pool_c[even, :] + pool_c[odd, :]) * 0.25
    pool_d[0:8] = level_three
    pool_d[8:16] = jnp.zeros((8, 128), F32)
    even, odd = pl.ds(0, 8, stride=2), pl.ds(1, 8, stride=2)
    level_four = (pool_d[even, :] + pool_d[odd, :]) * 0.5
    plane_ref[0] = dot(exact_triple(level_four), pools_ref[:, 384:])
    swap = pltpu.make_async_remote_copy(
        src_ref=plane_ref.at[0],
        dst_ref=plane_ref.at[1],
        send_sem=swap_send,
        recv_sem=swap_recv,
        device_id=device(0, 0, 1),
        device_id_type=MESH,
    )
    swap.start()
    third = dot(exact_triple(level_three), pools_ref[:, 256:384])
    three_ref[0] = third[:, :16]
    second = dot(exact_triple(jnp.concatenate(level_two, axis=0)), pools_ref[:, 128:256])
    for k in (0, 1):
        two_ref[k] = second[16 * k : 16 * k + 16, :32]
    full = dot(exact_triple(jnp.concatenate(level_one, axis=0)), pools_ref[:, :128])
    for k in range(4):
        one_ref[k] = full[32 * k : 32 * k + 32, :64]
    swap.wait_recv()
    fourth = (plane_ref[0] + plane_ref[1]) * 0.5
    four_ref[0] = fourth[:4, :8]
    pool_d[0:8] = fourth
    fifth = pool_d[even, :] + pool_d[odd, :]
    source = lax.broadcasted_iota(jnp.int32, (384, 128), 0) % 128
    target = lax.broadcasted_iota(jnp.int32, (384, 128), 1)
    place = (source < 8) & (target == 4 * gy + source // 2)
    placed = dot(exact_triple(fifth), jnp.where(place, 0.25, 0.0).astype(BF16))
    tile_ref[...] = placed[0:1] + pltpu.roll(placed[1:2], 4 * ny, 1)
    me = gx * ny + gy

    pl.semaphore_wait(widest_sem, len(widest))
    for dx, dy in far:
        pltpu.make_async_remote_copy(
            src_ref=tile_ref,
            dst_ref=gathered.at[me],
            send_sem=all_send,
            recv_sem=all_recv,
            device_id=device(dx, dy),
            device_id_type=MESH,
        ).start()
    gathered[me] = tile_ref[...]
    others = gathered.at[pl.ds(0, count - 1)]
    everyone = pltpu.make_async_remote_copy(
        src_ref=others,
        dst_ref=others,
        send_sem=all_send,
        recv_sem=all_recv,
        device_id=device(0, 1),
        device_id_type=MESH,
    )
    everyone.wait_recv()
    strips = jnp.sum(gathered[...].reshape(nx, ny, 128), axis=1)
    five_ref[0, pl.ds(0, nx, stride=2), :] = strips[:, : 4 * ny]
    five_ref[0, pl.ds(1, nx, stride=2), :] = pltpu.roll(strips, 128 - 4 * ny, 1)[:, : 4 * ny]

    for copy in along + corners + across + late_along + late_corners + late_across:
        copy.wait_send()
    for turn in (0, 1):
        for z in range(8):
            partner_copy(turn, z).wait_send()
    swap.wait_send()
    everyone.wait_send()


def hand_over(*refs):
    sources, targets, sems = refs[:6], refs[6:12], refs[12]
    copies = [pltpu.make_async_copy(a, b, sems.at[k]) for k, (a, b) in enumerate(zip(sources, targets))]
    for copy in copies:
        copy.start()
    for copy in copies:
        copy.wait()


def local(nx, ny, estimate, view_data, psf_stack, view_index):
    vmem = pl.BlockSpec(memory_space=pltpu.VMEM)
    anywhere = pl.BlockSpec(memory_space=pl.ANY)
    shape = jax.ShapeDtypeStruct
    out_shape = (
        shape((8, 64, 128), F32),
        shape((4, 32, 64), F32),
        shape((2, 16, 32), F32),
        shape((1, 8, 16), F32),
        shape((1, 4, 8), F32),
        shape((1, 2 * nx, 4 * ny), F32),
    )
    constants = [jnp.asarray(t) for t in tables()]
    kept = [
        pltpu.with_memory_space_constraint(x, pltpu.HBM)
        for x in (estimate, view_data, psf_stack, *constants)
    ]
    results = pl.pallas_call(
        functools.partial(body, nx, ny),
        out_shape=out_shape,
        in_specs=[pl.BlockSpec(memory_space=pltpu.SMEM)]
        + [pl.BlockSpec(memory_space=pltpu.HBM)] * len(kept),
        out_specs=(vmem,) * 6,
        scratch_shapes=[
            pltpu.VMEM(estimate.shape, F32),
            pltpu.VMEM(view_data.shape, F32),
            pltpu.VMEM(psf_stack.shape, F32),
        ]
        + [pltpu.VMEM(c.shape, c.dtype) for c in constants]
        + [
            pltpu.VMEM((32, 32, 128), F32),
            pltpu.VMEM((32, 32, 256), F32),
            pltpu.VMEM((32, 3 * LX, 128), F32),
            pltpu.VMEM((8, ROWS, COLUMNS), F32),
            pltpu.VMEM((2, 2, 8, EDGE, 128), F32),
            pltpu.VMEM((2, 2, LX, 128), F32),
            pltpu.VMEM((2, 2, ROWS, 128), F32),
            pltpu.VMEM((2, 8, 2 * LX, 128), F32),
            pltpu.VMEM((2, 8, 2 * LX, 128), F32),
            pltpu.VMEM((8, 2 * LX, 128), F32),
            pltpu.VMEM((4, 64, 128), F32),
            pltpu.VMEM((2, 32, 128), F32),
            pltpu.VMEM((16, 128), F32),
            pltpu.VMEM((16, 128), F32),
            pltpu.VMEM((2, 8, 128), F32),
            pltpu.VMEM((1, 128), F32),
            pltpu.VMEM((nx * ny, 1, 128), F32),
            pltpu.SemaphoreType.DMA((len(kept),)),
            pltpu.SemaphoreType.DMA((2, 10)),
            pltpu.SemaphoreType.DMA((2, 10)),
            pltpu.SemaphoreType.DMA((2, 8)),
            pltpu.SemaphoreType.DMA((2, 8)),
            pltpu.SemaphoreType.DMA,
            pltpu.SemaphoreType.DMA,
            pltpu.SemaphoreType.DMA,
            pltpu.SemaphoreType.DMA,
            pltpu.SemaphoreType.REGULAR,
            pltpu.SemaphoreType.REGULAR,
        ],
        compiler_params=pltpu.CompilerParams(
            collective_id=0, has_side_effects=True, vmem_limit_bytes=32 << 20
        ),
    )(view_index, *kept)
    return pl.pallas_call(
        hand_over,
        out_shape=out_shape,
        in_specs=[vmem] * 6,
        out_specs=(anywhere,) * 6,
        scratch_shapes=[pltpu.SemaphoreType.DMA((6,))],
        compiler_params=pltpu.CompilerParams(vmem_limit_bytes=4 << 20),
    )(*results)


def solution(mesh):
    spread = P("gz", "gx", "gy")
    return jax.shard_map(
        functools.partial(local, mesh.shape["gx"], mesh.shape["gy"]),
        mesh=mesh,
        in_specs=(spread, spread, P(), P()),
        out_specs=(spread, spread, spread, spread, P(None, "gx", "gy"), P()),
        check_vma=False,
    )
```

```python
import functools

import jax
import jax.numpy as jnp
import numpy as np
from jax import lax
from jax.experimental import pallas as pl
from jax.experimental.pallas import tpu as pltpu
from jax.sharding import PartitionSpec as P

MESH = pl.DeviceIdType.MESH
HALO = 15
EDGE = 16
ROWS, COLUMNS = 64, 128
LX, LY = ROWS + 2 * EDGE, COLUMNS + 2 * EDGE
HALF = LY // 2 + 1
TAPS = 2 * HALO + 1
BF16, F32 = jnp.bfloat16, jnp.float32


def parts_of(table):
    table = np.asarray(table, np.float64)
    high = table.astype(np.float32).astype(BF16)
    low = (table - high.astype(np.float64)).astype(np.float32).astype(BF16)
    return high, low


def stacked(table):
    high, low = parts_of(table)
    return np.concatenate([high, low, high], axis=0)


def beside(table):
    high, low = parts_of(table)
    return np.concatenate([high, high, low], axis=1)


def column_table(positions):
    angle = 2.0 * np.pi / LY * np.outer(positions, np.arange(HALF))
    table = np.zeros((len(positions), 256))
    table[:, :HALF] = np.cos(angle)
    table[:, 128 : 128 + HALF] = -np.sin(angle)
    return table


def row_table(positions):
    angle = 2.0 * np.pi / LX * np.outer(np.arange(LX), positions)
    c, s = np.cos(angle), np.sin(angle)
    return np.block([[c, s], [-s, c]])


def tables():
    inner = column_table(EDGE + np.arange(COLUMNS))
    left = column_table(np.arange(EDGE))
    right = column_table(LY - EDGE + np.arange(EDGE))
    columns = stacked(np.concatenate([inner] + [left, right] * 4))
    inner_rows = beside(row_table(EDGE + np.arange(ROWS)))
    edge_rows = beside(row_table(np.concatenate([np.arange(EDGE), LX - EDGE + np.arange(EDGE)])))
    angle = 2.0 * np.pi / LX * np.outer(EDGE + np.arange(ROWS), np.arange(LX))
    c, s = np.cos(angle), np.sin(angle)
    rows_back = beside(np.block([[c, -s], [s, c]]))
    angle = 2.0 * np.pi / LY * np.outer(np.arange(HALF), EDGE + np.arange(COLUMNS))
    weight = np.where(np.isin(np.arange(HALF), (0, LY // 2)), 1.0, 2.0)[:, None] / (LX * LY)
    back = np.zeros((256, COLUMNS))
    back[:HALF] = weight * np.cos(angle)
    back[128 : 128 + HALF] = -weight * np.sin(angle)
    high, low = parts_of(back)
    columns_back = np.block([[high, low], [high, np.zeros_like(low)]])
    taps = column_table(np.concatenate([np.arange(TAPS) - HALO, [0]]))
    taps[TAPS] = 0.0
    tap_columns = np.concatenate([stacked(taps), np.zeros((32, 256), BF16)], axis=0)
    tap_rows_table = row_table(np.concatenate([np.arange(TAPS) - HALO, [0]]))
    tap_rows_table[:, TAPS] = 0.0
    tap_rows_table[:, 32 + TAPS] = 0.0
    tap_rows = beside(tap_rows_table)
    pools = np.zeros((128, 512), np.float32)
    for level in range(4):
        step = 2 ** (level + 1)
        for column in range(COLUMNS):
            pools[column, 128 * level + column // step] = 1.0 / step
    pools = np.concatenate([pools] * 3, axis=0).astype(BF16)
    return (
        columns,
        inner_rows,
        edge_rows,
        rows_back,
        columns_back,
        tap_columns,
        tap_rows,
        pools,
    )


def two(x):
    high = x.astype(BF16)
    return high, (x - high.astype(F32)).astype(BF16)


def dot(a, b):
    return jnp.dot(a, b, preferred_element_type=F32)


def left_triple(x):
    high, low = two(x)
    return jnp.concatenate([high, high, low], axis=1)


def right_triple(x):
    high, low = two(x)
    return jnp.concatenate([high, low, high], axis=0)


def exact_triple(x):
    high = x.astype(BF16)
    rest = x - high.astype(F32)
    middle = rest.astype(BF16)
    low = (rest - middle.astype(F32)).astype(BF16)
    return jnp.concatenate([high, middle, low], axis=1)


def body(nx, ny, index_ref, *refs):
    inputs, refs = refs[:11], refs[11:]
    updated_ref, one_ref, two_ref, three_ref, four_ref, five_ref = refs[:6]
    held, refs = refs[6:17], refs[17:]
    (
        est_ref,
        view_ref,
        psf_ref,
        columns_ref,
        inner_rows_ref,
        edge_rows_ref,
        rows_back_ref,
        columns_back_ref,
        tap_columns_ref,
        tap_rows_ref,
        pools_ref,
    ) = held
    (
        taps_ref,
        tap_half_ref,
        kernel_ref,
        ratio_ref,
        edge_rows,
        edge_columns,
        packed,
        own_ref,
        other_ref,
        product_ref,
        pool_a,
        pool_b,
        pool_c,
        pool_d,
        plane_ref,
        tile_ref,
        gathered,
        local_sem,
        send_sem,
        recv_sem,
        part_send,
        part_recv,
        swap_send,
        swap_recv,
        all_send,
        all_recv,
        near_sem,
        wider_sem,
        widest_sem,
    ) = refs
    gx, gy, gz = lax.axis_index("gx"), lax.axis_index("gy"), lax.axis_index("gz")

    def turned(at, offset, length):
        offset = offset % length
        if offset == 0:
            return at
        return jnp.where(at >= length - offset, at + offset - length, at + offset)

    def device(dx, dy, dz=0):
        return {"gx": turned(gx, dx, nx), "gy": turned(gy, dy, ny), "gz": turned(gz, dz, 2)}

    fetches = [
        pltpu.make_async_copy(source, target, local_sem.at[k])
        for k, (source, target) in enumerate(zip(inputs, held))
    ]
    fetches[0].start()

    peers = [(dx, dy, 0) for dx in (-1, 0, 1) for dy in (-1, 0, 1) if (dx, dy) != (0, 0)]
    peers.append((0, 0, 1))
    count = nx * ny

    def hops(offset):
        dx, dy = offset
        ring = lambda k, n: min(k, n - k)
        return ring(dx % 4, 4) + ring(dx // 4, nx // 4) + ring(dy, ny)

    far = sorted(((dx, dy) for dx in range(nx) for dy in range(ny)), key=hops, reverse=True)[:-1]
    barrier = pltpu.get_barrier_semaphore()
    for peer in peers:
        pl.semaphore_signal(barrier, inc=1, device_id=device(*peer), device_id_type=MESH)
    for k in (2, 8, 9, 3, 4, 5, 6, 7, 1, 10):
        fetches[k].start()

    def spread_word(sem, offsets):
        for dx, dy in offsets:
            pl.semaphore_signal(sem, inc=1, device_id=device(dx, dy), device_id_type=MESH)

    wider = [(dx, dy) for dx in (-2, 0, 2) for dy in (-2, 0, 2) if (dx, dy) != (0, 0)]
    widest = [(-4, 0), (4, 0)]
    close = [(dx, dy) for dx, dy, dz in peers if dz == 0]

    def pack(source, turn, group):
        lane = lax.broadcasted_iota(jnp.int32, (ROWS, 128), 1)
        if group == 0:
            to_right = jnp.zeros((ROWS, 128), F32)
            to_left = jnp.zeros((ROWS, 128), F32)
        else:
            to_right, to_left = packed[turn, 0], packed[turn, 1]
        for j in range(4):
            base = 32 * j
            low, high = (base, base + EDGE) if group == 0 else (base + EDGE, base)
            plane = source[4 * group + j]
            shift = (low - (COLUMNS - EDGE)) % 128
            rolled = pltpu.roll(plane, shift, 1) if shift else plane
            to_right = jnp.where((lane >= low) & (lane < low + EDGE), rolled, to_right)
            rolled = pltpu.roll(plane, high, 1) if high else plane
            to_left = jnp.where((lane >= high) & (lane < high + EDGE), rolled, to_left)
        packed[turn, 0] = to_right
        packed[turn, 1] = to_left

    middle, top, bottom = pl.ds(EDGE, ROWS), pl.ds(0, EDGE), pl.ds(EDGE + ROWS, EDGE)
    head, tail = pl.ds(0, EDGE), pl.ds(ROWS - EDGE, EDGE)

    def there(dx, dy):
        tests = []
        if dx:
            tests.append(gx > 0 if dx < 0 else gx < nx - 1)
        if dy:
            tests.append(gy > 0 if dy < 0 else gy < ny - 1)
        return tests[0] if len(tests) == 1 else tests[0] & tests[1]

    def send(copies):
        for copy, ahead, _ in copies:
            pl.when(ahead)(copy.start)

    def receive(copies):
        for copy, _, behind in copies:
            pl.when(behind)(copy.wait_recv)

    def halo_copies(source, turn):
        def copy(src, dst, at, dx, dy):
            sent = pltpu.make_async_remote_copy(
                src_ref=src,
                dst_ref=dst,
                send_sem=send_sem.at[turn, at],
                recv_sem=recv_sem.at[turn, at],
                device_id=device(dx, dy),
                device_id_type=MESH,
            )
            return sent, there(dx, dy), there(-dx, -dy)

        right, left = packed.at[turn, 0], packed.at[turn, 1]
        from_left, from_right = edge_columns.at[turn, 0], edge_columns.at[turn, 1]
        along = []
        for group in (0, 1):
            planes = pl.ds(4 * group, 4)
            into = edge_rows.at[turn, 0, planes], edge_rows.at[turn, 1, planes]
            along.append(copy(source.at[planes, tail, :], into[0], 2 * group, 1, 0))
            along.append(copy(source.at[planes, head, :], into[1], 2 * group + 1, -1, 0))
        corners = [
            copy(right.at[tail, :], from_left.at[top, :], 4, 1, 1),
            copy(right.at[head, :], from_left.at[bottom, :], 5, -1, 1),
            copy(left.at[tail, :], from_right.at[top, :], 6, 1, -1),
            copy(left.at[head, :], from_right.at[bottom, :], 7, -1, -1),
        ]
        across = [
            copy(right, from_left.at[middle, :], 8, 0, 1),
            copy(left, from_right.at[middle, :], 9, 0, -1),
        ]
        return along, corners, across

    def clear_borders():
        rows, columns = jnp.zeros((8, EDGE, 128), F32), jnp.zeros((LX, 128), F32)
        for end, at, part in ((gx == 0, 0, top), (gx == nx - 1, 1, bottom)):

            @pl.when(end)
            def _():
                for turn in (0, 1):
                    edge_rows[turn, at] = rows
                    for side in (0, 1):
                        edge_columns[turn, side, part, :] = columns[:EDGE]

        for end, side in ((gy == 0, 0), (gy == ny - 1, 1)):

            @pl.when(end)
            def _():
                for turn in (0, 1):
                    edge_columns[turn, side] = columns

    def partner_copy(turn, z):
        return pltpu.make_async_remote_copy(
            src_ref=own_ref.at[turn, z],
            dst_ref=other_ref.at[turn, z],
            send_sem=part_send.at[turn, z],
            recv_sem=part_recv.at[turn, z],
            device_id=device(0, 0, 1),
            device_id_type=MESH,
        )

    def transform(turn, height, plane_of, left, right, rows_table, adding):
        lane = lax.broadcasted_iota(jnp.int32, (height, 128), 1)
        even = (lane & EDGE) == 0
        mixed = (
            jnp.where(even, left, right),
            jnp.where(even, pltpu.roll(left, 128 - EDGE, 1), pltpu.roll(right, EDGE, 1)),
        )
        rows = []
        for z in range(8):
            j = 32 * (z % 4)
            side = jnp.where((lane >= j) & (lane < j + 32), mixed[z // 4], 0.0)
            rows.append(jnp.concatenate([plane_of(z), side], axis=1))
        half = dot(left_triple(jnp.concatenate(rows, axis=0)), columns_ref[...])
        for group in (0, 1):
            for pair in (0, 1):
                z = 4 * group + 2 * pair
                a = half[z * height : (z + 1) * height]
                b = half[(z + 1) * height : (z + 2) * height]
                joint = jnp.concatenate(
                    [
                        jnp.concatenate([a[:, :128], b[:, :128]], axis=1),
                        jnp.concatenate([a[:, 128:], b[:, 128:]], axis=1),
                    ],
                    axis=0,
                )
                full = dot(rows_table[...], right_triple(joint))
                for b in (0, 1):
                    part = full[:, 128 * b : 128 * b + 128]
                    if adding:
                        own_ref[turn, z + b] = own_ref[turn, z + b] + part
                        partner_copy(turn, z + b).start()
                    else:
                        own_ref[turn, z + b] = part

    def forward_inner(source, turn):
        left, right = edge_columns[turn, 0, middle, :], edge_columns[turn, 1, middle, :]
        transform(turn, ROWS, lambda z: source[z], left, right, inner_rows_ref, False)

    def forward_edge(turn):
        def both(a, b):
            return jnp.concatenate([a, b], axis=0)

        left, right = [
            both(edge_columns[turn, side, top, :], edge_columns[turn, side, bottom, :])
            for side in (0, 1)
        ]

        def plane_of(z):
            return both(edge_rows[turn, 0, z], edge_rows[turn, 1, z])

        transform(turn, 2 * EDGE, plane_of, left, right, edge_rows_ref, True)

    def depth(x_ref, turn, base, mirrored, adding):
        def blocks(step, carry):
            block(2 * step)
            block(2 * step + 1)
            return carry

        def block(step):
            at = pl.multiple_of(step * 8, 8)
            re, im = pl.ds(at, 8), pl.ds(pl.multiple_of(at + LX, 8), 8)
            xr = [x_ref[turn, z, re, :] for z in range(8)]
            xi = [x_ref[turn, z, im, :] for z in range(8)]
            if adding:
                yr = [product_ref[z, re, :] for z in range(8)]
                yi = [product_ref[z, im, :] for z in range(8)]
            else:
                yr, yi = [None] * 8, [None] * 8
            xs = [r + i for r, i in zip(xr, xi)]
            sums = [[None] * 8 for _ in range(3)]
            for d in range(-7, 8):
                taps = [kernel_ref[base + d, pl.ds(at + LX * k, 8), :] for k in range(3)]
                values = (xs, xi, xr) if mirrored else (xs, xr, xi)
                for out in range(8):
                    z = out + d if mirrored else out - d
                    if not 0 <= z < 8:
                        continue
                    for k in range(3):
                        term = taps[k] * values[k][z]
                        sums[k][out] = term if sums[k][out] is None else sums[k][out] + term
            for z in range(8):
                one, two_, three = (sums[k][z] for k in range(3))
                r = one + two_ if mirrored else one - three
                i = one - three if mirrored else one + two_
                yr[z] = r if yr[z] is None else yr[z] + r
                yi[z] = i if yi[z] is None else yi[z] + i
            for z in range(8):
                product_ref[z, re, :] = yr[z]
                product_ref[z, im, :] = yi[z]

        lax.fori_loop(0, LX // 16, blocks, 0)

    def inverse(planes):
        rows = []
        for z in planes[::2]:
            joint = jnp.concatenate([product_ref[z], product_ref[z + 1]], axis=1)
            half = dot(rows_back_ref[...], right_triple(joint))
            for b in (0, 1):
                lanes = slice(128 * b, 128 * b + 128)
                rows.append(jnp.concatenate([half[:ROWS, lanes], half[ROWS:, lanes]], axis=1))
        full = dot(jnp.concatenate(two(jnp.concatenate(rows, axis=0)), axis=1), columns_back_ref[...])
        return (full[:, :COLUMNS] + full[:, COLUMNS:]).reshape(len(planes), ROWS, COLUMNS)

    def convolve(turn, mirrored):
        depth(own_ref, turn, HALO, mirrored, False)
        for z in range(8):
            partner_copy(turn, z).wait_recv()
        base = HALO + 8 - 16 * gz if mirrored else HALO - 8 + 16 * gz
        depth(other_ref, turn, base, mirrored, True)

    def spectrum():
        for k in (2, 8, 9):
            fetches[k].wait()
        view = index_ref[0]
        taps_ref[...] = jnp.zeros((32, 32, 128), F32)

        taps_ref[0:TAPS, 0:TAPS, 0:TAPS] = psf_ref[view]
        total = jnp.sum(jnp.sum(taps_ref[...], axis=0), axis=(0, 1), keepdims=True)
        scale = 1.0 / total

        for step in range(4):
            x = taps_ref[8 * step : 8 * step + 8].reshape(256, 128) * scale
            high = x.astype(BF16).astype(F32)
            low = x - high
            joint = high + pltpu.roll(high, 32, 1) + pltpu.roll(low, 64, 1)
            half = dot(joint.astype(BF16), tap_columns_ref[...])
            tap_half_ref[8 * step : 8 * step + 8] = half.reshape(8, 32, 256)

        def rows(step, carry):
            for pair in range(4):
                z = 8 * step + 2 * pair
                a, b = tap_half_ref[z], tap_half_ref[z + 1]
                joint = jnp.concatenate(
                    [
                        jnp.concatenate([a[:, :128], b[:, :128]], axis=1),
                        jnp.concatenate([a[:, 128:], b[:, 128:]], axis=1),
                    ],
                    axis=0,
                )
                full = dot(tap_rows_ref[...], right_triple(joint))
                for b in (0, 1):
                    re = full[:LX, 128 * b : 128 * b + 128]
                    im = full[LX:, 128 * b : 128 * b + 128]
                    kernel_ref[z + b, 0:LX] = re
                    kernel_ref[z + b, LX : 2 * LX] = im - re
                    kernel_ref[z + b, 2 * LX :] = im + re
            return carry

        lax.fori_loop(0, 4, rows, 0)

    fetches[0].wait()
    pack(est_ref, 0, 0)
    pack(est_ref, 0, 1)
    pl.semaphore_wait(barrier, len(peers))
    spread_word(near_sem, close)
    along, corners, across = halo_copies(est_ref, 0)
    send(corners + across + along)
    clear_borders()
    spectrum()
    for k in (3, 4, 5, 6, 7, 1, 10):
        fetches[k].wait()
    receive(across)
    forward_inner(est_ref, 0)
    pl.semaphore_wait(near_sem, len(close))
    spread_word(wider_sem, wider)
    receive(along + corners)
    forward_edge(0)
    convolve(0, False)
    late_along, late_corners, late_across = halo_copies(ratio_ref, 1)
    for group in (0, 1):
        at = pl.ds(4 * group, 4)
        ratio_ref[at] = view_ref[at] / inverse(range(4 * group, 4 * group + 4))
        if group == 1:
            pack(ratio_ref, 1, 1)
            send(late_corners + late_across)
        send(late_along[2 * group : 2 * group + 2])
        if group == 0:
            pack(ratio_ref, 1, 0)
    pl.semaphore_wait(wider_sem, len(wider))
    spread_word(widest_sem, widest)
    receive(late_across)
    forward_inner(ratio_ref, 1)
    receive(late_along + late_corners)
    forward_edge(1)
    convolve(1, True)
    correction = inverse(range(8))
    for group in (0, 1):
        at = pl.ds(4 * group, 4)
        updated = est_ref[at] * correction[4 * group : 4 * group + 4]
        updated_ref[at] = updated
        for pair in (0, 1):
            pool_a[2 * group + pair] = updated[2 * pair] + updated[2 * pair + 1]

    even, odd = pl.ds(0, ROWS // 2, stride=2), pl.ds(1, ROWS // 2, stride=2)
    level_one = [(pool_a[k, even, :] + pool_a[k, odd, :]) * 0.25 for k in range(4)]
    for k in (0, 1):
        pool_b[k] = level_one[2 * k] + level_one[2 * k + 1]
    even, odd = pl.ds(0, ROWS // 4, stride=2), pl.ds(1, ROWS // 4, stride=2)
    level_two = [(pool_b[k, even, :] + pool_b[k, odd, :]) * 0.25 for k in (0, 1)]
    pool_c[...] = level_two[0] + level_two[1]
    even, odd = pl.ds(0, ROWS // 8, stride=2), pl.ds(1, ROWS // 8, stride=2)
    level_three = (pool_c[even, :] + pool_c[odd, :]) * 0.25
    pool_d[0:8] = level_three
    pool_d[8:16] = jnp.zeros((8, 128), F32)
    even, odd = pl.ds(0, 8, stride=2), pl.ds(1, 8, stride=2)
    level_four = (pool_d[even, :] + pool_d[odd, :]) * 0.5
    plane_ref[0] = dot(exact_triple(level_four), pools_ref[:, 384:])
    swap = pltpu.make_async_remote_copy(
        src_ref=plane_ref.at[0],
        dst_ref=plane_ref.at[1],
        send_sem=swap_send,
        recv_sem=swap_recv,
        device_id=device(0, 0, 1),
        device_id_type=MESH,
    )
    swap.start()
    third = dot(exact_triple(level_three), pools_ref[:, 256:384])
    three_ref[0] = third[:, :16]
    second = dot(exact_triple(jnp.concatenate(level_two, axis=0)), pools_ref[:, 128:256])
    for k in (0, 1):
        two_ref[k] = second[16 * k : 16 * k + 16, :32]
    full = dot(exact_triple(jnp.concatenate(level_one, axis=0)), pools_ref[:, :128])
    for k in range(4):
        one_ref[k] = full[32 * k : 32 * k + 32, :64]
    swap.wait_recv()
    fourth = (plane_ref[0] + plane_ref[1]) * 0.5
    four_ref[0] = fourth[:4, :8]
    pool_d[0:8] = fourth
    fifth = pool_d[even, :] + pool_d[odd, :]
    source = lax.broadcasted_iota(jnp.int32, (384, 128), 0) % 128
    target = lax.broadcasted_iota(jnp.int32, (384, 128), 1)
    place = (source < 8) & (target == 4 * gy + source // 2)
    placed = dot(exact_triple(fifth), jnp.where(place, 0.25, 0.0).astype(BF16))
    tile_ref[...] = placed[0:1] + pltpu.roll(placed[1:2], 4 * ny, 1)
    me = gx * ny + gy

    pl.semaphore_wait(widest_sem, len(widest))
    for dx, dy in far:
        pltpu.make_async_remote_copy(
            src_ref=tile_ref,
            dst_ref=gathered.at[me],
            send_sem=all_send,
            recv_sem=all_recv,
            device_id=device(dx, dy),
            device_id_type=MESH,
        ).start()
    gathered[me] = tile_ref[...]
    others = gathered.at[pl.ds(0, count - 1)]
    everyone = pltpu.make_async_remote_copy(
        src_ref=others,
        dst_ref=others,
        send_sem=all_send,
        recv_sem=all_recv,
        device_id=device(0, 1),
        device_id_type=MESH,
    )
    everyone.wait_recv()
    strips = jnp.sum(gathered[...].reshape(nx, ny, 128), axis=1)
    five_ref[0, pl.ds(0, nx, stride=2), :] = strips[:, : 4 * ny]
    five_ref[0, pl.ds(1, nx, stride=2), :] = pltpu.roll(strips, 128 - 4 * ny, 1)[:, : 4 * ny]

    for copy, ahead, _ in along + corners + across + late_along + late_corners + late_across:
        pl.when(ahead)(copy.wait_send)
    for turn in (0, 1):
        for z in range(8):
            partner_copy(turn, z).wait_send()
    swap.wait_send()
    everyone.wait_send()


def hand_over(*refs):
    sources, targets, sems = refs[:6], refs[6:12], refs[12]
    copies = [pltpu.make_async_copy(a, b, sems.at[k]) for k, (a, b) in enumerate(zip(sources, targets))]
    for copy in copies:
        copy.start()
    for copy in copies:
        copy.wait()


def local(nx, ny, estimate, view_data, psf_stack, view_index):
    vmem = pl.BlockSpec(memory_space=pltpu.VMEM)
    anywhere = pl.BlockSpec(memory_space=pl.ANY)
    shape = jax.ShapeDtypeStruct
    out_shape = (
        shape((8, 64, 128), F32),
        shape((4, 32, 64), F32),
        shape((2, 16, 32), F32),
        shape((1, 8, 16), F32),
        shape((1, 4, 8), F32),
        shape((1, 2 * nx, 4 * ny), F32),
    )
    constants = [jnp.asarray(t) for t in tables()]
    kept = [
        pltpu.with_memory_space_constraint(x, pltpu.HBM)
        for x in (estimate, view_data, psf_stack, *constants)
    ]
    results = pl.pallas_call(
        functools.partial(body, nx, ny),
        out_shape=out_shape,
        in_specs=[pl.BlockSpec(memory_space=pltpu.SMEM)]
        + [pl.BlockSpec(memory_space=pltpu.HBM)] * len(kept),
        out_specs=(vmem,) * 6,
        scratch_shapes=[
            pltpu.VMEM(estimate.shape, F32),
            pltpu.VMEM(view_data.shape, F32),
            pltpu.VMEM(psf_stack.shape, F32),
        ]
        + [pltpu.VMEM(c.shape, c.dtype) for c in constants]
        + [
            pltpu.VMEM((32, 32, 128), F32),
            pltpu.VMEM((32, 32, 256), F32),
            pltpu.VMEM((32, 3 * LX, 128), F32),
            pltpu.VMEM((8, ROWS, COLUMNS), F32),
            pltpu.VMEM((2, 2, 8, EDGE, 128), F32),
            pltpu.VMEM((2, 2, LX, 128), F32),
            pltpu.VMEM((2, 2, ROWS, 128), F32),
            pltpu.VMEM((2, 8, 2 * LX, 128), F32),
            pltpu.VMEM((2, 8, 2 * LX, 128), F32),
            pltpu.VMEM((8, 2 * LX, 128), F32),
            pltpu.VMEM((4, 64, 128), F32),
            pltpu.VMEM((2, 32, 128), F32),
            pltpu.VMEM((16, 128), F32),
            pltpu.VMEM((16, 128), F32),
            pltpu.VMEM((2, 8, 128), F32),
            pltpu.VMEM((1, 128), F32),
            pltpu.VMEM((nx * ny, 1, 128), F32),
            pltpu.SemaphoreType.DMA((len(kept),)),
            pltpu.SemaphoreType.DMA((2, 10)),
            pltpu.SemaphoreType.DMA((2, 10)),
            pltpu.SemaphoreType.DMA((2, 8)),
            pltpu.SemaphoreType.DMA((2, 8)),
            pltpu.SemaphoreType.DMA,
            pltpu.SemaphoreType.DMA,
            pltpu.SemaphoreType.DMA,
            pltpu.SemaphoreType.DMA,
            pltpu.SemaphoreType.REGULAR,
            pltpu.SemaphoreType.REGULAR,
            pltpu.SemaphoreType.REGULAR,
        ],
        compiler_params=pltpu.CompilerParams(
            collective_id=0, has_side_effects=True, vmem_limit_bytes=32 << 20
        ),
    )(view_index, *kept)
    return pl.pallas_call(
        hand_over,
        out_shape=out_shape,
        in_specs=[vmem] * 6,
        out_specs=(anywhere,) * 6,
        scratch_shapes=[pltpu.SemaphoreType.DMA((6,))],
        compiler_params=pltpu.CompilerParams(vmem_limit_bytes=4 << 20),
    )(*results)


def solution(mesh):
    spread = P("gz", "gx", "gy")
    return jax.shard_map(
        functools.partial(local, mesh.shape["gx"], mesh.shape["gy"]),
        mesh=mesh,
        in_specs=(spread, spread, P(), P()),
        out_specs=(spread, spread, spread, spread, P(None, "gx", "gy"), P()),
        check_vma=False,
    )
```

```python
import functools

import jax
import jax.numpy as jnp
import numpy as np
from jax import lax
from jax.experimental import pallas as pl
from jax.experimental.pallas import tpu as pltpu
from jax.sharding import PartitionSpec as P

MESH = pl.DeviceIdType.MESH
HALO = 15
EDGE = 16
ROWS, COLUMNS = 64, 128
LX, LY = ROWS + 2 * EDGE, COLUMNS + 2 * EDGE
HALF = LY // 2 + 1
TAPS = 2 * HALO + 1
BF16, F32 = jnp.bfloat16, jnp.float32


def parts_of(table):
    table = np.asarray(table, np.float64)
    high = table.astype(np.float32).astype(BF16)
    low = (table - high.astype(np.float64)).astype(np.float32).astype(BF16)
    return high, low


def stacked(table):
    high, low = parts_of(table)
    return np.concatenate([high, low, high], axis=0)


def beside(table):
    high, low = parts_of(table)
    return np.concatenate([high, high, low], axis=1)


def column_table(positions):
    angle = 2.0 * np.pi / LY * np.outer(positions, np.arange(HALF))
    table = np.zeros((len(positions), 256))
    table[:, :HALF] = np.cos(angle)
    table[:, 128 : 128 + HALF] = -np.sin(angle)
    return table


def row_table(positions):
    angle = 2.0 * np.pi / LX * np.outer(np.arange(LX), positions)
    c, s = np.cos(angle), np.sin(angle)
    return np.block([[c, s], [-s, c]])


def tables():
    inner = column_table(EDGE + np.arange(COLUMNS))
    left = column_table(np.arange(EDGE))
    right = column_table(LY - EDGE + np.arange(EDGE))
    columns = stacked(np.concatenate([inner] + [left, right] * 4))
    inner_rows = beside(row_table(EDGE + np.arange(ROWS)))
    edge_rows = beside(row_table(np.concatenate([np.arange(EDGE), LX - EDGE + np.arange(EDGE)])))
    angle = 2.0 * np.pi / LX * np.outer(EDGE + np.arange(ROWS), np.arange(LX))
    c, s = np.cos(angle), np.sin(angle)
    rows_back = beside(np.block([[c, -s], [s, c]]))
    angle = 2.0 * np.pi / LY * np.outer(np.arange(HALF), EDGE + np.arange(COLUMNS))
    weight = np.where(np.isin(np.arange(HALF), (0, LY // 2)), 1.0, 2.0)[:, None] / (LX * LY)
    back = np.zeros((256, COLUMNS))
    back[:HALF] = weight * np.cos(angle)
    back[128 : 128 + HALF] = -weight * np.sin(angle)
    high, low = parts_of(back)
    columns_back = np.block([[high, low], [high, np.zeros_like(low)]])
    taps = column_table(np.concatenate([np.arange(TAPS) - HALO, [0]]))
    taps[TAPS] = 0.0
    tap_columns = np.concatenate([stacked(taps), np.zeros((32, 256), BF16)], axis=0)
    tap_rows_table = row_table(np.concatenate([np.arange(TAPS) - HALO, [0]]))
    tap_rows_table[:, TAPS] = 0.0
    tap_rows_table[:, 32 + TAPS] = 0.0
    tap_rows = beside(tap_rows_table)
    pools = np.zeros((128, 512), np.float32)
    for level in range(4):
        step = 2 ** (level + 1)
        for column in range(COLUMNS):
            pools[column, 128 * level + column // step] = 1.0 / step
    pools = np.concatenate([pools] * 3, axis=0).astype(BF16)
    tall = np.concatenate([columns, columns_back, tap_columns, pools[:, :256], pools[:, 256:]])
    wide = np.zeros((2 * LX, 1536), BF16)
    wide[:, :384] = inner_rows
    wide[:, 384:576] = edge_rows
    wide[:, 640:832] = tap_rows
    wide[: 2 * ROWS, 896:1472] = rows_back
    return tall, wide


def two(x):
    high = x.astype(BF16)
    return high, (x - high.astype(F32)).astype(BF16)


def dot(a, b):
    return jnp.dot(a, b, preferred_element_type=F32)


def left_triple(x):
    high, low = two(x)
    return jnp.concatenate([high, high, low], axis=1)


def right_triple(x):
    high, low = two(x)
    return jnp.concatenate([high, low, high], axis=0)


def exact_triple(x):
    high = x.astype(BF16)
    rest = x - high.astype(F32)
    middle = rest.astype(BF16)
    low = (rest - middle.astype(F32)).astype(BF16)
    return jnp.concatenate([high, middle, low], axis=1)


def body(nx, ny, index_ref, *refs):
    inputs, refs = refs[:5], refs[5:]
    updated_ref, one_ref, two_ref, three_ref, four_ref, five_ref = refs[:6]
    held, refs = refs[6:11], refs[11:]
    est_ref, view_ref, psf_ref, tall_ref, wide_ref = held
    (
        taps_ref,
        tap_half_ref,
        kernel_ref,
        ratio_ref,
        edge_rows,
        edge_columns,
        packed,
        own_ref,
        other_ref,
        product_ref,
        pool_a,
        pool_b,
        pool_c,
        pool_d,
        plane_ref,
        tile_ref,
        gathered,
        local_sem,
        send_sem,
        recv_sem,
        part_send,
        part_recv,
        swap_send,
        swap_recv,
        all_send,
        all_recv,
        word_sem,
        pair_sem,
    ) = refs
    gx, gy, gz = lax.axis_index("gx"), lax.axis_index("gy"), lax.axis_index("gz")

    def turned(at, offset, length):
        offset = offset % length
        if offset == 0:
            return at
        return jnp.where(at >= length - offset, at + offset - length, at + offset)

    def device(dx, dy, dz=0):
        return {"gx": turned(gx, dx, nx), "gy": turned(gy, dy, ny), "gz": turned(gz, dz, 2)}

    fetches = [
        pltpu.make_async_copy(source, target, local_sem.at[k])
        for k, (source, target) in enumerate(zip(inputs, held))
    ]
    fetches[0].start()

    count = nx * ny

    def there(dx, dy):
        tests = []
        if dx:
            tests.append(gx >= -dx if dx < 0 else gx < nx - dx)
        if dy:
            tests.append(gy >= -dy if dy < 0 else gy < ny - dy)
        return tests[0] if len(tests) == 1 else tests[0] & tests[1]

    def box(reach):
        steps = (-reach, 0, reach)
        return [(dx, dy) for dx in steps for dy in steps if (dx, dy) != (0, 0)]

    def hops(offset):
        dx, dy, dz = offset
        ring = lambda k, n: min(k, n - k)
        return ring(dx % 4, 4) + ring(dx // 4, nx // 4) + ring(dy, ny) + 0.5 * dz

    every = ((dx, dy, dz) for dx in range(nx) for dy in range(ny) for dz in (0, 1))
    far = sorted(every, key=hops, reverse=True)[:-1]

    def signal_all(sem, offsets):
        for dx, dy in offsets:

            @pl.when(there(dx, dy))
            def _():
                pl.semaphore_signal(sem, inc=1, device_id=device(dx, dy), device_id_type=MESH)

    def number(offsets):
        return sum(jnp.where(there(dx, dy), 1, 0) for dx, dy in offsets)

    rounds = [box(1), box(2), box(4), [(-8, 0), (8, 0)]]

    def spread_word(k):
        signal_all(word_sem.at[k], rounds[k])

    def hear_word(k):
        pl.semaphore_wait(word_sem.at[k], number(rounds[k]))

    barrier = pltpu.get_barrier_semaphore()
    pl.semaphore_signal(barrier, inc=1, device_id=device(0, 0, 1), device_id_type=MESH)
    signal_all(barrier, box(1))
    for k in (4, 3, 2, 1):
        fetches[k].start()

    def pack(source, turn, group):
        lane = lax.broadcasted_iota(jnp.int32, (ROWS, 128), 1)
        if group == 0:
            to_right = jnp.zeros((ROWS, 128), F32)
            to_left = jnp.zeros((ROWS, 128), F32)
        else:
            to_right, to_left = packed[turn, 0], packed[turn, 1]
        for j in range(4):
            base = 32 * j
            low, high = (base, base + EDGE) if group == 0 else (base + EDGE, base)
            plane = source[4 * group + j]
            shift = (low - (COLUMNS - EDGE)) % 128
            rolled = pltpu.roll(plane, shift, 1) if shift else plane
            to_right = jnp.where((lane >= low) & (lane < low + EDGE), rolled, to_right)
            rolled = pltpu.roll(plane, high, 1) if high else plane
            to_left = jnp.where((lane >= high) & (lane < high + EDGE), rolled, to_left)
        packed[turn, 0] = to_right
        packed[turn, 1] = to_left

    middle, top, bottom = pl.ds(EDGE, ROWS), pl.ds(0, EDGE), pl.ds(EDGE + ROWS, EDGE)
    head, tail = pl.ds(0, EDGE), pl.ds(ROWS - EDGE, EDGE)

    def send(copies):
        for copy, ahead in copies:
            pl.when(ahead)(copy.start)

    def wait_units(sem, units, send):
        for last_x in (True, False):
            for last_y in (True, False):
                end_x = (gx == 0) | (gx == nx - 1)
                end_y = (gy == 0) | (gy == ny - 1)
                here = (end_x if last_x else ~end_x) & (end_y if last_y else ~end_y)
                total = units(1 if last_x else 2, 1 if last_y else 2)
                slab = kernel_ref.at[pl.ds(0, 2), pl.ds(0, total * EDGE // 2)]
                copy = pltpu.make_async_remote_copy(
                    src_ref=slab,
                    dst_ref=slab,
                    send_sem=sem,
                    recv_sem=sem,
                    device_id=device(0, 0, 1),
                    device_id_type=MESH,
                )
                pl.when(here)(copy.wait_send if send else copy.wait_recv)

    def receive_strips(turn):
        wait_units(recv_sem.at[turn, 1], lambda sx, sy: 4 * sy, False)

    def receive_edges(turn):
        wait_units(recv_sem.at[turn, 0], lambda sx, sy: sx * (8 + sy), False)

    def finish_sends(turn):
        wait_units(send_sem.at[turn], lambda sx, sy: 4 * sy + sx * (8 + sy), True)

    def halo_copies(source, turn):
        def copy(src, dst, at, dx, dy):
            sent = pltpu.make_async_remote_copy(
                src_ref=src,
                dst_ref=dst,
                send_sem=send_sem.at[turn],
                recv_sem=recv_sem.at[turn, at],
                device_id=device(dx, dy),
                device_id_type=MESH,
            )
            return sent, there(dx, dy)

        right, left = packed.at[turn, 0], packed.at[turn, 1]
        from_left, from_right = edge_columns.at[turn, 0], edge_columns.at[turn, 1]
        along = []
        for group in (0, 1):
            planes = pl.ds(4 * group, 4)
            into = edge_rows.at[turn, 0, planes], edge_rows.at[turn, 1, planes]
            along.append(copy(source.at[planes, tail, :], into[0], 0, 1, 0))
            along.append(copy(source.at[planes, head, :], into[1], 0, -1, 0))
        corners = [
            copy(right.at[tail, :], from_left.at[top, :], 0, 1, 1),
            copy(right.at[head, :], from_left.at[bottom, :], 0, -1, 1),
            copy(left.at[tail, :], from_right.at[top, :], 0, 1, -1),
            copy(left.at[head, :], from_right.at[bottom, :], 0, -1, -1),
        ]
        across = [
            copy(right, from_left.at[middle, :], 1, 0, 1),
            copy(left, from_right.at[middle, :], 1, 0, -1),
        ]
        return along, corners, across

    def clear_borders():
        rows, columns = jnp.zeros((8, EDGE, 128), F32), jnp.zeros((LX, 128), F32)
        for end, at, part in ((gx == 0, 0, top), (gx == nx - 1, 1, bottom)):

            @pl.when(end)
            def _():
                for turn in (0, 1):
                    edge_rows[turn, at] = rows
                    for side in (0, 1):
                        edge_columns[turn, side, part, :] = columns[:EDGE]

        for end, side in ((gy == 0, 0), (gy == ny - 1, 1)):

            @pl.when(end)
            def _():
                for turn in (0, 1):
                    edge_columns[turn, side] = columns

    def partner_copy(turn, z):
        return pltpu.make_async_remote_copy(
            src_ref=own_ref.at[turn, z],
            dst_ref=other_ref.at[turn, z],
            send_sem=part_send,
            recv_sem=part_recv.at[turn],
            device_id=device(0, 0, 1),
            device_id_type=MESH,
        )

    def transform(turn, height, plane_of, left, right, rows_table, adding):
        lane = lax.broadcasted_iota(jnp.int32, (height, 128), 1)
        even = (lane & EDGE) == 0
        mixed = (
            jnp.where(even, left, right),
            jnp.where(even, pltpu.roll(left, 128 - EDGE, 1), pltpu.roll(right, EDGE, 1)),
        )
        rows = []
        for z in range(8):
            j = 32 * (z % 4)
            side = jnp.where((lane >= j) & (lane < j + 32), mixed[z // 4], 0.0)
            rows.append(jnp.concatenate([plane_of(z), side], axis=1))
        half = dot(left_triple(jnp.concatenate(rows, axis=0)), tall_ref[0:768, :])
        for group in (0, 1):
            for pair in (0, 1):
                z = 4 * group + 2 * pair
                a = half[z * height : (z + 1) * height]
                b = half[(z + 1) * height : (z + 2) * height]
                joint = jnp.concatenate(
                    [
                        jnp.concatenate([a[:, :128], b[:, :128]], axis=1),
                        jnp.concatenate([a[:, 128:], b[:, 128:]], axis=1),
                    ],
                    axis=0,
                )
                full = dot(wide_ref[:, rows_table], right_triple(joint))
                for b in (0, 1):
                    part = full[:, 128 * b : 128 * b + 128]
                    if adding:
                        own_ref[turn, z + b] = own_ref[turn, z + b] + part
                        partner_copy(turn, z + b).start()
                    else:
                        own_ref[turn, z + b] = part

    def forward_inner(source, turn):
        left, right = edge_columns[turn, 0, middle, :], edge_columns[turn, 1, middle, :]
        transform(turn, ROWS, lambda z: source[z], left, right, slice(0, 384), False)

    def forward_edge(turn):
        def both(a, b):
            return jnp.concatenate([a, b], axis=0)

        left, right = [
            both(edge_columns[turn, side, top, :], edge_columns[turn, side, bottom, :])
            for side in (0, 1)
        ]

        def plane_of(z):
            return both(edge_rows[turn, 0, z], edge_rows[turn, 1, z])

        transform(turn, 2 * EDGE, plane_of, left, right, slice(384, 576), True)

    def depth(x_ref, turn, base, mirrored, adding):
        def blocks(step, carry):
            block(2 * step)
            block(2 * step + 1)
            return carry

        def block(step):
            at = pl.multiple_of(step * 8, 8)
            re, im = pl.ds(at, 8), pl.ds(pl.multiple_of(at + LX, 8), 8)
            xr = [x_ref[turn, z, re, :] for z in range(8)]
            xi = [x_ref[turn, z, im, :] for z in range(8)]
            if adding:
                yr = [product_ref[z, re, :] for z in range(8)]
                yi = [product_ref[z, im, :] for z in range(8)]
            else:
                yr, yi = [None] * 8, [None] * 8
            xs = [r + i for r, i in zip(xr, xi)]
            sums = [[None] * 8 for _ in range(3)]
            for d in range(-7, 8):
                taps = [kernel_ref[base + d, pl.ds(at + LX * k, 8), :] for k in range(3)]
                values = (xs, xi, xr) if mirrored else (xs, xr, xi)
                for out in range(8):
                    z = out + d if mirrored else out - d
                    if not 0 <= z < 8:
                        continue
                    for k in range(3):
                        term = taps[k] * values[k][z]
                        sums[k][out] = term if sums[k][out] is None else sums[k][out] + term
            for z in range(8):
                one, two_, three = (sums[k][z] for k in range(3))
                r = one + two_ if mirrored else one - three
                i = one - three if mirrored else one + two_
                yr[z] = r if yr[z] is None else yr[z] + r
                yi[z] = i if yi[z] is None else yi[z] + i
            for z in range(8):
                product_ref[z, re, :] = yr[z]
                product_ref[z, im, :] = yi[z]

        lax.fori_loop(0, LX // 16, blocks, 0)

    def inverse(planes):
        rows = []
        for z in planes[::2]:
            joint = jnp.concatenate([product_ref[z], product_ref[z + 1]], axis=1)
            half = dot(wide_ref[0:128, 896:1472], right_triple(joint))
            for b in (0, 1):
                lanes = slice(128 * b, 128 * b + 128)
                rows.append(jnp.concatenate([half[:ROWS, lanes], half[ROWS:, lanes]], axis=1))
        full = dot(jnp.concatenate(two(jnp.concatenate(rows, axis=0)), axis=1), tall_ref[768:1280, :])
        return (full[:, :COLUMNS] + full[:, COLUMNS:]).reshape(len(planes), ROWS, COLUMNS)

    def convolve(turn, mirrored, between):
        depth(own_ref, turn, HALO, mirrored, False)
        between()
        planes = other_ref.at[turn]
        pltpu.make_async_remote_copy(
            src_ref=planes,
            dst_ref=planes,
            send_sem=part_send,
            recv_sem=part_recv.at[turn],
            device_id=device(0, 0, 1),
            device_id_type=MESH,
        ).wait_recv()
        base = HALO + 8 - 16 * gz if mirrored else HALO - 8 + 16 * gz
        depth(other_ref, turn, base, mirrored, True)

    def spectrum():
        for k in (4, 3, 2):
            fetches[k].wait()
        view = index_ref[0]
        taps_ref[...] = jnp.zeros((32, 32, 128), F32)

        taps_ref[0:TAPS, 0:TAPS, 0:TAPS] = psf_ref[view]
        total = jnp.sum(jnp.sum(taps_ref[...], axis=0), axis=(0, 1), keepdims=True)
        scale = 1.0 / total

        for step in range(4):
            x = taps_ref[8 * step : 8 * step + 8].reshape(256, 128) * scale
            high = x.astype(BF16).astype(F32)
            low = x - high
            joint = high + pltpu.roll(high, 32, 1) + pltpu.roll(low, 64, 1)
            half = dot(joint.astype(BF16), tall_ref[1280:1408, :])
            tap_half_ref[8 * step : 8 * step + 8] = half.reshape(8, 32, 256)

        def rows(step, carry):
            for pair in range(4):
                z = 8 * step + 2 * pair
                a, b = tap_half_ref[z], tap_half_ref[z + 1]
                joint = jnp.concatenate(
                    [
                        jnp.concatenate([a[:, :128], b[:, :128]], axis=1),
                        jnp.concatenate([a[:, 128:], b[:, 128:]], axis=1),
                    ],
                    axis=0,
                )
                full = dot(wide_ref[:, 640:832], right_triple(joint))
                for b in (0, 1):
                    re = full[:LX, 128 * b : 128 * b + 128]
                    im = full[LX:, 128 * b : 128 * b + 128]
                    kernel_ref[z + b, 0:LX] = re
                    kernel_ref[z + b, LX : 2 * LX] = im - re
                    kernel_ref[z + b, 2 * LX :] = im + re
            return carry

        lax.fori_loop(0, 4, rows, 0)

    fetches[0].wait()
    pack(est_ref, 0, 0)
    pack(est_ref, 0, 1)
    pl.semaphore_wait(barrier, 1 + number(box(1)))
    spread_word(0)
    along, corners, across = halo_copies(est_ref, 0)
    send(corners + across + along)
    clear_borders()
    spectrum()
    fetches[1].wait()
    receive_strips(0)
    forward_inner(est_ref, 0)
    receive_edges(0)
    forward_edge(0)
    hear_word(0)
    spread_word(1)
    convolve(0, False, lambda: None)
    late_along, late_corners, late_across = halo_copies(ratio_ref, 1)
    for group in (0, 1):
        at = pl.ds(4 * group, 4)
        ratio_ref[at] = view_ref[at] / inverse(range(4 * group, 4 * group + 4))
        if group == 1:
            pack(ratio_ref, 1, 1)
            send(late_corners + late_across)
        send(late_along[2 * group : 2 * group + 2])
        if group == 0:
            pack(ratio_ref, 1, 0)
    hear_word(1)
    spread_word(2)
    receive_strips(1)
    forward_inner(ratio_ref, 1)
    receive_edges(1)
    forward_edge(1)
    hear_word(2)
    spread_word(3)

    def tell_partner():
        hear_word(3)
        pl.semaphore_signal(pair_sem, inc=1, device_id=device(0, 0, 1), device_id_type=MESH)

    convolve(1, True, tell_partner)
    updated = est_ref[...] * inverse(range(8))
    column_sums = jnp.sum(updated, axis=0)
    halves = [jnp.sum(column_sums[32 * i : 32 * i + 32], axis=0, keepdims=True) for i in (0, 1)]
    source = lax.broadcasted_iota(jnp.int32, (384, 128), 0) % 128
    target = lax.broadcasted_iota(jnp.int32, (384, 128), 1)
    place = jnp.where(target == 4 * gy + source // 32, 2.0**-14, 0.0).astype(BF16)
    eight = jnp.concatenate(halves + [jnp.zeros((6, 128), F32)], axis=0)
    placed = dot(exact_triple(eight), place)
    tile_ref[...] = placed[0:1] + pltpu.roll(placed[1:2], 4 * ny, 1)
    me = gz * count + gx * ny + gy
    pl.semaphore_wait(pair_sem, 1)
    for dx, dy, dz in far:
        pltpu.make_async_remote_copy(
            src_ref=tile_ref,
            dst_ref=gathered.at[me],
            send_sem=all_send,
            recv_sem=all_recv,
            device_id=device(dx, dy, dz),
            device_id_type=MESH,
        ).start()
    gathered[me] = tile_ref[...]

    updated_ref[...] = updated
    for k in range(4):
        pool_a[k] = updated[2 * k] + updated[2 * k + 1]
    even, odd = pl.ds(0, ROWS // 2, stride=2), pl.ds(1, ROWS // 2, stride=2)
    level_one = [(pool_a[k, even, :] + pool_a[k, odd, :]) * 0.25 for k in range(4)]
    for k in (0, 1):
        pool_b[k] = level_one[2 * k] + level_one[2 * k + 1]
    even, odd = pl.ds(0, ROWS // 4, stride=2), pl.ds(1, ROWS // 4, stride=2)
    level_two = [(pool_b[k, even, :] + pool_b[k, odd, :]) * 0.25 for k in (0, 1)]
    pool_c[...] = level_two[0] + level_two[1]
    even, odd = pl.ds(0, ROWS // 8, stride=2), pl.ds(1, ROWS // 8, stride=2)
    level_three = (pool_c[even, :] + pool_c[odd, :]) * 0.25
    pool_d[0:8] = level_three
    pool_d[8:16] = jnp.zeros((8, 128), F32)
    even, odd = pl.ds(0, 8, stride=2), pl.ds(1, 8, stride=2)
    level_four = (pool_d[even, :] + pool_d[odd, :]) * 0.5
    plane_ref[0] = dot(exact_triple(level_four), tall_ref[1792:2176, 128:256])
    swap = pltpu.make_async_remote_copy(
        src_ref=plane_ref.at[0],
        dst_ref=plane_ref.at[1],
        send_sem=swap_send,
        recv_sem=swap_recv,
        device_id=device(0, 0, 1),
        device_id_type=MESH,
    )
    swap.start()
    third = dot(exact_triple(level_three), tall_ref[1792:2176, 0:128])
    three_ref[0] = third[:, :16]
    second = dot(exact_triple(jnp.concatenate(level_two, axis=0)), tall_ref[1408:1792, 128:256])
    for k in (0, 1):
        two_ref[k] = second[16 * k : 16 * k + 16, :32]
    full = dot(exact_triple(jnp.concatenate(level_one, axis=0)), tall_ref[1408:1792, 0:128])
    for k in range(4):
        one_ref[k] = full[32 * k : 32 * k + 32, :64]
    swap.wait_recv()
    fourth = (plane_ref[0] + plane_ref[1]) * 0.5
    four_ref[0] = fourth[:4, :8]

    finish_sends(0)
    finish_sends(1)
    swap.wait_send()
    pltpu.make_async_remote_copy(
        src_ref=own_ref,
        dst_ref=own_ref,
        send_sem=part_send,
        recv_sem=part_send,
        device_id=device(0, 0, 1),
        device_id_type=MESH,
    ).wait_send()
    others = gathered.at[pl.ds(0, 2 * count - 1)]
    everyone = pltpu.make_async_remote_copy(
        src_ref=others,
        dst_ref=others,
        send_sem=all_send,
        recv_sem=all_recv,
        device_id=device(0, 0, 1),
        device_id_type=MESH,
    )
    everyone.wait_send()
    everyone.wait_recv()
    strips = jnp.sum(gathered[...].reshape(2, nx, ny, 128), axis=(0, 2))
    five_ref[0, pl.ds(0, nx, stride=2), :] = strips[:, : 4 * ny]
    five_ref[0, pl.ds(1, nx, stride=2), :] = pltpu.roll(strips, 128 - 4 * ny, 1)[:, : 4 * ny]


def hand_over(*refs):
    sources, targets, sems = refs[:6], refs[6:12], refs[12]
    copies = [pltpu.make_async_copy(a, b, sems.at[k]) for k, (a, b) in enumerate(zip(sources, targets))]
    for copy in copies:
        copy.start()
    for copy in copies:
        copy.wait()


def local(nx, ny, estimate, view_data, psf_stack, view_index):
    vmem = pl.BlockSpec(memory_space=pltpu.VMEM)
    anywhere = pl.BlockSpec(memory_space=pl.ANY)
    shape = jax.ShapeDtypeStruct
    out_shape = (
        shape((8, 64, 128), F32),
        shape((4, 32, 64), F32),
        shape((2, 16, 32), F32),
        shape((1, 8, 16), F32),
        shape((1, 4, 8), F32),
        shape((1, 2 * nx, 4 * ny), F32),
    )
    constants = [jnp.asarray(t) for t in tables()]
    kept = [
        pltpu.with_memory_space_constraint(x, pltpu.HBM)
        for x in (estimate, view_data, psf_stack, *constants)
    ]
    results = pl.pallas_call(
        functools.partial(body, nx, ny),
        out_shape=out_shape,
        in_specs=[pl.BlockSpec(memory_space=pltpu.SMEM)]
        + [pl.BlockSpec(memory_space=pltpu.HBM)] * len(kept),
        out_specs=(vmem,) * 6,
        scratch_shapes=[
            pltpu.VMEM(estimate.shape, F32),
            pltpu.VMEM(view_data.shape, F32),
            pltpu.VMEM(psf_stack.shape, F32),
        ]
        + [pltpu.VMEM(c.shape, c.dtype) for c in constants]
        + [
            pltpu.VMEM((32, 32, 128), F32),
            pltpu.VMEM((32, 32, 256), F32),
            pltpu.VMEM((32, 3 * LX, 128), F32),
            pltpu.VMEM((8, ROWS, COLUMNS), F32),
            pltpu.VMEM((2, 2, 8, EDGE, 128), F32),
            pltpu.VMEM((2, 2, LX, 128), F32),
            pltpu.VMEM((2, 2, ROWS, 128), F32),
            pltpu.VMEM((2, 8, 2 * LX, 128), F32),
            pltpu.VMEM((2, 8, 2 * LX, 128), F32),
            pltpu.VMEM((8, 2 * LX, 128), F32),
            pltpu.VMEM((4, 64, 128), F32),
            pltpu.VMEM((2, 32, 128), F32),
            pltpu.VMEM((16, 128), F32),
            pltpu.VMEM((16, 128), F32),
            pltpu.VMEM((2, 8, 128), F32),
            pltpu.VMEM((1, 128), F32),
            pltpu.VMEM((2 * nx * ny, 1, 128), F32),
            pltpu.SemaphoreType.DMA((len(kept),)),
            pltpu.SemaphoreType.DMA((2,)),
            pltpu.SemaphoreType.DMA((2, 2)),
            pltpu.SemaphoreType.DMA,
            pltpu.SemaphoreType.DMA((2,)),
            pltpu.SemaphoreType.DMA,
            pltpu.SemaphoreType.DMA,
            pltpu.SemaphoreType.DMA,
            pltpu.SemaphoreType.DMA,
            pltpu.SemaphoreType.REGULAR((4,)),
            pltpu.SemaphoreType.REGULAR,
        ],
        compiler_params=pltpu.CompilerParams(
            collective_id=0, has_side_effects=True, vmem_limit_bytes=32 << 20
        ),
    )(view_index, *kept)
    return pl.pallas_call(
        hand_over,
        out_shape=out_shape,
        in_specs=[vmem] * 6,
        out_specs=(anywhere,) * 6,
        scratch_shapes=[pltpu.SemaphoreType.DMA((6,))],
        compiler_params=pltpu.CompilerParams(vmem_limit_bytes=4 << 20),
    )(*results)


def solution(mesh):
    spread = P("gz", "gx", "gy")
    return jax.shard_map(
        functools.partial(local, mesh.shape["gx"], mesh.shape["gy"]),
        mesh=mesh,
        in_specs=(spread, spread, P(), P()),
        out_specs=(spread, spread, spread, spread, P(None, "gx", "gy"), P()),
        check_vma=False,
    )
```

```python
import functools

import jax
import jax.numpy as jnp
import numpy as np
from jax import lax
from jax.experimental import pallas as pl
from jax.experimental.pallas import tpu as pltpu
from jax.sharding import PartitionSpec as P

MESH = pl.DeviceIdType.MESH
HALO = 15
EDGE = 16
ROWS, COLUMNS = 64, 128
LX, LY = ROWS + 2 * EDGE, COLUMNS + 2 * EDGE
HALF = LY // 2 + 1
TAPS = 2 * HALO + 1
BF16, F32 = jnp.bfloat16, jnp.float32


def parts_of(table):
    table = np.asarray(table, np.float64)
    high = table.astype(np.float32).astype(BF16)
    low = (table - high.astype(np.float64)).astype(np.float32).astype(BF16)
    return high, low


def stacked(table):
    high, low = parts_of(table)
    return np.concatenate([high, low, high], axis=0)


def beside(table):
    high, low = parts_of(table)
    return np.concatenate([high, high, low], axis=1)


def column_table(positions):
    angle = 2.0 * np.pi / LY * np.outer(positions, np.arange(HALF))
    table = np.zeros((len(positions), 256))
    table[:, :HALF] = np.cos(angle)
    table[:, 128 : 128 + HALF] = -np.sin(angle)
    return table


def row_table(positions):
    angle = 2.0 * np.pi / LX * np.outer(np.arange(LX), positions)
    c, s = np.cos(angle), np.sin(angle)
    return np.block([[c, s], [-s, c]])


def tables():
    inner = column_table(EDGE + np.arange(COLUMNS))
    left = column_table(np.arange(EDGE))
    right = column_table(LY - EDGE + np.arange(EDGE))
    columns = stacked(np.concatenate([inner] + [left, right] * 4))
    inner_rows = beside(row_table(EDGE + np.arange(ROWS)))
    edge_rows = beside(row_table(np.concatenate([np.arange(EDGE), LX - EDGE + np.arange(EDGE)])))
    kept = np.arange(ROWS)
    halves = []
    for part in (np.concatenate([kept[:EDGE], kept[-EDGE:]]), kept[EDGE:-EDGE]):
        angle = 2.0 * np.pi / LX * np.outer(EDGE + part, np.arange(LX))
        c, s = np.cos(angle), np.sin(angle)
        halves.append(beside(np.block([[c, -s], [s, c]])))
    rows_back = np.concatenate(halves)
    angle = 2.0 * np.pi / LY * np.outer(np.arange(HALF), EDGE + np.arange(COLUMNS))
    weight = np.where(np.isin(np.arange(HALF), (0, LY // 2)), 1.0, 2.0)[:, None] / (LX * LY)
    back = np.zeros((256, COLUMNS))
    back[:HALF] = weight * np.cos(angle)
    back[128 : 128 + HALF] = -weight * np.sin(angle)
    high, low = parts_of(back)
    columns_back = np.block([[high, low], [high, np.zeros_like(low)]])
    taps = column_table(np.concatenate([np.arange(TAPS) - HALO, [0]]))
    taps[TAPS] = 0.0
    tap_columns = np.concatenate([stacked(taps), np.zeros((32, 256), BF16)], axis=0)
    tap_rows_table = row_table(np.concatenate([np.arange(TAPS) - HALO, [0]]))
    tap_rows_table[:, TAPS] = 0.0
    tap_rows_table[:, 32 + TAPS] = 0.0
    tap_rows = beside(tap_rows_table)
    pools = np.zeros((128, 512), np.float32)
    for level in range(4):
        step = 2 ** (level + 1)
        for column in range(COLUMNS):
            pools[column, 128 * level + column // step] = 1.0 / step
    pools = np.concatenate([pools] * 3, axis=0).astype(BF16)
    tall = np.concatenate([columns, columns_back, tap_columns, pools[:, :256], pools[:, 256:]])
    wide = np.zeros((2 * LX, 1536), BF16)
    wide[:, :384] = inner_rows
    wide[:, 384:576] = edge_rows
    wide[:, 640:832] = tap_rows
    wide[: 2 * ROWS, 896:1472] = rows_back
    return tall, wide


def two(x):
    high = x.astype(BF16)
    return high, (x - high.astype(F32)).astype(BF16)


def dot(a, b):
    return jnp.dot(a, b, preferred_element_type=F32)


def left_triple(x):
    high, low = two(x)
    return jnp.concatenate([high, high, low], axis=1)


def right_triple(x):
    high, low = two(x)
    return jnp.concatenate([high, low, high], axis=0)


def exact_triple(x):
    high = x.astype(BF16)
    rest = x - high.astype(F32)
    middle = rest.astype(BF16)
    low = (rest - middle.astype(F32)).astype(BF16)
    return jnp.concatenate([high, middle, low], axis=1)


def body(nx, ny, index_ref, *refs):
    inputs, refs = refs[:5], refs[5:]
    updated_ref, one_ref, two_ref, three_ref, four_ref, five_ref = refs[:6]
    held, refs = refs[6:11], refs[11:]
    est_ref, view_ref, psf_ref, tall_ref, wide_ref = held
    (
        taps_ref,
        tap_half_ref,
        kernel_ref,
        ratio_ref,
        edge_rows,
        edge_columns,
        packed,
        own_ref,
        other_ref,
        product_ref,
        pool_a,
        pool_b,
        pool_c,
        pool_d,
        plane_ref,
        tile_ref,
        gathered,
        local_sem,
        send_sem,
        recv_sem,
        part_send,
        part_recv,
        swap_send,
        swap_recv,
        all_send,
        all_recv,
        word_sem,
        pair_sem,
    ) = refs
    gx, gy, gz = lax.axis_index("gx"), lax.axis_index("gy"), lax.axis_index("gz")

    def turned(at, offset, length):
        offset = offset % length
        if offset == 0:
            return at
        return jnp.where(at >= length - offset, at + offset - length, at + offset)

    def device(dx, dy, dz=0):
        return {"gx": turned(gx, dx, nx), "gy": turned(gy, dy, ny), "gz": turned(gz, dz, 2)}

    fetches = [
        pltpu.make_async_copy(source, target, local_sem.at[k])
        for k, (source, target) in enumerate(zip(inputs, held))
    ]
    fetches[0].start()

    count = nx * ny

    def there(dx, dy):
        tests = []
        if dx:
            tests.append(gx >= -dx if dx < 0 else gx < nx - dx)
        if dy:
            tests.append(gy >= -dy if dy < 0 else gy < ny - dy)
        return tests[0] if len(tests) == 1 else tests[0] & tests[1]

    def box(reach):
        steps = (-reach, 0, reach)
        return [(dx, dy) for dx in steps for dy in steps if (dx, dy) != (0, 0)]

    def hops(offset):
        dx, dy, dz = offset
        ring = lambda k, n: min(k, n - k)
        return ring(dx % 4, 4) + ring(dx // 4, nx // 4) + ring(dy, ny) + 0.5 * dz

    every = ((dx, dy, dz) for dx in range(nx) for dy in range(ny) for dz in (0, 1))
    far = sorted(every, key=hops, reverse=True)[:-1]

    def signal_all(sem, offsets):
        for dx, dy in offsets:

            @pl.when(there(dx, dy))
            def _():
                pl.semaphore_signal(sem, inc=1, device_id=device(dx, dy), device_id_type=MESH)

    def number(offsets):
        return sum(jnp.where(there(dx, dy), 1, 0) for dx, dy in offsets)

    rounds = [box(1), box(2), box(4), [(-8, 0), (8, 0)]]

    def spread_word(k):
        signal_all(word_sem.at[k], rounds[k])

    def hear_word(k):
        pl.semaphore_wait(word_sem.at[k], number(rounds[k]))

    barrier = pltpu.get_barrier_semaphore()
    pl.semaphore_signal(barrier, inc=1, device_id=device(0, 0, 1), device_id_type=MESH)
    signal_all(barrier, box(1))
    for k in (4, 3, 2, 1):
        fetches[k].start()

    def pack(planes):
        lane = lax.broadcasted_iota(jnp.int32, planes[0].shape, 1)
        to_right = jnp.zeros(planes[0].shape, F32)
        to_left = jnp.zeros(planes[0].shape, F32)
        for z, plane in enumerate(planes):
            base = (z % 4) * 32
            low, high = (base, base + EDGE) if z < 4 else (base + EDGE, base)
            shift = (low - (COLUMNS - EDGE)) % 128
            rolled = pltpu.roll(plane, shift, 1) if shift else plane
            to_right = jnp.where((lane >= low) & (lane < low + EDGE), rolled, to_right)
            rolled = pltpu.roll(plane, high, 1) if high else plane
            to_left = jnp.where((lane >= high) & (lane < high + EDGE), rolled, to_left)
        return to_right, to_left

    middle, top, bottom = pl.ds(EDGE, ROWS), pl.ds(0, EDGE), pl.ds(EDGE + ROWS, EDGE)
    head, tail, trunk = pl.ds(0, EDGE), pl.ds(ROWS - EDGE, EDGE), pl.ds(EDGE, ROWS - 2 * EDGE)

    def send(copies):
        for copy, ahead in copies:
            pl.when(ahead)(copy.start)

    def wait_units(sem, units, send):
        for last_x in (True, False):
            for last_y in (True, False):
                end_x = (gx == 0) | (gx == nx - 1)
                end_y = (gy == 0) | (gy == ny - 1)
                here = (end_x if last_x else ~end_x) & (end_y if last_y else ~end_y)
                total = units(1 if last_x else 2, 1 if last_y else 2)
                slab = kernel_ref.at[pl.ds(0, 2), pl.ds(0, total * EDGE // 2)]
                copy = pltpu.make_async_remote_copy(
                    src_ref=slab,
                    dst_ref=slab,
                    send_sem=sem,
                    recv_sem=sem,
                    device_id=device(0, 0, 1),
                    device_id_type=MESH,
                )
                pl.when(here)(copy.wait_send if send else copy.wait_recv)

    def receive_strips(turn):
        wait_units(recv_sem.at[turn, 1], lambda sx, sy: 4 * sy, False)

    def receive_edges(turn):
        wait_units(recv_sem.at[turn, 0], lambda sx, sy: sx * (8 + sy), False)

    def finish_sends(turn):
        wait_units(send_sem.at[turn], lambda sx, sy: 4 * sy + sx * (8 + sy), True)

    def halo_copies(source, turn):
        def copy(src, dst, at, dx, dy):
            sent = pltpu.make_async_remote_copy(
                src_ref=src,
                dst_ref=dst,
                send_sem=send_sem.at[turn],
                recv_sem=recv_sem.at[turn, at],
                device_id=device(dx, dy),
                device_id_type=MESH,
            )
            return sent, there(dx, dy)

        right, left = packed.at[turn, 0], packed.at[turn, 1]
        from_left, from_right = edge_columns.at[turn, 0], edge_columns.at[turn, 1]
        early = [
            copy(source.at[:, tail, :], edge_rows.at[turn, 0], 0, 1, 0),
            copy(source.at[:, head, :], edge_rows.at[turn, 1], 0, -1, 0),
            copy(right.at[tail, :], from_left.at[top, :], 0, 1, 1),
            copy(right.at[head, :], from_left.at[bottom, :], 0, -1, 1),
            copy(left.at[tail, :], from_right.at[top, :], 0, 1, -1),
            copy(left.at[head, :], from_right.at[bottom, :], 0, -1, -1),
        ]
        for rows in (head, tail, trunk):
            into = pl.ds(rows.start + EDGE, rows.size)
            early.append(copy(right.at[rows, :], from_left.at[into, :], 1, 0, 1))
            early.append(copy(left.at[rows, :], from_right.at[into, :], 1, 0, -1))
        return early[:-2], early[-2:]

    def clear_borders():
        rows, columns = jnp.zeros((8, EDGE, 128), F32), jnp.zeros((LX, 128), F32)
        for end, at, part in ((gx == 0, 0, top), (gx == nx - 1, 1, bottom)):

            @pl.when(end)
            def _():
                for turn in (0, 1):
                    edge_rows[turn, at] = rows
                    for side in (0, 1):
                        edge_columns[turn, side, part, :] = columns[:EDGE]

        for end, side in ((gy == 0, 0), (gy == ny - 1, 1)):

            @pl.when(end)
            def _():
                for turn in (0, 1):
                    edge_columns[turn, side] = columns

    def partner_copy(turn, z):
        return pltpu.make_async_remote_copy(
            src_ref=own_ref.at[turn, z],
            dst_ref=other_ref.at[turn, z],
            send_sem=part_send,
            recv_sem=part_recv.at[turn],
            device_id=device(0, 0, 1),
            device_id_type=MESH,
        )

    def transform(turn, height, plane_of, left, right, rows_table, adding):
        lane = lax.broadcasted_iota(jnp.int32, (height, 128), 1)
        even = (lane & EDGE) == 0
        mixed = (
            jnp.where(even, left, right),
            jnp.where(even, pltpu.roll(left, 128 - EDGE, 1), pltpu.roll(right, EDGE, 1)),
        )
        rows = []
        for z in range(8):
            j = 32 * (z % 4)
            side = jnp.where((lane >= j) & (lane < j + 32), mixed[z // 4], 0.0)
            rows.append(jnp.concatenate([plane_of(z), side], axis=1))
        half = dot(left_triple(jnp.concatenate(rows, axis=0)), tall_ref[0:768, :])
        for group in (0, 1):
            for pair in (0, 1):
                z = 4 * group + 2 * pair
                a = half[z * height : (z + 1) * height]
                b = half[(z + 1) * height : (z + 2) * height]
                joint = jnp.concatenate(
                    [
                        jnp.concatenate([a[:, :128], b[:, :128]], axis=1),
                        jnp.concatenate([a[:, 128:], b[:, 128:]], axis=1),
                    ],
                    axis=0,
                )
                full = dot(wide_ref[:, rows_table], right_triple(joint))
                for b in (0, 1):
                    part = full[:, 128 * b : 128 * b + 128]
                    if adding:
                        own_ref[turn, z + b] = own_ref[turn, z + b] + part
                        partner_copy(turn, z + b).start()
                    else:
                        own_ref[turn, z + b] = part

    def forward_inner(source, turn):
        left, right = edge_columns[turn, 0, middle, :], edge_columns[turn, 1, middle, :]
        transform(turn, ROWS, lambda z: source[z], left, right, slice(0, 384), False)

    def forward_edge(turn):
        def both(a, b):
            return jnp.concatenate([a, b], axis=0)

        left, right = [
            both(edge_columns[turn, side, top, :], edge_columns[turn, side, bottom, :])
            for side in (0, 1)
        ]

        def plane_of(z):
            return both(edge_rows[turn, 0, z], edge_rows[turn, 1, z])

        transform(turn, 2 * EDGE, plane_of, left, right, slice(384, 576), True)

    def depth(x_ref, turn, base, mirrored, adding):
        def blocks(step, carry):
            block(2 * step)
            block(2 * step + 1)
            return carry

        def block(step):
            at = pl.multiple_of(step * 8, 8)
            re, im = pl.ds(at, 8), pl.ds(pl.multiple_of(at + LX, 8), 8)
            xr = [x_ref[turn, z, re, :] for z in range(8)]
            xi = [x_ref[turn, z, im, :] for z in range(8)]
            if adding:
                yr = [product_ref[z, re, :] for z in range(8)]
                yi = [product_ref[z, im, :] for z in range(8)]
            else:
                yr, yi = [None] * 8, [None] * 8
            xs = [r + i for r, i in zip(xr, xi)]
            sums = [[None] * 8 for _ in range(3)]
            for d in range(-7, 8):
                taps = [kernel_ref[base + d, pl.ds(at + LX * k, 8), :] for k in range(3)]
                values = (xs, xi, xr) if mirrored else (xs, xr, xi)
                for out in range(8):
                    z = out + d if mirrored else out - d
                    if not 0 <= z < 8:
                        continue
                    for k in range(3):
                        term = taps[k] * values[k][z]
                        sums[k][out] = term if sums[k][out] is None else sums[k][out] + term
            for z in range(8):
                one, two_, three = (sums[k][z] for k in range(3))
                r = one + two_ if mirrored else one - three
                i = one - three if mirrored else one + two_
                yr[z] = r if yr[z] is None else yr[z] + r
                yi[z] = i if yi[z] is None else yi[z] + i
            for z in range(8):
                product_ref[z, re, :] = yr[z]
                product_ref[z, im, :] = yi[z]

        lax.fori_loop(0, LX // 16, blocks, 0)

    def inverse(parts):
        rows = []
        table = slice(64 * parts[0], 64 * parts[-1] + 64)
        for z in range(0, 8, 2):
            joint = jnp.concatenate([product_ref[z], product_ref[z + 1]], axis=1)
            half = dot(wide_ref[table, 896:1472], right_triple(joint))
            for b in (0, 1):
                lanes = slice(128 * b, 128 * b + 128)
                for k in range(len(parts)):
                    re, im = half[64 * k : 64 * k + 32, lanes], half[64 * k + 32 : 64 * k + 64, lanes]
                    rows.append(jnp.concatenate([re, im], axis=1))
        full = dot(jnp.concatenate(two(jnp.concatenate(rows, axis=0)), axis=1), tall_ref[768:1280, :])
        return (full[:, :COLUMNS] + full[:, COLUMNS:]).reshape(8, 32 * len(parts), COLUMNS)

    def convolve(turn, mirrored):
        depth(own_ref, turn, HALO, mirrored, False)
        planes = other_ref.at[turn]
        pltpu.make_async_remote_copy(
            src_ref=planes,
            dst_ref=planes,
            send_sem=part_send,
            recv_sem=part_recv.at[turn],
            device_id=device(0, 0, 1),
            device_id_type=MESH,
        ).wait_recv()
        base = HALO + 8 - 16 * gz if mirrored else HALO - 8 + 16 * gz
        depth(other_ref, turn, base, mirrored, True)

    def spectrum():
        for k in (4, 3, 2):
            fetches[k].wait()
        view = index_ref[0]
        taps_ref[...] = jnp.zeros((32, 32, 128), F32)

        taps_ref[0:TAPS, 0:TAPS, 0:TAPS] = psf_ref[view]
        total = jnp.sum(jnp.sum(taps_ref[...], axis=0), axis=(0, 1), keepdims=True)
        scale = 1.0 / total

        for step in range(4):
            x = taps_ref[8 * step : 8 * step + 8].reshape(256, 128) * scale
            high = x.astype(BF16).astype(F32)
            low = x - high
            joint = high + pltpu.roll(high, 32, 1) + pltpu.roll(low, 64, 1)
            half = dot(joint.astype(BF16), tall_ref[1280:1408, :])
            tap_half_ref[8 * step : 8 * step + 8] = half.reshape(8, 32, 256)

        def rows(step, carry):
            for pair in range(4):
                z = 8 * step + 2 * pair
                a, b = tap_half_ref[z], tap_half_ref[z + 1]
                joint = jnp.concatenate(
                    [
                        jnp.concatenate([a[:, :128], b[:, :128]], axis=1),
                        jnp.concatenate([a[:, 128:], b[:, 128:]], axis=1),
                    ],
                    axis=0,
                )
                full = dot(wide_ref[:, 640:832], right_triple(joint))
                for b in (0, 1):
                    re = full[:LX, 128 * b : 128 * b + 128]
                    im = full[LX:, 128 * b : 128 * b + 128]
                    kernel_ref[z + b, 0:LX] = re
                    kernel_ref[z + b, LX : 2 * LX] = im - re
                    kernel_ref[z + b, 2 * LX :] = im + re
            return carry

        lax.fori_loop(0, 4, rows, 0)

    fetches[0].wait()
    packed[0, 0], packed[0, 1] = pack([est_ref[z] for z in range(8)])
    pl.semaphore_wait(barrier, 1 + number(box(1)))
    spread_word(0)
    early, late = halo_copies(est_ref, 0)
    send(early + late)
    clear_borders()
    spectrum()
    fetches[1].wait()
    receive_strips(0)
    forward_inner(est_ref, 0)
    receive_edges(0)
    hear_word(0)
    spread_word(1)
    forward_edge(0)
    convolve(0, False)
    early, late = halo_copies(ratio_ref, 1)
    blurred = inverse((0,))
    ends = []
    for rows, at in ((head, slice(0, EDGE)), (tail, slice(EDGE, 2 * EDGE))):
        ratio = view_ref[:, rows, :] / blurred[:, at]
        ratio_ref[:, rows, :] = ratio
        ends.append(ratio)
    ends = jnp.concatenate(ends, axis=1)
    for side, strip in enumerate(pack([ends[z] for z in range(8)])):
        packed[1, side, head, :] = strip[:EDGE]
        packed[1, side, tail, :] = strip[EDGE:]
    send(early)
    ratio = view_ref[:, trunk, :] / inverse((1,))
    ratio_ref[:, trunk, :] = ratio
    for side, strip in enumerate(pack([ratio[z] for z in range(8)])):
        packed[1, side, trunk, :] = strip
    send(late)
    hear_word(1)
    spread_word(2)
    receive_strips(1)
    forward_inner(ratio_ref, 1)
    receive_edges(1)
    forward_edge(1)
    hear_word(2)
    spread_word(3)
    convolve(1, True)
    hear_word(3)
    pl.semaphore_signal(pair_sem, inc=1, device_id=device(0, 0, 1), device_id_type=MESH)
    correction = inverse((0, 1))
    pieces = [correction[:, :EDGE], correction[:, 2 * EDGE :], correction[:, EDGE : 2 * EDGE]]
    updated = est_ref[...] * jnp.concatenate(pieces, axis=1)
    column_sums = jnp.sum(updated, axis=0)
    halves = [jnp.sum(column_sums[32 * i : 32 * i + 32], axis=0, keepdims=True) for i in (0, 1)]
    source = lax.broadcasted_iota(jnp.int32, (384, 128), 0) % 128
    target = lax.broadcasted_iota(jnp.int32, (384, 128), 1)
    place = jnp.where(target == 4 * gy + source // 32, 2.0**-14, 0.0).astype(BF16)
    eight = jnp.concatenate(halves + [jnp.zeros((6, 128), F32)], axis=0)
    placed = dot(exact_triple(eight), place)
    tile_ref[...] = placed[0:1] + pltpu.roll(placed[1:2], 4 * ny, 1)
    me = gz * count + gx * ny + gy
    pl.semaphore_wait(pair_sem, 1)
    for dx, dy, dz in far:
        pltpu.make_async_remote_copy(
            src_ref=tile_ref,
            dst_ref=gathered.at[me],
            send_sem=all_send,
            recv_sem=all_recv,
            device_id=device(dx, dy, dz),
            device_id_type=MESH,
        ).start()
    gathered[me] = tile_ref[...]

    updated_ref[...] = updated
    for k in range(4):
        pool_a[k] = updated[2 * k] + updated[2 * k + 1]
    even, odd = pl.ds(0, ROWS // 2, stride=2), pl.ds(1, ROWS // 2, stride=2)
    level_one = [(pool_a[k, even, :] + pool_a[k, odd, :]) * 0.25 for k in range(4)]
    for k in (0, 1):
        pool_b[k] = level_one[2 * k] + level_one[2 * k + 1]
    even, odd = pl.ds(0, ROWS // 4, stride=2), pl.ds(1, ROWS // 4, stride=2)
    level_two = [(pool_b[k, even, :] + pool_b[k, odd, :]) * 0.25 for k in (0, 1)]
    pool_c[...] = level_two[0] + level_two[1]
    even, odd = pl.ds(0, ROWS // 8, stride=2), pl.ds(1, ROWS // 8, stride=2)
    level_three = (pool_c[even, :] + pool_c[odd, :]) * 0.25
    pool_d[0:8] = level_three
    pool_d[8:16] = jnp.zeros((8, 128), F32)
    even, odd = pl.ds(0, 8, stride=2), pl.ds(1, 8, stride=2)
    level_four = (pool_d[even, :] + pool_d[odd, :]) * 0.5
    plane_ref[0] = dot(exact_triple(level_four), tall_ref[1792:2176, 128:256])
    swap = pltpu.make_async_remote_copy(
        src_ref=plane_ref.at[0],
        dst_ref=plane_ref.at[1],
        send_sem=swap_send,
        recv_sem=swap_recv,
        device_id=device(0, 0, 1),
        device_id_type=MESH,
    )
    swap.start()
    third = dot(exact_triple(level_three), tall_ref[1792:2176, 0:128])
    three_ref[0] = third[:, :16]
    second = dot(exact_triple(jnp.concatenate(level_two, axis=0)), tall_ref[1408:1792, 128:256])
    for k in (0, 1):
        two_ref[k] = second[16 * k : 16 * k + 16, :32]
    full = dot(exact_triple(jnp.concatenate(level_one, axis=0)), tall_ref[1408:1792, 0:128])
    for k in range(4):
        one_ref[k] = full[32 * k : 32 * k + 32, :64]
    swap.wait_recv()
    fourth = (plane_ref[0] + plane_ref[1]) * 0.5
    four_ref[0] = fourth[:4, :8]

    finish_sends(0)
    finish_sends(1)
    swap.wait_send()
    pltpu.make_async_remote_copy(
        src_ref=own_ref,
        dst_ref=own_ref,
        send_sem=part_send,
        recv_sem=part_send,
        device_id=device(0, 0, 1),
        device_id_type=MESH,
    ).wait_send()
    others = gathered.at[pl.ds(0, 2 * count - 1)]
    everyone = pltpu.make_async_remote_copy(
        src_ref=others,
        dst_ref=others,
        send_sem=all_send,
        recv_sem=all_recv,
        device_id=device(0, 0, 1),
        device_id_type=MESH,
    )
    everyone.wait_send()
    everyone.wait_recv()
    strips = jnp.sum(gathered[...].reshape(2, nx, ny, 128), axis=(0, 2))
    five_ref[0, pl.ds(0, nx, stride=2), :] = strips[:, : 4 * ny]
    five_ref[0, pl.ds(1, nx, stride=2), :] = pltpu.roll(strips, 128 - 4 * ny, 1)[:, : 4 * ny]


def hand_over(*refs):
    sources, targets, sems = refs[:6], refs[6:12], refs[12]
    copies = [pltpu.make_async_copy(a, b, sems.at[k]) for k, (a, b) in enumerate(zip(sources, targets))]
    for copy in copies:
        copy.start()
    for copy in copies:
        copy.wait()


def local(nx, ny, estimate, view_data, psf_stack, view_index):
    vmem = pl.BlockSpec(memory_space=pltpu.VMEM)
    anywhere = pl.BlockSpec(memory_space=pl.ANY)
    shape = jax.ShapeDtypeStruct
    out_shape = (
        shape((8, 64, 128), F32),
        shape((4, 32, 64), F32),
        shape((2, 16, 32), F32),
        shape((1, 8, 16), F32),
        shape((1, 4, 8), F32),
        shape((1, 2 * nx, 4 * ny), F32),
    )
    constants = [jnp.asarray(t) for t in tables()]
    kept = [
        pltpu.with_memory_space_constraint(x, pltpu.HBM)
        for x in (estimate, view_data, psf_stack, *constants)
    ]
    results = pl.pallas_call(
        functools.partial(body, nx, ny),
        out_shape=out_shape,
        in_specs=[pl.BlockSpec(memory_space=pltpu.SMEM)]
        + [pl.BlockSpec(memory_space=pltpu.HBM)] * len(kept),
        out_specs=(vmem,) * 6,
        scratch_shapes=[
            pltpu.VMEM(estimate.shape, F32),
            pltpu.VMEM(view_data.shape, F32),
            pltpu.VMEM(psf_stack.shape, F32),
        ]
        + [pltpu.VMEM(c.shape, c.dtype) for c in constants]
        + [
            pltpu.VMEM((32, 32, 128), F32),
            pltpu.VMEM((32, 32, 256), F32),
            pltpu.VMEM((32, 3 * LX, 128), F32),
            pltpu.VMEM((8, ROWS, COLUMNS), F32),
            pltpu.VMEM((2, 2, 8, EDGE, 128), F32),
            pltpu.VMEM((2, 2, LX, 128), F32),
            pltpu.VMEM((2, 2, ROWS, 128), F32),
            pltpu.VMEM((2, 8, 2 * LX, 128), F32),
            pltpu.VMEM((2, 8, 2 * LX, 128), F32),
            pltpu.VMEM((8, 2 * LX, 128), F32),
            pltpu.VMEM((4, 64, 128), F32),
            pltpu.VMEM((2, 32, 128), F32),
            pltpu.VMEM((16, 128), F32),
            pltpu.VMEM((16, 128), F32),
            pltpu.VMEM((2, 8, 128), F32),
            pltpu.VMEM((1, 128), F32),
            pltpu.VMEM((2 * nx * ny, 1, 128), F32),
            pltpu.SemaphoreType.DMA((len(kept),)),
            pltpu.SemaphoreType.DMA((2,)),
            pltpu.SemaphoreType.DMA((2, 2)),
            pltpu.SemaphoreType.DMA,
            pltpu.SemaphoreType.DMA((2,)),
            pltpu.SemaphoreType.DMA,
            pltpu.SemaphoreType.DMA,
            pltpu.SemaphoreType.DMA,
            pltpu.SemaphoreType.DMA,
            pltpu.SemaphoreType.REGULAR((4,)),
            pltpu.SemaphoreType.REGULAR,
        ],
        compiler_params=pltpu.CompilerParams(
            collective_id=0, has_side_effects=True, vmem_limit_bytes=32 << 20
        ),
    )(view_index, *kept)
    return pl.pallas_call(
        hand_over,
        out_shape=out_shape,
        in_specs=[vmem] * 6,
        out_specs=(anywhere,) * 6,
        scratch_shapes=[pltpu.SemaphoreType.DMA((6,))],
        compiler_params=pltpu.CompilerParams(vmem_limit_bytes=4 << 20),
    )(*results)


def solution(mesh):
    spread = P("gz", "gx", "gy")
    return jax.shard_map(
        functools.partial(local, mesh.shape["gx"], mesh.shape["gy"]),
        mesh=mesh,
        in_specs=(spread, spread, P(), P()),
        out_specs=(spread, spread, spread, spread, P(None, "gx", "gy"), P()),
        check_vma=False,
    )
```

```python
import functools

import jax
import jax.numpy as jnp
import numpy as np
from jax import lax
from jax.experimental import pallas as pl
from jax.experimental.pallas import tpu as pltpu
from jax.sharding import PartitionSpec as P

MESH = pl.DeviceIdType.MESH
HALO = 15
EDGE = 16
ROWS, COLUMNS = 64, 128
LX, LY = ROWS + 2 * EDGE, COLUMNS + 2 * EDGE
HALF = LY // 2 + 1
TAPS = 2 * HALO + 1
BF16, F32 = jnp.bfloat16, jnp.float32


def parts_of(table):
    table = np.asarray(table, np.float64)
    high = table.astype(np.float32).astype(BF16)
    low = (table - high.astype(np.float64)).astype(np.float32).astype(BF16)
    return high, low


def stacked(table):
    high, low = parts_of(table)
    return np.concatenate([high, low, high], axis=0)


def beside(table):
    high, low = parts_of(table)
    return np.concatenate([high, high, low], axis=1)


def column_table(positions):
    angle = 2.0 * np.pi / LY * np.outer(positions, np.arange(HALF))
    table = np.zeros((len(positions), 256))
    table[:, :HALF] = np.cos(angle)
    table[:, 128 : 128 + HALF] = -np.sin(angle)
    return table


def row_table(positions):
    angle = 2.0 * np.pi / LX * np.outer(np.arange(LX), positions)
    c, s = np.cos(angle), np.sin(angle)
    return np.block([[c, s], [-s, c]])


def tables():
    inner = column_table(EDGE + np.arange(COLUMNS))
    left = column_table(np.arange(EDGE))
    right = column_table(LY - EDGE + np.arange(EDGE))
    columns = stacked(np.concatenate([inner] + [left, right] * 4))
    inner_rows = beside(row_table(EDGE + np.arange(ROWS)))
    edge_rows = beside(row_table(np.concatenate([np.arange(EDGE), LX - EDGE + np.arange(EDGE)])))
    kept = np.arange(ROWS)
    halves = []
    for part in (np.concatenate([kept[:EDGE], kept[-EDGE:]]), kept[EDGE:-EDGE]):
        angle = 2.0 * np.pi / LX * np.outer(EDGE + part, np.arange(LX))
        c, s = np.cos(angle), np.sin(angle)
        halves.append(beside(np.block([[c, -s], [s, c]])))
    rows_back = np.concatenate(halves)
    angle = 2.0 * np.pi / LY * np.outer(np.arange(HALF), EDGE + np.arange(COLUMNS))
    weight = np.where(np.isin(np.arange(HALF), (0, LY // 2)), 1.0, 2.0)[:, None] / (LX * LY)
    back = np.zeros((256, COLUMNS))
    back[:HALF] = weight * np.cos(angle)
    back[128 : 128 + HALF] = -weight * np.sin(angle)
    high, low = parts_of(back)
    columns_back = np.block([[high, low], [high, np.zeros_like(low)]])
    taps = column_table(np.concatenate([np.arange(TAPS) - HALO, [0]]))
    taps[TAPS] = 0.0
    tap_columns = np.concatenate([stacked(taps), np.zeros((32, 256), BF16)], axis=0)
    tap_rows_table = row_table(np.concatenate([np.arange(TAPS) - HALO, [0]]))
    tap_rows_table[:, TAPS] = 0.0
    tap_rows_table[:, 32 + TAPS] = 0.0
    tap_rows = beside(tap_rows_table)
    pools = np.zeros((128, 512), np.float32)
    for level in range(4):
        step = 2 ** (level + 1)
        for column in range(COLUMNS):
            pools[column, 128 * level + column // step] = 1.0 / step
    pools = np.concatenate([pools] * 3, axis=0).astype(BF16)
    tall = np.concatenate([columns, columns_back, tap_columns, pools[:, :256], pools[:, 256:]])
    wide = np.zeros((2 * LX, 1536), BF16)
    wide[:, :384] = inner_rows
    wide[:, 384:576] = edge_rows
    wide[:, 640:832] = tap_rows
    wide[: 2 * ROWS, 896:1472] = rows_back
    return tall, wide


def two(x):
    high = x.astype(BF16)
    return high, (x - high.astype(F32)).astype(BF16)


def dot(a, b):
    return jnp.dot(a, b, preferred_element_type=F32)


def left_triple(x):
    high, low = two(x)
    return jnp.concatenate([high, high, low], axis=1)


def right_triple(x):
    high, low = two(x)
    return jnp.concatenate([high, low, high], axis=0)


def exact_triple(x):
    high = x.astype(BF16)
    rest = x - high.astype(F32)
    middle = rest.astype(BF16)
    low = (rest - middle.astype(F32)).astype(BF16)
    return jnp.concatenate([high, middle, low], axis=1)


def body(nx, ny, index_ref, *refs):
    inputs, refs = refs[:5], refs[5:]
    updated_ref, one_ref, two_ref, three_ref, four_ref, five_ref = refs[:6]
    held, refs = refs[6:11], refs[11:]
    est_ref, view_ref, psf_ref, tall_ref, wide_ref = held
    (
        taps_ref,
        tap_half_ref,
        kernel_ref,
        ratio_ref,
        edge_rows,
        edge_columns,
        packed,
        own_ref,
        other_ref,
        product_ref,
        pool_a,
        pool_b,
        pool_c,
        pool_d,
        plane_ref,
        tile_ref,
        gathered,
        local_sem,
        send_sem,
        recv_sem,
        part_send,
        part_recv,
        swap_send,
        swap_recv,
        all_send,
        all_recv,
        word_sem,
        pair_sem,
    ) = refs
    gx, gy, gz = lax.axis_index("gx"), lax.axis_index("gy"), lax.axis_index("gz")

    def turned(at, offset, length):
        offset = offset % length
        if offset == 0:
            return at
        return jnp.where(at >= length - offset, at + offset - length, at + offset)

    def device(dx, dy, dz=0):
        return {"gx": turned(gx, dx, nx), "gy": turned(gy, dy, ny), "gz": turned(gz, dz, 2)}

    fetches = [
        pltpu.make_async_copy(source, target, local_sem.at[k])
        for k, (source, target) in enumerate(zip(inputs, held))
    ]
    fetches[0].start()

    count = nx * ny

    def there(dx, dy):
        tests = []
        if dx:
            tests.append(gx >= -dx if dx < 0 else gx < nx - dx)
        if dy:
            tests.append(gy >= -dy if dy < 0 else gy < ny - dy)
        return tests[0] if len(tests) == 1 else tests[0] & tests[1]

    def box(reach):
        steps = (-reach, 0, reach)
        return [(dx, dy) for dx in steps for dy in steps if (dx, dy) != (0, 0)]

    def hops(offset):
        dx, dy, dz = offset
        ring = lambda k, n: min(k, n - k)
        return ring(dx % 4, 4) + ring(dx // 4, nx // 4) + ring(dy, ny) + 0.5 * dz

    every = ((dx, dy, dz) for dx in range(nx) for dy in range(ny) for dz in (0, 1))
    far = sorted(every, key=hops, reverse=True)[:-1]

    def signal_all(sem, offsets):
        for dx, dy in offsets:

            @pl.when(there(dx, dy))
            def _():
                pl.semaphore_signal(sem, inc=1, device_id=device(dx, dy), device_id_type=MESH)

    def number(offsets):
        return sum(jnp.where(there(dx, dy), 1, 0) for dx, dy in offsets)

    rounds = [box(1), box(2), box(4), [(-8, 0), (8, 0)]]

    def spread_word(k):
        signal_all(word_sem.at[k], rounds[k])

    def hear_word(k):
        pl.semaphore_wait(word_sem.at[k], number(rounds[k]))

    barrier = pltpu.get_barrier_semaphore()
    pl.semaphore_signal(barrier, inc=1, device_id=device(0, 0, 1), device_id_type=MESH)
    signal_all(barrier, box(1))
    for k in (4, 3, 2, 1):
        fetches[k].start()

    def pack(planes):
        lane = lax.broadcasted_iota(jnp.int32, planes[0].shape, 1)
        to_right = jnp.zeros(planes[0].shape, F32)
        to_left = jnp.zeros(planes[0].shape, F32)
        for z, plane in enumerate(planes):
            base = (z % 4) * 32
            low, high = (base, base + EDGE) if z < 4 else (base + EDGE, base)
            shift = (low - (COLUMNS - EDGE)) % 128
            rolled = pltpu.roll(plane, shift, 1) if shift else plane
            to_right = jnp.where((lane >= low) & (lane < low + EDGE), rolled, to_right)
            rolled = pltpu.roll(plane, high, 1) if high else plane
            to_left = jnp.where((lane >= high) & (lane < high + EDGE), rolled, to_left)
        return to_right, to_left

    middle, top, bottom = pl.ds(EDGE, ROWS), pl.ds(0, EDGE), pl.ds(EDGE + ROWS, EDGE)
    head, tail, trunk = pl.ds(0, EDGE), pl.ds(ROWS - EDGE, EDGE), pl.ds(EDGE, ROWS - 2 * EDGE)

    def send(copies):
        for copy, ahead in copies:
            pl.when(ahead)(copy.start)

    def wait_units(sem, units, send):
        for last_x in (True, False):
            for last_y in (True, False):
                end_x = (gx == 0) | (gx == nx - 1)
                end_y = (gy == 0) | (gy == ny - 1)
                here = (end_x if last_x else ~end_x) & (end_y if last_y else ~end_y)
                total = units(1 if last_x else 2, 1 if last_y else 2)
                slab = kernel_ref.at[pl.ds(0, 2), pl.ds(0, total * EDGE // 2)]
                copy = pltpu.make_async_remote_copy(
                    src_ref=slab,
                    dst_ref=slab,
                    send_sem=sem,
                    recv_sem=sem,
                    device_id=device(0, 0, 1),
                    device_id_type=MESH,
                )
                pl.when(here)(copy.wait_send if send else copy.wait_recv)

    def receive_strips(turn):
        wait_units(recv_sem.at[turn, 1], lambda sx, sy: 4 * sy, False)

    def receive_edges(turn):
        wait_units(recv_sem.at[turn, 0], lambda sx, sy: sx * (8 + sy), False)

    def finish_sends(turn):
        wait_units(send_sem.at[turn], lambda sx, sy: 4 * sy + sx * (8 + sy), True)

    def halo_copies(source, turn):
        def copy(src, dst, at, dx, dy):
            sent = pltpu.make_async_remote_copy(
                src_ref=src,
                dst_ref=dst,
                send_sem=send_sem.at[turn],
                recv_sem=recv_sem.at[turn, at],
                device_id=device(dx, dy),
                device_id_type=MESH,
            )
            return sent, there(dx, dy)

        right, left = packed.at[turn, 0], packed.at[turn, 1]
        from_left, from_right = edge_columns.at[turn, 0], edge_columns.at[turn, 1]
        early = [
            copy(source.at[:, tail, :], edge_rows.at[turn, 0], 0, 1, 0),
            copy(source.at[:, head, :], edge_rows.at[turn, 1], 0, -1, 0),
            copy(right.at[tail, :], from_left.at[top, :], 0, 1, 1),
            copy(right.at[head, :], from_left.at[bottom, :], 0, -1, 1),
            copy(left.at[tail, :], from_right.at[top, :], 0, 1, -1),
            copy(left.at[head, :], from_right.at[bottom, :], 0, -1, -1),
        ]
        for rows in (head, tail, trunk):
            into = pl.ds(rows.start + EDGE, rows.size)
            early.append(copy(right.at[rows, :], from_left.at[into, :], 1, 0, 1))
            early.append(copy(left.at[rows, :], from_right.at[into, :], 1, 0, -1))
        return early[:-2], early[-2:]

    def clear_borders():
        rows, columns = jnp.zeros((8, EDGE, 128), F32), jnp.zeros((LX, 128), F32)
        for end, at, part in ((gx == 0, 0, top), (gx == nx - 1, 1, bottom)):

            @pl.when(end)
            def _():
                for turn in (0, 1):
                    edge_rows[turn, at] = rows
                    for side in (0, 1):
                        edge_columns[turn, side, part, :] = columns[:EDGE]

        for end, side in ((gy == 0, 0), (gy == ny - 1, 1)):

            @pl.when(end)
            def _():
                for turn in (0, 1):
                    edge_columns[turn, side] = columns

    def partner_copy(turn, group):
        planes = pl.ds(4 * group, 4)
        return pltpu.make_async_remote_copy(
            src_ref=own_ref.at[turn, planes],
            dst_ref=other_ref.at[turn, planes],
            send_sem=part_send,
            recv_sem=part_recv.at[turn, group],
            device_id=device(0, 0, 1),
            device_id_type=MESH,
        )

    def transform(turn, height, plane_of, left, right, rows_table, adding):
        lane = lax.broadcasted_iota(jnp.int32, (height, 128), 1)
        even = (lane & EDGE) == 0
        mixed = (
            jnp.where(even, left, right),
            jnp.where(even, pltpu.roll(left, 128 - EDGE, 1), pltpu.roll(right, EDGE, 1)),
        )
        rows = []
        for z in range(8):
            j = 32 * (z % 4)
            side = jnp.where((lane >= j) & (lane < j + 32), mixed[z // 4], 0.0)
            rows.append(jnp.concatenate([plane_of(z), side], axis=1))
        half = dot(left_triple(jnp.concatenate(rows, axis=0)), tall_ref[0:768, :])
        for group in (0, 1):
            whole = []
            for z in (4 * group, 4 * group + 2):
                a = half[z * height : (z + 1) * height]
                b = half[(z + 1) * height : (z + 2) * height]
                joint = jnp.concatenate(
                    [
                        jnp.concatenate([a[:, :128], b[:, :128]], axis=1),
                        jnp.concatenate([a[:, 128:], b[:, 128:]], axis=1),
                    ],
                    axis=0,
                )
                full = dot(wide_ref[:, rows_table], right_triple(joint))
                whole += [full[:, :128], full[:, 128:]]
            for z, part in enumerate(whole, 4 * group):
                own_ref[turn, z] = own_ref[turn, z] + part if adding else part
            if adding:
                partner_copy(turn, group).start()

    def forward_inner(source, turn):
        left, right = edge_columns[turn, 0, middle, :], edge_columns[turn, 1, middle, :]
        transform(turn, ROWS, lambda z: source[z], left, right, slice(0, 384), False)

    def forward_edge(turn):
        def both(a, b):
            return jnp.concatenate([a, b], axis=0)

        left, right = [
            both(edge_columns[turn, side, top, :], edge_columns[turn, side, bottom, :])
            for side in (0, 1)
        ]

        def plane_of(z):
            return both(edge_rows[turn, 0, z], edge_rows[turn, 1, z])

        transform(turn, 2 * EDGE, plane_of, left, right, slice(384, 576), True)

    def depth(x_ref, turn, base, mirrored, adding, planes):
        def blocks(step, carry):
            block(2 * step)
            block(2 * step + 1)
            return carry

        def block(step):
            at = pl.multiple_of(step * 8, 8)
            re, im = pl.ds(at, 8), pl.ds(pl.multiple_of(at + LX, 8), 8)
            xr = {z: x_ref[turn, z, re, :] for z in planes}
            xi = {z: x_ref[turn, z, im, :] for z in planes}
            if adding:
                yr = [product_ref[z, re, :] for z in range(8)]
                yi = [product_ref[z, im, :] for z in range(8)]
            else:
                yr, yi = [None] * 8, [None] * 8
            xs = {z: xr[z] + xi[z] for z in planes}
            sums = [[None] * 8 for _ in range(3)]
            for d in range(-7, 8):
                taps = [kernel_ref[base + d, pl.ds(at + LX * k, 8), :] for k in range(3)]
                values = (xs, xi, xr) if mirrored else (xs, xr, xi)
                for out in range(8):
                    z = out + d if mirrored else out - d
                    if z not in planes:
                        continue
                    for k in range(3):
                        term = taps[k] * values[k][z]
                        sums[k][out] = term if sums[k][out] is None else sums[k][out] + term
            for z in range(8):
                one, two_, three = (sums[k][z] for k in range(3))
                r = one + two_ if mirrored else one - three
                i = one - three if mirrored else one + two_
                yr[z] = r if yr[z] is None else yr[z] + r
                yi[z] = i if yi[z] is None else yi[z] + i
            for z in range(8):
                product_ref[z, re, :] = yr[z]
                product_ref[z, im, :] = yi[z]

        lax.fori_loop(0, LX // 16, blocks, 0)

    def inverse(parts):
        rows = []
        table = slice(64 * parts[0], 64 * parts[-1] + 64)
        for z in range(0, 8, 2):
            joint = jnp.concatenate([product_ref[z], product_ref[z + 1]], axis=1)
            half = dot(wide_ref[table, 896:1472], right_triple(joint))
            for b in (0, 1):
                lanes = slice(128 * b, 128 * b + 128)
                for k in range(len(parts)):
                    re, im = half[64 * k : 64 * k + 32, lanes], half[64 * k + 32 : 64 * k + 64, lanes]
                    rows.append(jnp.concatenate([re, im], axis=1))
        full = dot(jnp.concatenate(two(jnp.concatenate(rows, axis=0)), axis=1), tall_ref[768:1280, :])
        return (full[:, :COLUMNS] + full[:, COLUMNS:]).reshape(8, 32 * len(parts), COLUMNS)

    def convolve(turn, mirrored):
        depth(own_ref, turn, HALO, mirrored, False, range(8))
        base = HALO + 8 - 16 * gz if mirrored else HALO - 8 + 16 * gz
        for group in (0, 1):
            partner_copy(turn, group).wait_recv()
            depth(other_ref, turn, base, mirrored, True, range(4 * group, 4 * group + 4))

    def spectrum():
        for k in (4, 3, 2):
            fetches[k].wait()
        view = index_ref[0]
        taps_ref[...] = jnp.zeros((32, 32, 128), F32)

        taps_ref[0:TAPS, 0:TAPS, 0:TAPS] = psf_ref[view]
        total = jnp.sum(jnp.sum(taps_ref[...], axis=0), axis=(0, 1), keepdims=True)
        scale = 1.0 / total

        for step in range(4):
            x = taps_ref[8 * step : 8 * step + 8].reshape(256, 128) * scale
            high = x.astype(BF16).astype(F32)
            low = x - high
            joint = high + pltpu.roll(high, 32, 1) + pltpu.roll(low, 64, 1)
            half = dot(joint.astype(BF16), tall_ref[1280:1408, :])
            tap_half_ref[8 * step : 8 * step + 8] = half.reshape(8, 32, 256)

        def rows(step, carry):
            for pair in range(4):
                z = 8 * step + 2 * pair
                a, b = tap_half_ref[z], tap_half_ref[z + 1]
                joint = jnp.concatenate(
                    [
                        jnp.concatenate([a[:, :128], b[:, :128]], axis=1),
                        jnp.concatenate([a[:, 128:], b[:, 128:]], axis=1),
                    ],
                    axis=0,
                )
                full = dot(wide_ref[:, 640:832], right_triple(joint))
                for b in (0, 1):
                    re = full[:LX, 128 * b : 128 * b + 128]
                    im = full[LX:, 128 * b : 128 * b + 128]
                    kernel_ref[z + b, 0:LX] = re
                    kernel_ref[z + b, LX : 2 * LX] = im - re
                    kernel_ref[z + b, 2 * LX :] = im + re
            return carry

        lax.fori_loop(0, 4, rows, 0)

    fetches[0].wait()
    packed[0, 0], packed[0, 1] = pack([est_ref[z] for z in range(8)])
    pl.semaphore_wait(barrier, 1 + number(box(1)))
    spread_word(0)
    early, late = halo_copies(est_ref, 0)
    send(early + late)
    clear_borders()
    spectrum()
    fetches[1].wait()
    receive_strips(0)
    forward_inner(est_ref, 0)
    receive_edges(0)
    hear_word(0)
    spread_word(1)
    forward_edge(0)
    convolve(0, False)
    early, late = halo_copies(ratio_ref, 1)
    blurred = inverse((0,))
    ends = []
    for rows, at in ((head, slice(0, EDGE)), (tail, slice(EDGE, 2 * EDGE))):
        ratio = view_ref[:, rows, :] / blurred[:, at]
        ratio_ref[:, rows, :] = ratio
        ends.append(ratio)
    ends = jnp.concatenate(ends, axis=1)
    for side, strip in enumerate(pack([ends[z] for z in range(8)])):
        packed[1, side, head, :] = strip[:EDGE]
        packed[1, side, tail, :] = strip[EDGE:]
    send(early)
    ratio = view_ref[:, trunk, :] / inverse((1,))
    ratio_ref[:, trunk, :] = ratio
    for side, strip in enumerate(pack([ratio[z] for z in range(8)])):
        packed[1, side, trunk, :] = strip
    send(late)
    hear_word(1)
    spread_word(2)
    receive_strips(1)
    forward_inner(ratio_ref, 1)
    receive_edges(1)
    forward_edge(1)
    hear_word(2)
    spread_word(3)
    convolve(1, True)
    hear_word(3)
    pl.semaphore_signal(pair_sem, inc=1, device_id=device(0, 0, 1), device_id_type=MESH)
    correction = inverse((0, 1))
    pieces = [correction[:, :EDGE], correction[:, 2 * EDGE :], correction[:, EDGE : 2 * EDGE]]
    updated = est_ref[...] * jnp.concatenate(pieces, axis=1)
    column_sums = jnp.sum(updated, axis=0)
    halves = [jnp.sum(column_sums[32 * i : 32 * i + 32], axis=0, keepdims=True) for i in (0, 1)]
    source = lax.broadcasted_iota(jnp.int32, (384, 128), 0) % 128
    target = lax.broadcasted_iota(jnp.int32, (384, 128), 1)
    place = jnp.where(target == 4 * gy + source // 32, 2.0**-14, 0.0).astype(BF16)
    eight = jnp.concatenate(halves + [jnp.zeros((6, 128), F32)], axis=0)
    placed = dot(exact_triple(eight), place)
    tile_ref[...] = placed[0:1] + pltpu.roll(placed[1:2], 4 * ny, 1)
    me = gz * count + gx * ny + gy
    pl.semaphore_wait(pair_sem, 1)
    for dx, dy, dz in far:
        pltpu.make_async_remote_copy(
            src_ref=tile_ref,
            dst_ref=gathered.at[me],
            send_sem=all_send,
            recv_sem=all_recv,
            device_id=device(dx, dy, dz),
            device_id_type=MESH,
        ).start()
    gathered[me] = tile_ref[...]

    updated_ref[...] = updated
    for k in range(4):
        pool_a[k] = updated[2 * k] + updated[2 * k + 1]
    even, odd = pl.ds(0, ROWS // 2, stride=2), pl.ds(1, ROWS // 2, stride=2)
    level_one = [(pool_a[k, even, :] + pool_a[k, odd, :]) * 0.25 for k in range(4)]
    for k in (0, 1):
        pool_b[k] = level_one[2 * k] + level_one[2 * k + 1]
    even, odd = pl.ds(0, ROWS // 4, stride=2), pl.ds(1, ROWS // 4, stride=2)
    level_two = [(pool_b[k, even, :] + pool_b[k, odd, :]) * 0.25 for k in (0, 1)]
    pool_c[...] = level_two[0] + level_two[1]
    even, odd = pl.ds(0, ROWS // 8, stride=2), pl.ds(1, ROWS // 8, stride=2)
    level_three = (pool_c[even, :] + pool_c[odd, :]) * 0.25
    pool_d[0:8] = level_three
    pool_d[8:16] = jnp.zeros((8, 128), F32)
    even, odd = pl.ds(0, 8, stride=2), pl.ds(1, 8, stride=2)
    level_four = (pool_d[even, :] + pool_d[odd, :]) * 0.5
    plane_ref[0] = dot(exact_triple(level_four), tall_ref[1792:2176, 128:256])
    swap = pltpu.make_async_remote_copy(
        src_ref=plane_ref.at[0],
        dst_ref=plane_ref.at[1],
        send_sem=swap_send,
        recv_sem=swap_recv,
        device_id=device(0, 0, 1),
        device_id_type=MESH,
    )
    swap.start()
    third = dot(exact_triple(level_three), tall_ref[1792:2176, 0:128])
    three_ref[0] = third[:, :16]
    second = dot(exact_triple(jnp.concatenate(level_two, axis=0)), tall_ref[1408:1792, 128:256])
    for k in (0, 1):
        two_ref[k] = second[16 * k : 16 * k + 16, :32]
    full = dot(exact_triple(jnp.concatenate(level_one, axis=0)), tall_ref[1408:1792, 0:128])
    for k in range(4):
        one_ref[k] = full[32 * k : 32 * k + 32, :64]
    swap.wait_recv()
    fourth = (plane_ref[0] + plane_ref[1]) * 0.5
    four_ref[0] = fourth[:4, :8]

    finish_sends(0)
    finish_sends(1)
    swap.wait_send()
    pltpu.make_async_remote_copy(
        src_ref=own_ref,
        dst_ref=own_ref,
        send_sem=part_send,
        recv_sem=part_send,
        device_id=device(0, 0, 1),
        device_id_type=MESH,
    ).wait_send()
    others = gathered.at[pl.ds(0, 2 * count - 1)]
    everyone = pltpu.make_async_remote_copy(
        src_ref=others,
        dst_ref=others,
        send_sem=all_send,
        recv_sem=all_recv,
        device_id=device(0, 0, 1),
        device_id_type=MESH,
    )
    everyone.wait_send()
    everyone.wait_recv()
    strips = jnp.sum(gathered[...].reshape(2, nx, ny, 128), axis=(0, 2))
    five_ref[0, pl.ds(0, nx, stride=2), :] = strips[:, : 4 * ny]
    five_ref[0, pl.ds(1, nx, stride=2), :] = pltpu.roll(strips, 128 - 4 * ny, 1)[:, : 4 * ny]


def hand_over(*refs):
    sources, targets, sems = refs[:6], refs[6:12], refs[12]
    copies = [pltpu.make_async_copy(a, b, sems.at[k]) for k, (a, b) in enumerate(zip(sources, targets))]
    for copy in copies:
        copy.start()
    for copy in copies:
        copy.wait()


def local(nx, ny, estimate, view_data, psf_stack, view_index):
    vmem = pl.BlockSpec(memory_space=pltpu.VMEM)
    anywhere = pl.BlockSpec(memory_space=pl.ANY)
    shape = jax.ShapeDtypeStruct
    out_shape = (
        shape((8, 64, 128), F32),
        shape((4, 32, 64), F32),
        shape((2, 16, 32), F32),
        shape((1, 8, 16), F32),
        shape((1, 4, 8), F32),
        shape((1, 2 * nx, 4 * ny), F32),
    )
    constants = [jnp.asarray(t) for t in tables()]
    kept = [
        pltpu.with_memory_space_constraint(x, pltpu.HBM)
        for x in (estimate, view_data, psf_stack, *constants)
    ]
    results = pl.pallas_call(
        functools.partial(body, nx, ny),
        out_shape=out_shape,
        in_specs=[pl.BlockSpec(memory_space=pltpu.SMEM)]
        + [pl.BlockSpec(memory_space=pltpu.HBM)] * len(kept),
        out_specs=(vmem,) * 6,
        scratch_shapes=[
            pltpu.VMEM(estimate.shape, F32),
            pltpu.VMEM(view_data.shape, F32),
            pltpu.VMEM(psf_stack.shape, F32),
        ]
        + [pltpu.VMEM(c.shape, c.dtype) for c in constants]
        + [
            pltpu.VMEM((32, 32, 128), F32),
            pltpu.VMEM((32, 32, 256), F32),
            pltpu.VMEM((32, 3 * LX, 128), F32),
            pltpu.VMEM((8, ROWS, COLUMNS), F32),
            pltpu.VMEM((2, 2, 8, EDGE, 128), F32),
            pltpu.VMEM((2, 2, LX, 128), F32),
            pltpu.VMEM((2, 2, ROWS, 128), F32),
            pltpu.VMEM((2, 8, 2 * LX, 128), F32),
            pltpu.VMEM((2, 8, 2 * LX, 128), F32),
            pltpu.VMEM((8, 2 * LX, 128), F32),
            pltpu.VMEM((4, 64, 128), F32),
            pltpu.VMEM((2, 32, 128), F32),
            pltpu.VMEM((16, 128), F32),
            pltpu.VMEM((16, 128), F32),
            pltpu.VMEM((2, 8, 128), F32),
            pltpu.VMEM((1, 128), F32),
            pltpu.VMEM((2 * nx * ny, 1, 128), F32),
            pltpu.SemaphoreType.DMA((len(kept),)),
            pltpu.SemaphoreType.DMA((2,)),
            pltpu.SemaphoreType.DMA((2, 2)),
            pltpu.SemaphoreType.DMA,
            pltpu.SemaphoreType.DMA((2, 2)),
            pltpu.SemaphoreType.DMA,
            pltpu.SemaphoreType.DMA,
            pltpu.SemaphoreType.DMA,
            pltpu.SemaphoreType.DMA,
            pltpu.SemaphoreType.REGULAR((4,)),
            pltpu.SemaphoreType.REGULAR,
        ],
        compiler_params=pltpu.CompilerParams(
            collective_id=0, has_side_effects=True, vmem_limit_bytes=32 << 20
        ),
    )(view_index, *kept)
    return pl.pallas_call(
        hand_over,
        out_shape=out_shape,
        in_specs=[vmem] * 6,
        out_specs=(anywhere,) * 6,
        scratch_shapes=[pltpu.SemaphoreType.DMA((6,))],
        compiler_params=pltpu.CompilerParams(vmem_limit_bytes=4 << 20),
    )(*results)


def solution(mesh):
    spread = P("gz", "gx", "gy")
    return jax.shard_map(
        functools.partial(local, mesh.shape["gx"], mesh.shape["gy"]),
        mesh=mesh,
        in_specs=(spread, spread, P(), P()),
        out_specs=(spread, spread, spread, spread, P(None, "gx", "gy"), P()),
        check_vma=False,
    )
```

```python
import functools

import jax
import jax.numpy as jnp
import numpy as np
from jax import lax
from jax.experimental import pallas as pl
from jax.experimental.pallas import tpu as pltpu
from jax.sharding import PartitionSpec as P

MESH = pl.DeviceIdType.MESH
HALO = 15
EDGE = 16
ROWS, COLUMNS = 64, 128
LX, LY = ROWS + 2 * EDGE, COLUMNS + 2 * EDGE
HALF = LY // 2 + 1
TAPS = 2 * HALO + 1
BF16, F32 = jnp.bfloat16, jnp.float32


def parts_of(table):
    table = np.asarray(table, np.float64)
    high = table.astype(np.float32).astype(BF16)
    low = (table - high.astype(np.float64)).astype(np.float32).astype(BF16)
    return high, low


def stacked(table):
    high, low = parts_of(table)
    return np.concatenate([high, low, high], axis=0)


def beside(table):
    high, low = parts_of(table)
    return np.concatenate([high, high, low], axis=1)


def column_table(positions):
    angle = 2.0 * np.pi / LY * np.outer(positions, np.arange(HALF))
    table = np.zeros((len(positions), 256))
    table[:, :HALF] = np.cos(angle)
    table[:, 128 : 128 + HALF] = -np.sin(angle)
    return table


def row_table(positions):
    angle = 2.0 * np.pi / LX * np.outer(np.arange(LX), positions)
    c, s = np.cos(angle), np.sin(angle)
    return np.block([[c, s], [-s, c]])


def tables():
    inner = column_table(EDGE + np.arange(COLUMNS))
    left = column_table(np.arange(EDGE))
    right = column_table(LY - EDGE + np.arange(EDGE))
    columns = stacked(np.concatenate([inner] + [left, right] * 4))
    inner_rows = beside(row_table(EDGE + np.arange(ROWS)))
    edge_rows = beside(row_table(np.concatenate([np.arange(EDGE), LX - EDGE + np.arange(EDGE)])))
    kept = np.arange(ROWS)
    halves = []
    for part in (np.concatenate([kept[:EDGE], kept[-EDGE:]]), kept[EDGE:-EDGE]):
        angle = 2.0 * np.pi / LX * np.outer(EDGE + part, np.arange(LX))
        c, s = np.cos(angle), np.sin(angle)
        halves.append(beside(np.block([[c, -s], [s, c]])))
    rows_back = np.concatenate(halves)
    angle = 2.0 * np.pi / LY * np.outer(np.arange(HALF), EDGE + np.arange(COLUMNS))
    weight = np.where(np.isin(np.arange(HALF), (0, LY // 2)), 1.0, 2.0)[:, None] / (LX * LY)
    back = np.zeros((256, COLUMNS))
    back[:HALF] = weight * np.cos(angle)
    back[128 : 128 + HALF] = -weight * np.sin(angle)
    high, low = parts_of(back)
    columns_back = np.block([[high, low], [high, np.zeros_like(low)]])
    taps = column_table(np.concatenate([np.arange(TAPS) - HALO, [0]]))
    taps[TAPS] = 0.0
    tap_columns = np.concatenate([stacked(taps), np.zeros((32, 256), BF16)], axis=0)
    tap_rows_table = row_table(np.concatenate([np.arange(TAPS) - HALO, [0]]))
    tap_rows_table[:, TAPS] = 0.0
    tap_rows_table[:, 32 + TAPS] = 0.0
    tap_rows = beside(tap_rows_table)
    pools = np.zeros((128, 512), np.float32)
    for level in range(4):
        step = 2 ** (level + 1)
        for column in range(COLUMNS):
            pools[column, 128 * level + column // step] = 1.0 / step
    pools = np.concatenate([pools] * 3, axis=0).astype(BF16)
    tall = np.concatenate([columns, columns_back, tap_columns, pools[:, :256], pools[:, 256:]])
    wide = np.zeros((2 * LX, 1536), BF16)
    wide[:, :384] = inner_rows
    wide[:, 384:576] = edge_rows
    wide[:, 640:832] = tap_rows
    wide[: 2 * ROWS, 896:1472] = rows_back
    return tall, wide


def two(x):
    high = x.astype(BF16)
    return high, (x - high.astype(F32)).astype(BF16)


def dot(a, b):
    return jnp.dot(a, b, preferred_element_type=F32)


def left_triple(x):
    high, low = two(x)
    return jnp.concatenate([high, high, low], axis=1)


def right_triple(x):
    high, low = two(x)
    return jnp.concatenate([high, low, high], axis=0)


def exact_triple(x):
    high = x.astype(BF16)
    rest = x - high.astype(F32)
    middle = rest.astype(BF16)
    low = (rest - middle.astype(F32)).astype(BF16)
    return jnp.concatenate([high, middle, low], axis=1)


def body(nx, ny, index_ref, *refs):
    inputs, refs = refs[:5], refs[5:]
    updated_ref, one_ref, two_ref, three_ref, four_ref, five_ref = refs[:6]
    held, refs = refs[6:11], refs[11:]
    est_ref, view_ref, psf_ref, tall_ref, wide_ref = held
    (
        taps_ref,
        tap_half_ref,
        kernel_ref,
        ratio_ref,
        edge_rows,
        edge_columns,
        packed,
        own_ref,
        other_ref,
        product_ref,
        pool_a,
        pool_b,
        pool_c,
        pool_d,
        plane_ref,
        tile_ref,
        gathered,
        local_sem,
        send_sem,
        recv_sem,
        part_send,
        part_recv,
        swap_send,
        swap_recv,
        all_send,
        all_recv,
        word_sem,
        pair_sem,
    ) = refs
    gx, gy, gz = lax.axis_index("gx"), lax.axis_index("gy"), lax.axis_index("gz")

    def turned(at, offset, length):
        offset = offset % length
        if offset == 0:
            return at
        return jnp.where(at >= length - offset, at + offset - length, at + offset)

    def device(dx, dy, dz=0):
        return {"gx": turned(gx, dx, nx), "gy": turned(gy, dy, ny), "gz": turned(gz, dz, 2)}

    fetches = [
        pltpu.make_async_copy(source, target, local_sem.at[k])
        for k, (source, target) in enumerate(zip(inputs, held))
    ]
    fetches[0].start()

    count = nx * ny

    def there(dx, dy):
        tests = []
        if dx:
            tests.append(gx >= -dx if dx < 0 else gx < nx - dx)
        if dy:
            tests.append(gy >= -dy if dy < 0 else gy < ny - dy)
        return tests[0] if len(tests) == 1 else tests[0] & tests[1]

    def box(reach):
        steps = (-reach, 0, reach)
        return [(dx, dy) for dx in steps for dy in steps if (dx, dy) != (0, 0)]

    def hops(offset):
        dx, dy, dz = offset
        ring = lambda k, n: min(k, n - k)
        return ring(dx % 4, 4) + ring(dx // 4, nx // 4) + ring(dy, ny) + 0.5 * dz

    every = ((dx, dy, dz) for dx in range(nx) for dy in range(ny) for dz in (0, 1))
    far = sorted(every, key=hops, reverse=True)[:-1]

    def signal_all(sem, offsets):
        for dx, dy in offsets:

            @pl.when(there(dx, dy))
            def _():
                pl.semaphore_signal(sem, inc=1, device_id=device(dx, dy), device_id_type=MESH)

    def number(offsets):
        return sum(jnp.where(there(dx, dy), 1, 0) for dx, dy in offsets)

    rounds = [box(1), box(2), box(4), [(-8, 0), (8, 0)]]

    def spread_word(k):
        signal_all(word_sem.at[k], rounds[k])

    def hear_word(k):
        pl.semaphore_wait(word_sem.at[k], number(rounds[k]))

    barrier = pltpu.get_barrier_semaphore()
    pl.semaphore_signal(barrier, inc=1, device_id=device(0, 0, 1), device_id_type=MESH)
    signal_all(barrier, box(1))
    for k in (4, 3, 2, 1):
        fetches[k].start()

    def pack(planes):
        lane = lax.broadcasted_iota(jnp.int32, planes[0].shape, 1)
        to_right = jnp.zeros(planes[0].shape, F32)
        to_left = jnp.zeros(planes[0].shape, F32)
        for z, plane in enumerate(planes):
            base = (z % 4) * 32
            low, high = (base, base + EDGE) if z < 4 else (base + EDGE, base)
            shift = (low - (COLUMNS - EDGE)) % 128
            rolled = pltpu.roll(plane, shift, 1) if shift else plane
            to_right = jnp.where((lane >= low) & (lane < low + EDGE), rolled, to_right)
            rolled = pltpu.roll(plane, high, 1) if high else plane
            to_left = jnp.where((lane >= high) & (lane < high + EDGE), rolled, to_left)
        return to_right, to_left

    middle, top, bottom = pl.ds(EDGE, ROWS), pl.ds(0, EDGE), pl.ds(EDGE + ROWS, EDGE)
    head, tail, trunk = pl.ds(0, EDGE), pl.ds(ROWS - EDGE, EDGE), pl.ds(EDGE, ROWS - 2 * EDGE)

    def send(copies):
        for copy, ahead in copies:
            pl.when(ahead)(copy.start)

    def wait_units(sem, units, send):
        for last_x in (True, False):
            for last_y in (True, False):
                end_x = (gx == 0) | (gx == nx - 1)
                end_y = (gy == 0) | (gy == ny - 1)
                here = (end_x if last_x else ~end_x) & (end_y if last_y else ~end_y)
                total = units(1 if last_x else 2, 1 if last_y else 2)
                slab = kernel_ref.at[pl.ds(0, 2), pl.ds(0, total * EDGE // 2)]
                copy = pltpu.make_async_remote_copy(
                    src_ref=slab,
                    dst_ref=slab,
                    send_sem=sem,
                    recv_sem=sem,
                    device_id=device(0, 0, 1),
                    device_id_type=MESH,
                )
                pl.when(here)(copy.wait_send if send else copy.wait_recv)

    def receive_strips(turn):
        wait_units(recv_sem.at[turn, 1], lambda sx, sy: 4 * sy, False)

    def receive_edges(turn):
        wait_units(recv_sem.at[turn, 0], lambda sx, sy: sx * (8 + sy), False)

    def finish_sends(turn):
        wait_units(send_sem.at[turn], lambda sx, sy: 4 * sy + sx * (8 + sy), True)

    def halo_copies(source, turn):
        def copy(src, dst, at, dx, dy):
            sent = pltpu.make_async_remote_copy(
                src_ref=src,
                dst_ref=dst,
                send_sem=send_sem.at[turn],
                recv_sem=recv_sem.at[turn, at],
                device_id=device(dx, dy),
                device_id_type=MESH,
            )
            return sent, there(dx, dy)

        right, left = packed.at[turn, 0], packed.at[turn, 1]
        from_left, from_right = edge_columns.at[turn, 0], edge_columns.at[turn, 1]
        early = [
            copy(source.at[:, tail, :], edge_rows.at[turn, 0], 0, 1, 0),
            copy(source.at[:, head, :], edge_rows.at[turn, 1], 0, -1, 0),
            copy(right.at[tail, :], from_left.at[top, :], 0, 1, 1),
            copy(right.at[head, :], from_left.at[bottom, :], 0, -1, 1),
            copy(left.at[tail, :], from_right.at[top, :], 0, 1, -1),
            copy(left.at[head, :], from_right.at[bottom, :], 0, -1, -1),
        ]
        for rows in (head, tail, trunk):
            into = pl.ds(rows.start + EDGE, rows.size)
            early.append(copy(right.at[rows, :], from_left.at[into, :], 1, 0, 1))
            early.append(copy(left.at[rows, :], from_right.at[into, :], 1, 0, -1))
        return early[:-2], early[-2:]

    def clear_borders():
        rows, columns = jnp.zeros((8, EDGE, 128), F32), jnp.zeros((LX, 128), F32)
        for end, at, part in ((gx == 0, 0, top), (gx == nx - 1, 1, bottom)):

            @pl.when(end)
            def _():
                for turn in (0, 1):
                    edge_rows[turn, at] = rows
                    for side in (0, 1):
                        edge_columns[turn, side, part, :] = columns[:EDGE]

        for end, side in ((gy == 0, 0), (gy == ny - 1, 1)):

            @pl.when(end)
            def _():
                for turn in (0, 1):
                    edge_columns[turn, side] = columns

    def partner_copy(turn, group):
        planes = pl.ds(4 * group, 4)
        return pltpu.make_async_remote_copy(
            src_ref=own_ref.at[turn, planes],
            dst_ref=other_ref.at[turn, planes],
            send_sem=part_send,
            recv_sem=part_recv.at[turn, group],
            device_id=device(0, 0, 1),
            device_id_type=MESH,
        )

    def transform(turn, height, plane_of, left, right, rows_table, adding):
        lane = lax.broadcasted_iota(jnp.int32, (height, 128), 1)
        even = (lane & EDGE) == 0
        mixed = (
            jnp.where(even, left, right),
            jnp.where(even, pltpu.roll(left, 128 - EDGE, 1), pltpu.roll(right, EDGE, 1)),
        )
        rows = []
        for z in range(8):
            j = 32 * (z % 4)
            side = jnp.where((lane >= j) & (lane < j + 32), mixed[z // 4], 0.0)
            rows.append(jnp.concatenate([plane_of(z), side], axis=1))
        half = dot(left_triple(jnp.concatenate(rows, axis=0)), tall_ref[0:768, :])
        for group in (0, 1):
            whole = []
            for z in (4 * group, 4 * group + 2):
                a = half[z * height : (z + 1) * height]
                b = half[(z + 1) * height : (z + 2) * height]
                joint = jnp.concatenate(
                    [
                        jnp.concatenate([a[:, :128], b[:, :128]], axis=1),
                        jnp.concatenate([a[:, 128:], b[:, 128:]], axis=1),
                    ],
                    axis=0,
                )
                full = dot(wide_ref[:, rows_table], right_triple(joint))
                whole += [full[:, :128], full[:, 128:]]
            for z, part in enumerate(whole, 4 * group):
                own_ref[turn, z] = own_ref[turn, z] + part if adding else part
            if adding:
                partner_copy(turn, group).start()

    def forward_inner(source, turn):
        left, right = edge_columns[turn, 0, middle, :], edge_columns[turn, 1, middle, :]
        transform(turn, ROWS, lambda z: source[z], left, right, slice(0, 384), False)

    def forward_edge(turn):
        def both(a, b):
            return jnp.concatenate([a, b], axis=0)

        left, right = [
            both(edge_columns[turn, side, top, :], edge_columns[turn, side, bottom, :])
            for side in (0, 1)
        ]

        def plane_of(z):
            return both(edge_rows[turn, 0, z], edge_rows[turn, 1, z])

        transform(turn, 2 * EDGE, plane_of, left, right, slice(384, 576), True)

    def depth(x_ref, turn, base, mirrored, adding, planes):
        def blocks(step, carry):
            block(2 * step)
            block(2 * step + 1)
            return carry

        def block(step):
            at = pl.multiple_of(step * 8, 8)
            re, im = pl.ds(at, 8), pl.ds(pl.multiple_of(at + LX, 8), 8)
            xr = {z: x_ref[turn, z, re, :] for z in planes}
            xi = {z: x_ref[turn, z, im, :] for z in planes}
            if adding:
                yr = [product_ref[z, re, :] for z in range(8)]
                yi = [product_ref[z, im, :] for z in range(8)]
            else:
                yr, yi = [None] * 8, [None] * 8
            xs = {z: xr[z] + xi[z] for z in planes}
            sums = [[None] * 8 for _ in range(3)]
            for d in range(-7, 8):
                taps = [kernel_ref[base + d, pl.ds(at + LX * k, 8), :] for k in range(3)]
                values = (xs, xi, xr) if mirrored else (xs, xr, xi)
                for out in range(8):
                    z = out + d if mirrored else out - d
                    if z not in planes:
                        continue
                    for k in range(3):
                        term = taps[k] * values[k][z]
                        sums[k][out] = term if sums[k][out] is None else sums[k][out] + term
            for z in range(8):
                one, two_, three = (sums[k][z] for k in range(3))
                r = one + two_ if mirrored else one - three
                i = one - three if mirrored else one + two_
                yr[z] = r if yr[z] is None else yr[z] + r
                yi[z] = i if yi[z] is None else yi[z] + i
            for z in range(8):
                product_ref[z, re, :] = yr[z]
                product_ref[z, im, :] = yi[z]

        lax.fori_loop(0, LX // 16, blocks, 0)

    def inverse(parts):
        rows = []
        table = slice(64 * parts[0], 64 * parts[-1] + 64)
        for z in range(0, 8, 2):
            joint = jnp.concatenate([product_ref[z], product_ref[z + 1]], axis=1)
            half = dot(wide_ref[table, 896:1472], right_triple(joint))
            for b in (0, 1):
                lanes = slice(128 * b, 128 * b + 128)
                for k in range(len(parts)):
                    re, im = half[64 * k : 64 * k + 32, lanes], half[64 * k + 32 : 64 * k + 64, lanes]
                    rows.append(jnp.concatenate([re, im], axis=1))
        full = dot(jnp.concatenate(two(jnp.concatenate(rows, axis=0)), axis=1), tall_ref[768:1280, :])
        return (full[:, :COLUMNS] + full[:, COLUMNS:]).reshape(8, 32 * len(parts), COLUMNS)

    def convolve(turn, mirrored):
        depth(own_ref, turn, HALO, mirrored, False, range(8))
        base = HALO + 8 - 16 * gz if mirrored else HALO - 8 + 16 * gz
        for group in (0, 1):
            partner_copy(turn, group).wait_recv()
            depth(other_ref, turn, base, mirrored, True, range(4 * group, 4 * group + 4))

    def spectrum():
        for k in (4, 3, 2):
            fetches[k].wait()
        view = index_ref[0]
        taps_ref[...] = jnp.zeros((32, 32, 128), F32)

        taps_ref[0:TAPS, 0:TAPS, 0:TAPS] = psf_ref[view]
        total = jnp.sum(jnp.sum(taps_ref[...], axis=0), axis=(0, 1), keepdims=True)
        scale = 1.0 / total

        for step in range(4):
            x = taps_ref[8 * step : 8 * step + 8].reshape(256, 128) * scale
            high = x.astype(BF16).astype(F32)
            low = x - high
            joint = high + pltpu.roll(high, 32, 1) + pltpu.roll(low, 64, 1)
            half = dot(joint.astype(BF16), tall_ref[1280:1408, :])
            tap_half_ref[8 * step : 8 * step + 8] = half.reshape(8, 32, 256)

        def rows(step, carry):
            for pair in range(4):
                z = 8 * step + 2 * pair
                a, b = tap_half_ref[z], tap_half_ref[z + 1]
                joint = jnp.concatenate(
                    [
                        jnp.concatenate([a[:, :128], b[:, :128]], axis=1),
                        jnp.concatenate([a[:, 128:], b[:, 128:]], axis=1),
                    ],
                    axis=0,
                )
                full = dot(wide_ref[:, 640:832], right_triple(joint))
                for b in (0, 1):
                    re = full[:LX, 128 * b : 128 * b + 128]
                    im = full[LX:, 128 * b : 128 * b + 128]
                    kernel_ref[z + b, 0:LX] = re
                    kernel_ref[z + b, LX : 2 * LX] = im - re
                    kernel_ref[z + b, 2 * LX :] = im + re
            return carry

        lax.fori_loop(0, 4, rows, 0)

    fetches[0].wait()
    packed[0, 0], packed[0, 1] = pack([est_ref[z] for z in range(8)])
    pl.semaphore_wait(barrier, 1 + number(box(1)))
    spread_word(0)
    early, late = halo_copies(est_ref, 0)
    send(early + late)
    clear_borders()
    spectrum()
    fetches[1].wait()
    receive_strips(0)
    forward_inner(est_ref, 0)
    receive_edges(0)
    hear_word(0)
    spread_word(1)
    forward_edge(0)
    convolve(0, False)
    early, late = halo_copies(ratio_ref, 1)
    blurred = inverse((0,))
    ends = []
    for rows, at in ((head, slice(0, EDGE)), (tail, slice(EDGE, 2 * EDGE))):
        ratio = view_ref[:, rows, :] / blurred[:, at]
        ratio_ref[:, rows, :] = ratio
        ends.append(ratio)
    ends = jnp.concatenate(ends, axis=1)
    for side, strip in enumerate(pack([ends[z] for z in range(8)])):
        packed[1, side, head, :] = strip[:EDGE]
        packed[1, side, tail, :] = strip[EDGE:]
    send(early)
    ratio = view_ref[:, trunk, :] / inverse((1,))
    ratio_ref[:, trunk, :] = ratio
    for side, strip in enumerate(pack([ratio[z] for z in range(8)])):
        packed[1, side, trunk, :] = strip
    send(late)
    hear_word(1)
    spread_word(2)
    receive_strips(1)
    forward_inner(ratio_ref, 1)
    receive_edges(1)
    forward_edge(1)
    hear_word(2)
    spread_word(3)
    convolve(1, True)
    hear_word(3)
    pl.semaphore_signal(pair_sem, inc=1, device_id=device(0, 0, 1), device_id_type=MESH)
    correction = inverse((0, 1))
    pieces = [correction[:, :EDGE], correction[:, 2 * EDGE :], correction[:, EDGE : 2 * EDGE]]
    updated = est_ref[...] * jnp.concatenate(pieces, axis=1)
    column_sums = jnp.sum(updated, axis=0)
    halves = [jnp.sum(column_sums[32 * i : 32 * i + 32], axis=0, keepdims=True) for i in (0, 1)]
    source = lax.broadcasted_iota(jnp.int32, (384, 128), 0) % 128
    target = lax.broadcasted_iota(jnp.int32, (384, 128), 1)
    place = jnp.where(target == 4 * gy + source // 32, 2.0**-14, 0.0).astype(BF16)
    eight = jnp.concatenate(halves + [jnp.zeros((6, 128), F32)], axis=0)
    placed = dot(exact_triple(eight), place)
    tile_ref[...] = placed[0:1] + pltpu.roll(placed[1:2], 4 * ny, 1)
    me = gz * count + gx * ny + gy
    pl.semaphore_wait(pair_sem, 1)
    lead = (-gx, -gy, 1 - gz)
    lead = [jnp.where(d < 0, d + n, d) for d, n in zip(lead, (nx, ny, 2))]
    opening = far[0]
    alone = (lead[0] == 0) & (lead[1] == 0) & (lead[2] == 0)

    def wrapped(at, offset, length):
        moved = at + offset
        return jnp.where(moved >= length, moved - length, moved)

    for k, offset in enumerate(far):
        if k == 0:
            swapped = [jnp.where(alone, o, d) for o, d in zip(opening, lead)]
        else:
            same = (lead[0] == offset[0]) & (lead[1] == offset[1]) & (lead[2] == offset[2])
            swapped = [jnp.where(same, o, d) for o, d in zip(opening, offset)]
        pltpu.make_async_remote_copy(
            src_ref=tile_ref,
            dst_ref=gathered.at[me],
            send_sem=all_send,
            recv_sem=all_recv,
            device_id={
                "gx": wrapped(gx, swapped[0], nx),
                "gy": wrapped(gy, swapped[1], ny),
                "gz": wrapped(gz, swapped[2], 2),
            },
            device_id_type=MESH,
        ).start()
    gathered[me] = tile_ref[...]

    updated_ref[...] = updated
    for k in range(4):
        pool_a[k] = updated[2 * k] + updated[2 * k + 1]
    even, odd = pl.ds(0, ROWS // 2, stride=2), pl.ds(1, ROWS // 2, stride=2)
    level_one = [(pool_a[k, even, :] + pool_a[k, odd, :]) * 0.25 for k in range(4)]
    for k in (0, 1):
        pool_b[k] = level_one[2 * k] + level_one[2 * k + 1]
    even, odd = pl.ds(0, ROWS // 4, stride=2), pl.ds(1, ROWS // 4, stride=2)
    level_two = [(pool_b[k, even, :] + pool_b[k, odd, :]) * 0.25 for k in (0, 1)]
    pool_c[...] = level_two[0] + level_two[1]
    even, odd = pl.ds(0, ROWS // 8, stride=2), pl.ds(1, ROWS // 8, stride=2)
    level_three = (pool_c[even, :] + pool_c[odd, :]) * 0.25
    pool_d[0:8] = level_three
    pool_d[8:16] = jnp.zeros((8, 128), F32)
    even, odd = pl.ds(0, 8, stride=2), pl.ds(1, 8, stride=2)
    level_four = (pool_d[even, :] + pool_d[odd, :]) * 0.5
    plane_ref[0] = dot(exact_triple(level_four), tall_ref[1792:2176, 128:256])
    swap = pltpu.make_async_remote_copy(
        src_ref=plane_ref.at[0],
        dst_ref=plane_ref.at[1],
        send_sem=swap_send,
        recv_sem=swap_recv,
        device_id=device(0, 0, 1),
        device_id_type=MESH,
    )
    swap.start()
    third = dot(exact_triple(level_three), tall_ref[1792:2176, 0:128])
    three_ref[0] = third[:, :16]
    second = dot(exact_triple(jnp.concatenate(level_two, axis=0)), tall_ref[1408:1792, 128:256])
    for k in (0, 1):
        two_ref[k] = second[16 * k : 16 * k + 16, :32]
    full = dot(exact_triple(jnp.concatenate(level_one, axis=0)), tall_ref[1408:1792, 0:128])
    for k in range(4):
        one_ref[k] = full[32 * k : 32 * k + 32, :64]
    swap.wait_recv()
    fourth = (plane_ref[0] + plane_ref[1]) * 0.5
    four_ref[0] = fourth[:4, :8]

    finish_sends(0)
    finish_sends(1)
    swap.wait_send()
    pltpu.make_async_remote_copy(
        src_ref=own_ref,
        dst_ref=own_ref,
        send_sem=part_send,
        recv_sem=part_send,
        device_id=device(0, 0, 1),
        device_id_type=MESH,
    ).wait_send()
    others = gathered.at[pl.ds(0, 2 * count - 1)]
    everyone = pltpu.make_async_remote_copy(
        src_ref=others,
        dst_ref=others,
        send_sem=all_send,
        recv_sem=all_recv,
        device_id=device(0, 0, 1),
        device_id_type=MESH,
    )
    everyone.wait_send()
    everyone.wait_recv()
    strips = jnp.sum(gathered[...].reshape(2, nx, ny, 128), axis=(0, 2))
    five_ref[0, pl.ds(0, nx, stride=2), :] = strips[:, : 4 * ny]
    five_ref[0, pl.ds(1, nx, stride=2), :] = pltpu.roll(strips, 128 - 4 * ny, 1)[:, : 4 * ny]


def hand_over(*refs):
    sources, targets, sems = refs[:6], refs[6:12], refs[12]
    copies = [pltpu.make_async_copy(a, b, sems.at[k]) for k, (a, b) in enumerate(zip(sources, targets))]
    for copy in copies:
        copy.start()
    for copy in copies:
        copy.wait()


def local(nx, ny, estimate, view_data, psf_stack, view_index):
    vmem = pl.BlockSpec(memory_space=pltpu.VMEM)
    anywhere = pl.BlockSpec(memory_space=pl.ANY)
    shape = jax.ShapeDtypeStruct
    out_shape = (
        shape((8, 64, 128), F32),
        shape((4, 32, 64), F32),
        shape((2, 16, 32), F32),
        shape((1, 8, 16), F32),
        shape((1, 4, 8), F32),
        shape((1, 2 * nx, 4 * ny), F32),
    )
    constants = [jnp.asarray(t) for t in tables()]
    kept = [
        pltpu.with_memory_space_constraint(x, pltpu.HBM)
        for x in (estimate, view_data, psf_stack, *constants)
    ]
    results = pl.pallas_call(
        functools.partial(body, nx, ny),
        out_shape=out_shape,
        in_specs=[pl.BlockSpec(memory_space=pltpu.SMEM)]
        + [pl.BlockSpec(memory_space=pltpu.HBM)] * len(kept),
        out_specs=(vmem,) * 6,
        scratch_shapes=[
            pltpu.VMEM(estimate.shape, F32),
            pltpu.VMEM(view_data.shape, F32),
            pltpu.VMEM(psf_stack.shape, F32),
        ]
        + [pltpu.VMEM(c.shape, c.dtype) for c in constants]
        + [
            pltpu.VMEM((32, 32, 128), F32),
            pltpu.VMEM((32, 32, 256), F32),
            pltpu.VMEM((32, 3 * LX, 128), F32),
            pltpu.VMEM((8, ROWS, COLUMNS), F32),
            pltpu.VMEM((2, 2, 8, EDGE, 128), F32),
            pltpu.VMEM((2, 2, LX, 128), F32),
            pltpu.VMEM((2, 2, ROWS, 128), F32),
            pltpu.VMEM((2, 8, 2 * LX, 128), F32),
            pltpu.VMEM((2, 8, 2 * LX, 128), F32),
            pltpu.VMEM((8, 2 * LX, 128), F32),
            pltpu.VMEM((4, 64, 128), F32),
            pltpu.VMEM((2, 32, 128), F32),
            pltpu.VMEM((16, 128), F32),
            pltpu.VMEM((16, 128), F32),
            pltpu.VMEM((2, 8, 128), F32),
            pltpu.VMEM((1, 128), F32),
            pltpu.VMEM((2 * nx * ny, 1, 128), F32),
            pltpu.SemaphoreType.DMA((len(kept),)),
            pltpu.SemaphoreType.DMA((2,)),
            pltpu.SemaphoreType.DMA((2, 2)),
            pltpu.SemaphoreType.DMA,
            pltpu.SemaphoreType.DMA((2, 2)),
            pltpu.SemaphoreType.DMA,
            pltpu.SemaphoreType.DMA,
            pltpu.SemaphoreType.DMA,
            pltpu.SemaphoreType.DMA,
            pltpu.SemaphoreType.REGULAR((4,)),
            pltpu.SemaphoreType.REGULAR,
        ],
        compiler_params=pltpu.CompilerParams(
            collective_id=0, has_side_effects=True, vmem_limit_bytes=32 << 20
        ),
    )(view_index, *kept)
    return pl.pallas_call(
        hand_over,
        out_shape=out_shape,
        in_specs=[vmem] * 6,
        out_specs=(anywhere,) * 6,
        scratch_shapes=[pltpu.SemaphoreType.DMA((6,))],
        compiler_params=pltpu.CompilerParams(vmem_limit_bytes=4 << 20),
    )(*results)


def solution(mesh):
    spread = P("gz", "gx", "gy")
    return jax.shard_map(
        functools.partial(local, mesh.shape["gx"], mesh.shape["gy"]),
        mesh=mesh,
        in_specs=(spread, spread, P(), P()),
        out_specs=(spread, spread, spread, spread, P(None, "gx", "gy"), P()),
        check_vma=False,
    )
```

```python
import functools

import jax
import jax.numpy as jnp
import numpy as np
from jax import lax
from jax.experimental import pallas as pl
from jax.experimental.pallas import tpu as pltpu
from jax.sharding import PartitionSpec as P

MESH = pl.DeviceIdType.MESH
HALO = 15
EDGE = 16
ROWS, COLUMNS = 64, 128
LX, LY = ROWS + 2 * EDGE, COLUMNS + 2 * EDGE
HALF = LY // 2 + 1
TAPS = 2 * HALO + 1
BF16, F32 = jnp.bfloat16, jnp.float32


def parts_of(table):
    table = np.asarray(table, np.float64)
    high = table.astype(np.float32).astype(BF16)
    low = (table - high.astype(np.float64)).astype(np.float32).astype(BF16)
    return high, low


def stacked(table):
    high, low = parts_of(table)
    return np.concatenate([high, low, high], axis=0)


def beside(table):
    high, low = parts_of(table)
    return np.concatenate([high, high, low], axis=1)


def column_table(positions):
    angle = 2.0 * np.pi / LY * np.outer(positions, np.arange(HALF))
    table = np.zeros((len(positions), 256))
    table[:, :HALF] = np.cos(angle)
    table[:, 128 : 128 + HALF] = -np.sin(angle)
    return table


def row_table(positions):
    angle = 2.0 * np.pi / LX * np.outer(np.arange(LX), positions)
    c, s = np.cos(angle), np.sin(angle)
    return np.block([[c, s], [-s, c]])


def tables():
    inner = column_table(EDGE + np.arange(COLUMNS))
    left = column_table(np.arange(EDGE))
    right = column_table(LY - EDGE + np.arange(EDGE))
    columns = stacked(np.concatenate([inner] + [left, right] * 4))
    inner_rows = beside(row_table(EDGE + np.arange(ROWS)))
    edge_rows = beside(row_table(np.concatenate([np.arange(EDGE), LX - EDGE + np.arange(EDGE)])))
    kept = np.arange(ROWS)
    halves = []
    for part in (np.concatenate([kept[:EDGE], kept[-EDGE:]]), kept[EDGE:-EDGE]):
        angle = 2.0 * np.pi / LX * np.outer(EDGE + part, np.arange(LX))
        c, s = np.cos(angle), np.sin(angle)
        halves.append(beside(np.block([[c, -s], [s, c]])))
    rows_back = np.concatenate(halves)
    angle = 2.0 * np.pi / LY * np.outer(np.arange(HALF), EDGE + np.arange(COLUMNS))
    weight = np.where(np.isin(np.arange(HALF), (0, LY // 2)), 1.0, 2.0)[:, None] / (LX * LY)
    back = np.zeros((256, COLUMNS))
    back[:HALF] = weight * np.cos(angle)
    back[128 : 128 + HALF] = -weight * np.sin(angle)
    high, low = parts_of(back)
    columns_back = np.block([[high, low], [high, np.zeros_like(low)]])
    taps = column_table(np.concatenate([np.arange(TAPS) - HALO, [0]]))
    taps[TAPS] = 0.0
    tap_columns = np.concatenate([stacked(taps), np.zeros((32, 256), BF16)], axis=0)
    tap_rows_table = row_table(np.concatenate([np.arange(TAPS) - HALO, [0]]))
    tap_rows_table[:, TAPS] = 0.0
    tap_rows_table[:, 32 + TAPS] = 0.0
    tap_rows = beside(tap_rows_table)
    pools = np.zeros((128, 512), np.float32)
    for level in range(4):
        step = 2 ** (level + 1)
        for column in range(COLUMNS):
            pools[column, 128 * level + column // step] = 1.0 / step
    pools = np.concatenate([pools] * 3, axis=0).astype(BF16)
    tall = np.concatenate([columns, columns_back, tap_columns, pools[:, :256], pools[:, 256:]])
    wide = np.zeros((2 * LX, 1536), BF16)
    wide[:, :384] = inner_rows
    wide[:, 384:576] = edge_rows
    wide[:, 640:832] = tap_rows
    wide[: 2 * ROWS, 896:1472] = rows_back
    return tall, wide


def two(x):
    high = x.astype(BF16)
    return high, (x - high.astype(F32)).astype(BF16)


def dot(a, b):
    return jnp.dot(a, b, preferred_element_type=F32)


def left_triple(x):
    high, low = two(x)
    return jnp.concatenate([high, high, low], axis=1)


def right_triple(x):
    high, low = two(x)
    return jnp.concatenate([high, low, high], axis=0)


def exact_triple(x):
    high = x.astype(BF16)
    rest = x - high.astype(F32)
    middle = rest.astype(BF16)
    low = (rest - middle.astype(F32)).astype(BF16)
    return jnp.concatenate([high, middle, low], axis=1)


def body(nx, ny, index_ref, *refs):
    inputs, refs = refs[:5], refs[5:]
    updated_ref, one_ref, two_ref, three_ref, four_ref, five_ref = refs[:6]
    held, refs = refs[6:11], refs[11:]
    est_ref, view_ref, psf_ref, tall_ref, wide_ref = held
    (
        taps_ref,
        tap_half_ref,
        kernel_ref,
        ratio_ref,
        edge_rows,
        edge_columns,
        packed,
        own_ref,
        other_ref,
        product_ref,
        pool_a,
        pool_b,
        pool_c,
        pool_d,
        plane_ref,
        tile_ref,
        gathered,
        local_sem,
        send_sem,
        recv_sem,
        part_send,
        part_recv,
        swap_send,
        swap_recv,
        all_send,
        all_recv,
        word_sem,
        pair_sem,
    ) = refs
    gx, gy, gz = lax.axis_index("gx"), lax.axis_index("gy"), lax.axis_index("gz")

    def turned(at, offset, length):
        offset = offset % length
        if offset == 0:
            return at
        return jnp.where(at >= length - offset, at + offset - length, at + offset)

    def device(dx, dy, dz=0):
        return {"gx": turned(gx, dx, nx), "gy": turned(gy, dy, ny), "gz": turned(gz, dz, 2)}

    fetches = [
        pltpu.make_async_copy(source, target, local_sem.at[k])
        for k, (source, target) in enumerate(zip(inputs, held))
    ]
    fetches[0].start()

    count = nx * ny

    def there(dx, dy):
        tests = []
        if dx:
            tests.append(gx >= -dx if dx < 0 else gx < nx - dx)
        if dy:
            tests.append(gy >= -dy if dy < 0 else gy < ny - dy)
        return tests[0] if len(tests) == 1 else tests[0] & tests[1]

    def box(reach):
        steps = (-reach, 0, reach)
        return [(dx, dy) for dx in steps for dy in steps if (dx, dy) != (0, 0)]

    def hops(offset):
        dx, dy, dz = offset
        ring = lambda k, n: min(k, n - k)
        return ring(dx % 4, 4) + ring(dx // 4, nx // 4) + ring(dy, ny) + 0.5 * dz

    every = ((dx, dy, dz) for dx in range(nx) for dy in range(ny) for dz in (0, 1))
    far = sorted(every, key=hops, reverse=True)[:-1]

    def signal_all(sem, offsets):
        for dx, dy in offsets:

            @pl.when(there(dx, dy))
            def _():
                pl.semaphore_signal(sem, inc=1, device_id=device(dx, dy), device_id_type=MESH)

    def number(offsets):
        return sum(jnp.where(there(dx, dy), 1, 0) for dx, dy in offsets)

    rounds = [box(1), box(2), box(4), [(-8, 0), (8, 0)]]

    def spread_word(k):
        signal_all(word_sem.at[k], rounds[k])

    def hear_word(k):
        pl.semaphore_wait(word_sem.at[k], number(rounds[k]))

    barrier = pltpu.get_barrier_semaphore()
    pl.semaphore_signal(barrier, inc=1, device_id=device(0, 0, 1), device_id_type=MESH)
    signal_all(barrier, box(1))
    for k in (4, 3, 2, 1):
        fetches[k].start()

    def pack(planes):
        lane = lax.broadcasted_iota(jnp.int32, planes[0].shape, 1)
        to_right = jnp.zeros(planes[0].shape, F32)
        to_left = jnp.zeros(planes[0].shape, F32)
        for z, plane in enumerate(planes):
            base = (z % 4) * 32
            low, high = (base, base + EDGE) if z < 4 else (base + EDGE, base)
            shift = (low - (COLUMNS - EDGE)) % 128
            rolled = pltpu.roll(plane, shift, 1) if shift else plane
            to_right = jnp.where((lane >= low) & (lane < low + EDGE), rolled, to_right)
            rolled = pltpu.roll(plane, high, 1) if high else plane
            to_left = jnp.where((lane >= high) & (lane < high + EDGE), rolled, to_left)
        return to_right, to_left

    middle, top, bottom = pl.ds(EDGE, ROWS), pl.ds(0, EDGE), pl.ds(EDGE + ROWS, EDGE)
    head, tail, trunk = pl.ds(0, EDGE), pl.ds(ROWS - EDGE, EDGE), pl.ds(EDGE, ROWS - 2 * EDGE)

    def send(copies):
        for copy, ahead in copies:
            pl.when(ahead)(copy.start)

    def wait_units(sem, units, send):
        for last_x in (True, False):
            for last_y in (True, False):
                end_x = (gx == 0) | (gx == nx - 1)
                end_y = (gy == 0) | (gy == ny - 1)
                here = (end_x if last_x else ~end_x) & (end_y if last_y else ~end_y)
                total = units(1 if last_x else 2, 1 if last_y else 2)
                slab = kernel_ref.at[pl.ds(0, 2), pl.ds(0, total * EDGE // 2)]
                copy = pltpu.make_async_remote_copy(
                    src_ref=slab,
                    dst_ref=slab,
                    send_sem=sem,
                    recv_sem=sem,
                    device_id=device(0, 0, 1),
                    device_id_type=MESH,
                )
                pl.when(here)(copy.wait_send if send else copy.wait_recv)

    def receive_strips(turn):
        wait_units(recv_sem.at[turn, 1], lambda sx, sy: 4 * sy, False)

    def receive_edges(turn):
        wait_units(recv_sem.at[turn, 0], lambda sx, sy: sx * (8 + sy), False)

    def finish_sends(turn):
        wait_units(send_sem.at[turn], lambda sx, sy: 4 * sy + sx * (8 + sy), True)

    def halo_copies(source, turn):
        def copy(src, dst, at, dx, dy):
            sent = pltpu.make_async_remote_copy(
                src_ref=src,
                dst_ref=dst,
                send_sem=send_sem.at[turn],
                recv_sem=recv_sem.at[turn, at],
                device_id=device(dx, dy),
                device_id_type=MESH,
            )
            return sent, there(dx, dy)

        right, left = packed.at[turn, 0], packed.at[turn, 1]
        from_left, from_right = edge_columns.at[turn, 0], edge_columns.at[turn, 1]
        early = [
            copy(source.at[:, tail, :], edge_rows.at[turn, 0], 0, 1, 0),
            copy(source.at[:, head, :], edge_rows.at[turn, 1], 0, -1, 0),
            copy(right.at[tail, :], from_left.at[top, :], 0, 1, 1),
            copy(right.at[head, :], from_left.at[bottom, :], 0, -1, 1),
            copy(left.at[tail, :], from_right.at[top, :], 0, 1, -1),
            copy(left.at[head, :], from_right.at[bottom, :], 0, -1, -1),
        ]
        for rows in (head, tail, trunk):
            into = pl.ds(rows.start + EDGE, rows.size)
            early.append(copy(right.at[rows, :], from_left.at[into, :], 1, 0, 1))
            early.append(copy(left.at[rows, :], from_right.at[into, :], 1, 0, -1))
        return early[:-2], early[-2:]

    def clear_borders():
        rows, columns = jnp.zeros((8, EDGE, 128), F32), jnp.zeros((LX, 128), F32)
        for end, at, part in ((gx == 0, 0, top), (gx == nx - 1, 1, bottom)):

            @pl.when(end)
            def _():
                for turn in (0, 1):
                    edge_rows[turn, at] = rows
                    for side in (0, 1):
                        edge_columns[turn, side, part, :] = columns[:EDGE]

        for end, side in ((gy == 0, 0), (gy == ny - 1, 1)):

            @pl.when(end)
            def _():
                for turn in (0, 1):
                    edge_columns[turn, side] = columns

    def partner_copy(turn, group):
        planes = pl.ds(4 * group, 4)
        return pltpu.make_async_remote_copy(
            src_ref=own_ref.at[turn, planes],
            dst_ref=other_ref.at[turn, planes],
            send_sem=part_send,
            recv_sem=part_recv.at[turn, group],
            device_id=device(0, 0, 1),
            device_id_type=MESH,
        )

    def transform(turn, height, plane_of, left, right, rows_table, adding):
        lane = lax.broadcasted_iota(jnp.int32, (height, 128), 1)
        even = (lane & EDGE) == 0
        mixed = (
            jnp.where(even, left, right),
            jnp.where(even, pltpu.roll(left, 128 - EDGE, 1), pltpu.roll(right, EDGE, 1)),
        )
        rows = []
        for z in range(8):
            j = 32 * (z % 4)
            side = jnp.where((lane >= j) & (lane < j + 32), mixed[z // 4], 0.0)
            rows.append(jnp.concatenate([plane_of(z), side], axis=1))
        split = 2 if adding else 1
        size = 8 // split
        halves = [
            dot(left_triple(jnp.concatenate(rows[k * size : k * size + size], axis=0)), tall_ref[0:768, :])
            for k in range(split)
        ]
        half = halves[0] if split == 1 else jnp.concatenate(halves, axis=0)
        for group in (0, 1):
            whole = []
            for z in (4 * group, 4 * group + 2):
                a = half[z * height : (z + 1) * height]
                b = half[(z + 1) * height : (z + 2) * height]
                joint = jnp.concatenate(
                    [
                        jnp.concatenate([a[:, :128], b[:, :128]], axis=1),
                        jnp.concatenate([a[:, 128:], b[:, 128:]], axis=1),
                    ],
                    axis=0,
                )
                full = dot(wide_ref[:, rows_table], right_triple(joint))
                whole += [full[:, :128], full[:, 128:]]
            for z, part in enumerate(whole, 4 * group):
                own_ref[turn, z] = own_ref[turn, z] + part if adding else part
            if adding:
                partner_copy(turn, group).start()

    def forward_inner(source, turn):
        left, right = edge_columns[turn, 0, middle, :], edge_columns[turn, 1, middle, :]
        transform(turn, ROWS, lambda z: source[z], left, right, slice(0, 384), False)

    def forward_edge(turn):
        def both(a, b):
            return jnp.concatenate([a, b], axis=0)

        left, right = [
            both(edge_columns[turn, side, top, :], edge_columns[turn, side, bottom, :])
            for side in (0, 1)
        ]

        def plane_of(z):
            return both(edge_rows[turn, 0, z], edge_rows[turn, 1, z])

        transform(turn, 2 * EDGE, plane_of, left, right, slice(384, 576), True)

    def depth(x_ref, turn, base, mirrored, adding, planes):
        def blocks(step, carry):
            block(2 * step)
            block(2 * step + 1)
            return carry

        def block(step):
            at = pl.multiple_of(step * 8, 8)
            re, im = pl.ds(at, 8), pl.ds(pl.multiple_of(at + LX, 8), 8)
            xr = {z: x_ref[turn, z, re, :] for z in planes}
            xi = {z: x_ref[turn, z, im, :] for z in planes}
            if adding:
                yr = [product_ref[z, re, :] for z in range(8)]
                yi = [product_ref[z, im, :] for z in range(8)]
            else:
                yr, yi = [None] * 8, [None] * 8
            xs = {z: xr[z] + xi[z] for z in planes}
            sums = [[None] * 8 for _ in range(3)]
            for d in range(-7, 8):
                taps = [kernel_ref[base + d, pl.ds(at + LX * k, 8), :] for k in range(3)]
                values = (xs, xi, xr) if mirrored else (xs, xr, xi)
                for out in range(8):
                    z = out + d if mirrored else out - d
                    if z not in planes:
                        continue
                    for k in range(3):
                        term = taps[k] * values[k][z]
                        sums[k][out] = term if sums[k][out] is None else sums[k][out] + term
            for z in range(8):
                one, two_, three = (sums[k][z] for k in range(3))
                r = one + two_ if mirrored else one - three
                i = one - three if mirrored else one + two_
                yr[z] = r if yr[z] is None else yr[z] + r
                yi[z] = i if yi[z] is None else yi[z] + i
            for z in range(8):
                product_ref[z, re, :] = yr[z]
                product_ref[z, im, :] = yi[z]

        lax.fori_loop(0, LX // 16, blocks, 0)

    def inverse(parts):
        rows = []
        table = slice(64 * parts[0], 64 * parts[-1] + 64)
        for z in range(0, 8, 2):
            joint = jnp.concatenate([product_ref[z], product_ref[z + 1]], axis=1)
            half = dot(wide_ref[table, 896:1472], right_triple(joint))
            for b in (0, 1):
                lanes = slice(128 * b, 128 * b + 128)
                for k in range(len(parts)):
                    re, im = half[64 * k : 64 * k + 32, lanes], half[64 * k + 32 : 64 * k + 64, lanes]
                    rows.append(jnp.concatenate([re, im], axis=1))
        full = dot(jnp.concatenate(two(jnp.concatenate(rows, axis=0)), axis=1), tall_ref[768:1280, :])
        return (full[:, :COLUMNS] + full[:, COLUMNS:]).reshape(8, 32 * len(parts), COLUMNS)

    def convolve(turn, mirrored):
        depth(own_ref, turn, HALO, mirrored, False, range(8))
        base = HALO + 8 - 16 * gz if mirrored else HALO - 8 + 16 * gz
        for group in (0, 1):
            partner_copy(turn, group).wait_recv()
            depth(other_ref, turn, base, mirrored, True, range(4 * group, 4 * group + 4))

    def spectrum():
        for k in (4, 3, 2):
            fetches[k].wait()
        view = index_ref[0]
        taps_ref[...] = jnp.zeros((32, 32, 128), F32)

        taps_ref[0:TAPS, 0:TAPS, 0:TAPS] = psf_ref[view]
        total = jnp.sum(jnp.sum(taps_ref[...], axis=0), axis=(0, 1), keepdims=True)
        scale = 1.0 / total

        for step in range(4):
            x = taps_ref[8 * step : 8 * step + 8].reshape(256, 128) * scale
            high = x.astype(BF16).astype(F32)
            low = x - high
            joint = high + pltpu.roll(high, 32, 1) + pltpu.roll(low, 64, 1)
            half = dot(joint.astype(BF16), tall_ref[1280:1408, :])
            tap_half_ref[8 * step : 8 * step + 8] = half.reshape(8, 32, 256)

        def rows(step, carry):
            for pair in range(4):
                z = 8 * step + 2 * pair
                a, b = tap_half_ref[z], tap_half_ref[z + 1]
                joint = jnp.concatenate(
                    [
                        jnp.concatenate([a[:, :128], b[:, :128]], axis=1),
                        jnp.concatenate([a[:, 128:], b[:, 128:]], axis=1),
                    ],
                    axis=0,
                )
                full = dot(wide_ref[:, 640:832], right_triple(joint))
                for b in (0, 1):
                    re = full[:LX, 128 * b : 128 * b + 128]
                    im = full[LX:, 128 * b : 128 * b + 128]
                    kernel_ref[z + b, 0:LX] = re
                    kernel_ref[z + b, LX : 2 * LX] = im - re
                    kernel_ref[z + b, 2 * LX :] = im + re
            return carry

        lax.fori_loop(0, 4, rows, 0)

    fetches[0].wait()
    packed[0, 0], packed[0, 1] = pack([est_ref[z] for z in range(8)])
    pl.semaphore_wait(barrier, 1 + number(box(1)))
    spread_word(0)
    early, late = halo_copies(est_ref, 0)
    send(early + late)
    clear_borders()
    spectrum()
    fetches[1].wait()
    receive_strips(0)
    forward_inner(est_ref, 0)
    receive_edges(0)
    hear_word(0)
    spread_word(1)
    forward_edge(0)
    convolve(0, False)
    early, late = halo_copies(ratio_ref, 1)
    blurred = inverse((0,))
    ends = []
    for rows, at in ((head, slice(0, EDGE)), (tail, slice(EDGE, 2 * EDGE))):
        ratio = view_ref[:, rows, :] / blurred[:, at]
        ratio_ref[:, rows, :] = ratio
        ends.append(ratio)
    ends = jnp.concatenate(ends, axis=1)
    for side, strip in enumerate(pack([ends[z] for z in range(8)])):
        packed[1, side, head, :] = strip[:EDGE]
        packed[1, side, tail, :] = strip[EDGE:]
    send(early)
    ratio = view_ref[:, trunk, :] / inverse((1,))
    ratio_ref[:, trunk, :] = ratio
    for side, strip in enumerate(pack([ratio[z] for z in range(8)])):
        packed[1, side, trunk, :] = strip
    send(late)
    hear_word(1)
    spread_word(2)
    receive_strips(1)
    forward_inner(ratio_ref, 1)
    receive_edges(1)
    forward_edge(1)
    hear_word(2)
    spread_word(3)
    convolve(1, True)
    hear_word(3)
    pl.semaphore_signal(pair_sem, inc=1, device_id=device(0, 0, 1), device_id_type=MESH)
    correction = inverse((0, 1))
    pieces = [correction[:, :EDGE], correction[:, 2 * EDGE :], correction[:, EDGE : 2 * EDGE]]
    updated = est_ref[...] * jnp.concatenate(pieces, axis=1)
    column_sums = jnp.sum(updated, axis=0)
    halves = [jnp.sum(column_sums[32 * i : 32 * i + 32], axis=0, keepdims=True) for i in (0, 1)]
    source = lax.broadcasted_iota(jnp.int32, (384, 128), 0) % 128
    target = lax.broadcasted_iota(jnp.int32, (384, 128), 1)
    place = jnp.where(target == 4 * gy + source // 32, 2.0**-14, 0.0).astype(BF16)
    eight = jnp.concatenate(halves + [jnp.zeros((6, 128), F32)], axis=0)
    placed = dot(exact_triple(eight), place)
    tile_ref[...] = placed[0:1] + pltpu.roll(placed[1:2], 4 * ny, 1)
    me = gz * count + gx * ny + gy
    pl.semaphore_wait(pair_sem, 1)
    for dx, dy, dz in far:
        pltpu.make_async_remote_copy(
            src_ref=tile_ref,
            dst_ref=gathered.at[me],
            send_sem=all_send,
            recv_sem=all_recv,
            device_id=device(dx, dy, dz),
            device_id_type=MESH,
        ).start()
    gathered[me] = tile_ref[...]

    updated_ref[...] = updated
    for k in range(4):
        pool_a[k] = updated[2 * k] + updated[2 * k + 1]
    even, odd = pl.ds(0, ROWS // 2, stride=2), pl.ds(1, ROWS // 2, stride=2)
    level_one = [(pool_a[k, even, :] + pool_a[k, odd, :]) * 0.25 for k in range(4)]
    for k in (0, 1):
        pool_b[k] = level_one[2 * k] + level_one[2 * k + 1]
    even, odd = pl.ds(0, ROWS // 4, stride=2), pl.ds(1, ROWS // 4, stride=2)
    level_two = [(pool_b[k, even, :] + pool_b[k, odd, :]) * 0.25 for k in (0, 1)]
    pool_c[...] = level_two[0] + level_two[1]
    even, odd = pl.ds(0, ROWS // 8, stride=2), pl.ds(1, ROWS // 8, stride=2)
    level_three = (pool_c[even, :] + pool_c[odd, :]) * 0.25
    pool_d[0:8] = level_three
    pool_d[8:16] = jnp.zeros((8, 128), F32)
    even, odd = pl.ds(0, 8, stride=2), pl.ds(1, 8, stride=2)
    level_four = (pool_d[even, :] + pool_d[odd, :]) * 0.5
    plane_ref[0] = dot(exact_triple(level_four), tall_ref[1792:2176, 128:256])
    swap = pltpu.make_async_remote_copy(
        src_ref=plane_ref.at[0],
        dst_ref=plane_ref.at[1],
        send_sem=swap_send,
        recv_sem=swap_recv,
        device_id=device(0, 0, 1),
        device_id_type=MESH,
    )
    swap.start()
    third = dot(exact_triple(level_three), tall_ref[1792:2176, 0:128])
    three_ref[0] = third[:, :16]
    second = dot(exact_triple(jnp.concatenate(level_two, axis=0)), tall_ref[1408:1792, 128:256])
    for k in (0, 1):
        two_ref[k] = second[16 * k : 16 * k + 16, :32]
    full = dot(exact_triple(jnp.concatenate(level_one, axis=0)), tall_ref[1408:1792, 0:128])
    for k in range(4):
        one_ref[k] = full[32 * k : 32 * k + 32, :64]
    swap.wait_recv()
    fourth = (plane_ref[0] + plane_ref[1]) * 0.5
    four_ref[0] = fourth[:4, :8]

    finish_sends(0)
    finish_sends(1)
    swap.wait_send()
    pltpu.make_async_remote_copy(
        src_ref=own_ref,
        dst_ref=own_ref,
        send_sem=part_send,
        recv_sem=part_send,
        device_id=device(0, 0, 1),
        device_id_type=MESH,
    ).wait_send()
    others = gathered.at[pl.ds(0, 2 * count - 1)]
    everyone = pltpu.make_async_remote_copy(
        src_ref=others,
        dst_ref=others,
        send_sem=all_send,
        recv_sem=all_recv,
        device_id=device(0, 0, 1),
        device_id_type=MESH,
    )
    everyone.wait_send()
    everyone.wait_recv()
    strips = jnp.sum(gathered[...].reshape(2, nx, ny, 128), axis=(0, 2))
    five_ref[0, pl.ds(0, nx, stride=2), :] = strips[:, : 4 * ny]
    five_ref[0, pl.ds(1, nx, stride=2), :] = pltpu.roll(strips, 128 - 4 * ny, 1)[:, : 4 * ny]


def hand_over(*refs):
    sources, targets, sems = refs[:6], refs[6:12], refs[12]
    copies = [pltpu.make_async_copy(a, b, sems.at[k]) for k, (a, b) in enumerate(zip(sources, targets))]
    for copy in copies:
        copy.start()
    for copy in copies:
        copy.wait()


def local(nx, ny, estimate, view_data, psf_stack, view_index):
    vmem = pl.BlockSpec(memory_space=pltpu.VMEM)
    anywhere = pl.BlockSpec(memory_space=pl.ANY)
    shape = jax.ShapeDtypeStruct
    out_shape = (
        shape((8, 64, 128), F32),
        shape((4, 32, 64), F32),
        shape((2, 16, 32), F32),
        shape((1, 8, 16), F32),
        shape((1, 4, 8), F32),
        shape((1, 2 * nx, 4 * ny), F32),
    )
    constants = [jnp.asarray(t) for t in tables()]
    kept = [
        pltpu.with_memory_space_constraint(x, pltpu.HBM)
        for x in (estimate, view_data, psf_stack, *constants)
    ]
    results = pl.pallas_call(
        functools.partial(body, nx, ny),
        out_shape=out_shape,
        in_specs=[pl.BlockSpec(memory_space=pltpu.SMEM)]
        + [pl.BlockSpec(memory_space=pltpu.HBM)] * len(kept),
        out_specs=(vmem,) * 6,
        scratch_shapes=[
            pltpu.VMEM(estimate.shape, F32),
            pltpu.VMEM(view_data.shape, F32),
            pltpu.VMEM(psf_stack.shape, F32),
        ]
        + [pltpu.VMEM(c.shape, c.dtype) for c in constants]
        + [
            pltpu.VMEM((32, 32, 128), F32),
            pltpu.VMEM((32, 32, 256), F32),
            pltpu.VMEM((32, 3 * LX, 128), F32),
            pltpu.VMEM((8, ROWS, COLUMNS), F32),
            pltpu.VMEM((2, 2, 8, EDGE, 128), F32),
            pltpu.VMEM((2, 2, LX, 128), F32),
            pltpu.VMEM((2, 2, ROWS, 128), F32),
            pltpu.VMEM((2, 8, 2 * LX, 128), F32),
            pltpu.VMEM((2, 8, 2 * LX, 128), F32),
            pltpu.VMEM((8, 2 * LX, 128), F32),
            pltpu.VMEM((4, 64, 128), F32),
            pltpu.VMEM((2, 32, 128), F32),
            pltpu.VMEM((16, 128), F32),
            pltpu.VMEM((16, 128), F32),
            pltpu.VMEM((2, 8, 128), F32),
            pltpu.VMEM((1, 128), F32),
            pltpu.VMEM((2 * nx * ny, 1, 128), F32),
            pltpu.SemaphoreType.DMA((len(kept),)),
            pltpu.SemaphoreType.DMA((2,)),
            pltpu.SemaphoreType.DMA((2, 2)),
            pltpu.SemaphoreType.DMA,
            pltpu.SemaphoreType.DMA((2, 2)),
            pltpu.SemaphoreType.DMA,
            pltpu.SemaphoreType.DMA,
            pltpu.SemaphoreType.DMA,
            pltpu.SemaphoreType.DMA,
            pltpu.SemaphoreType.REGULAR((4,)),
            pltpu.SemaphoreType.REGULAR,
        ],
        compiler_params=pltpu.CompilerParams(
            collective_id=0, has_side_effects=True, vmem_limit_bytes=32 << 20
        ),
    )(view_index, *kept)
    return pl.pallas_call(
        hand_over,
        out_shape=out_shape,
        in_specs=[vmem] * 6,
        out_specs=(anywhere,) * 6,
        scratch_shapes=[pltpu.SemaphoreType.DMA((6,))],
        compiler_params=pltpu.CompilerParams(vmem_limit_bytes=4 << 20),
    )(*results)


def solution(mesh):
    spread = P("gz", "gx", "gy")
    return jax.shard_map(
        functools.partial(local, mesh.shape["gx"], mesh.shape["gy"]),
        mesh=mesh,
        in_specs=(spread, spread, P(), P()),
        out_specs=(spread, spread, spread, spread, P(None, "gx", "gy"), P()),
        check_vma=False,
    )
```
